256 devices in a mesh: dp: 64 (over z, y_lo, x), tensor: 4 (over y_hi, core).
Axes of the slice: x: 4, y: 4 (y_hi: 2, y_lo: 2; y = y_hi * 2 + y_lo), z: 8, core: 2. Of those that a mesh axis runs over, the one named last changes fastest.
Arguments:
- out_first: bfloat16 [64, 197, 1024], P('dp', None, 'tensor'), may hold values from -6 to 6
- out_second: bfloat16 [64, 197, 1024], P('dp', None, 'tensor'), may hold values from -6 to 6
- grad_first: bfloat16 [64, 197, 1024], P('dp', None, 'tensor'), may hold values from -6 to 6
- grad_second: bfloat16 [64, 197, 1024], P('dp', None, 'tensor'), may hold values from -16 to 16
- gain_attn: float32 [1024], replicated, may hold values from 0.25 to 1.75
- gain_mlp: float32 [1024], replicated, may hold values from 0.25 to 1.75
- qkv_weight: bfloat16 [1024, 3, 1024], P(None, None, 'tensor'), may hold values from -1 to 1
- proj_weight: bfloat16 [1024, 1024], P(None, 'tensor'), may hold values from -0.1875 to 0.1875
- inner_weight: bfloat16 [1024, 4096], P(None, 'tensor'), may hold values from -0.1875 to 0.1875
- inner_bias: float32 [4096], P('tensor'), may hold values from -3 to 3
- outer_weight: bfloat16 [1024, 4096], P(None, 'tensor'), may hold values from -0.09375 to 0.09375
Outputs:
- input_first: bfloat16 [64, 197, 1024], P('dp', None, 'tensor')
- input_second: bfloat16 [64, 197, 1024], P('dp', None, 'tensor')
- back_first: bfloat16 [64, 197, 1024], P('dp', None, 'tensor')
- back_second: bfloat16 [64, 197, 1024], P('dp', None, 'tensor')
- grad_qkv: float32 [1024, 3, 1024], P('dp', None, 'tensor')
- grad_proj: float32 [1024, 1024], P('dp', 'tensor')
- grad_inner: float32 [1024, 4096], P('dp', 'tensor')
- grad_bias: float32 [4096], P('tensor')
- grad_outer: float32 [1024, 4096], P('dp', 'tensor')
- grad_gain_attn: float32 [1024], P('tensor')
- grad_gain_mlp: float32 [1024], P('tensor')
The draws below stay inside these ranges and needn't reach their ends.
All inputs are finite; a program needn't handle non-finite values.
Results may differ from the reference program's by a relative error of at most 0.016.
Values may be sent and summed in bfloat16 or wider, within the bound.
A program may use at most 64 MiB of HBM per device.

```python
import jax
import jax.numpy as jnp
from jax import lax

D = 1024
HEADS = 16
FF = 4096
SEQ = 197
IMAGES = 64


def draw_qkv_weight(key, part):
    base_key = jax.random.fold_in(key, 0)
    base_draw = jax.random.truncated_normal(base_key, -6.0, 6.0, (D, 3, D), jnp.float32) / D ** 0.5
    return jnp.clip(base_draw, -1.0, 1.0).astype(jnp.bfloat16)


def strengthened(array, own_key, source, target, blocks, factor):
    def block_of(axis_at):
        return (jnp.arange(array.shape[axis_at]) // (array.shape[axis_at] // blocks)).reshape((-1,) + (1,) * (array.ndim - 1 - axis_at))

    first = jax.random.permutation(own_key, blocks)[block_of(target)]
    other_side = (block_of(target) + blocks // 2) % blocks
    return jnp.where((block_of(source) == first) | (block_of(source) == other_side), factor * array, array)


def steps_of(key, shape, cuts, least, high):
    level = 1.0
    for axis_at, shards_of in cuts:
        heights = jax.random.uniform(jax.random.fold_in(jax.random.fold_in(key, 6), axis_at), (shards_of,), jnp.float32, least / len(cuts), high / len(cuts))
        level = level * jnp.repeat(jnp.exp(heights), shape[axis_at] // shards_of).reshape((-1,) + (1,) * (len(shape) - 1 - axis_at))
    return level


def noise(rng, shape, deviation, limit, cuts=(), dtype=jnp.bfloat16):
    values = jax.random.normal(rng, shape, jnp.float32) * deviation
    if len(cuts) > 0:
        values = steps_of(rng, shape, cuts, -0.22, 0.18) * values
    return jnp.clip(values, min=-limit, max=limit).astype(dtype)


def heavy_noise(own_key, shape, deviation, limit, pieces, heavy, kind=jnp.bfloat16):
    array = deviation * jax.random.normal(own_key, shape, jnp.float32)
    if pieces:
        array = array * steps_of(own_key, shape, pieces, -0.22, 0.18)
    return jnp.clip(strengthened(array, jax.random.fold_in(own_key, 3), *heavy), -limit, limit).astype(kind)


def setup_inputs(seed: int = 0) -> dict:
    keys = jax.random.split(jax.random.key(seed), 12)
    out_first = noise(keys[0], (IMAGES, SEQ, D), 1.0, 6.0, ((0, 64), (2, 4)))
    out_second = noise(keys[1], (IMAGES, SEQ, D), 1.0, 6.0, ((0, 64), (2, 4)))
    grad_first = noise(keys[2], (IMAGES, SEQ, D), 1.0, 6.0, ((0, 64), (2, 4)))
    grad_second = heavy_noise(keys[3], (IMAGES, SEQ, D), 1.0, 16.0, ((0, 64), (2, 4)), (0, 2, 64, 4.0))
    gain_attn = jnp.clip(1.0 + 0.15 * jax.random.normal(keys[4], (D,), jnp.float32), 0.25, 1.75)
    gain_mlp = jnp.clip(1.0 + 0.15 * jax.random.normal(keys[5], (D,), jnp.float32), 0.25, 1.75)
    qkv_weight = draw_qkv_weight(jax.random.fold_in(keys[11], 71), 0)
    proj_weight = noise(keys[7], (D, D), D ** -0.5, 0.1875, ((1, 4),))
    inner_weight = noise(keys[8], (D, FF), D ** -0.5, 0.1875, ((1, 4),))
    inner_bias = noise(keys[9], (FF,), 0.5, 3.0, ((0, 4),), jnp.float32)
    outer_weight = noise(keys[10], (D, FF), FF ** -0.5, 0.09375, ((1, 4),))
    return {"out_first": out_first, "out_second": out_second, "grad_first": grad_first, "grad_second": grad_second, "gain_attn": gain_attn, "gain_mlp": gain_mlp, "qkv_weight": qkv_weight, "proj_weight": proj_weight, "inner_weight": inner_weight, "inner_bias": inner_bias, "outer_weight": outer_weight}


epsilon = 1e-06

def normalize(values):
    centre = values - lax.optimization_barrier(jnp.mean(values, -1, keepdims=True))
    spread = lax.rsqrt(lax.optimization_barrier(jnp.mean(centre * centre, -1, keepdims=True)) + epsilon)
    return (centre * spread, spread)

def norm_back(grad_in, normed, spread, gain):
    scaled = grad_in * gain
    first_mean = lax.optimization_barrier(jnp.mean(scaled, -1, keepdims=True))
    second_mean = lax.optimization_barrier(jnp.mean(scaled * normed, -1, keepdims=True))
    return spread * (scaled - first_mean - normed * second_mean)

def image_attention(members):
    queries = members[0].astype(jnp.float32)
    key_rows = members[1].astype(jnp.float32)
    value_rows = members[2].astype(jnp.float32)
    grad_heads = members[3].astype(jnp.float32)
    factor = (D // HEADS) ** (-0.5)
    scores = jnp.einsum('qhe,khe->hqk', queries, key_rows) * factor
    attn_probs = jax.nn.softmax(scores, -1)
    probs_low = attn_probs.astype(jnp.bfloat16)
    probs_wide = probs_low.astype(jnp.float32)
    heads_out = jnp.einsum('hqk,khe->qhe', probs_wide, value_rows).astype(jnp.bfloat16)
    grad_probs = jnp.einsum('qhe,khe->hqk', grad_heads, value_rows)
    grad_value = jnp.einsum('hqk,qhe->khe', probs_wide, grad_heads).astype(jnp.bfloat16)
    row_dot = lax.optimization_barrier(jnp.sum(grad_probs * attn_probs, -1, keepdims=True))
    grad_scores = (attn_probs * (grad_probs - row_dot)).astype(jnp.bfloat16).astype(jnp.float32)
    grad_query = (jnp.einsum('hqk,khe->qhe', grad_scores, key_rows) * factor).astype(jnp.bfloat16)
    grad_key = (jnp.einsum('hqk,qhe->khe', grad_scores, queries) * factor).astype(jnp.bfloat16)
    return (heads_out, grad_query, grad_key, grad_value)

def reference(out_first, out_second, grad_first, grad_second, gain_attn, gain_mlp, qkv_weight, proj_weight, inner_weight, inner_bias, outer_weight):
    rows_all = IMAGES * SEQ
    head_dim = D // HEADS
    first_rows = out_first.reshape(rows_all, D).astype(jnp.float32)
    second_rows = out_second.reshape(rows_all, D).astype(jnp.float32)
    upper_grad = grad_first.reshape(rows_all, D).astype(jnp.float32)
    lower_grad = grad_second.reshape(rows_all, D)
    normed_mlp, spread_mlp = normalize(first_rows)
    input_mlp = (normed_mlp * gain_mlp).astype(jnp.bfloat16)
    hidden = jnp.dot(input_mlp, inner_weight, preferred_element_type=jnp.float32) + inner_bias
    active = jax.nn.gelu(hidden).astype(jnp.bfloat16)
    mlp_out = jnp.dot(active, outer_weight.T, preferred_element_type=jnp.float32)
    input_second = (second_rows - mlp_out).astype(jnp.bfloat16)
    grad_active = jnp.dot(lower_grad, outer_weight, preferred_element_type=jnp.float32)
    grad_hidden = jax.vjp(jax.nn.gelu, hidden)[1](grad_active)[0].astype(jnp.bfloat16)
    grad_outer = jnp.dot(lower_grad.T, active, preferred_element_type=jnp.float32)
    grad_inner = jnp.dot(input_mlp.T, grad_hidden, preferred_element_type=jnp.float32)
    grad_bias = lax.optimization_barrier(jnp.sum(grad_hidden.astype(jnp.float32), 0))
    grad_norm_mlp = jnp.dot(grad_hidden, inner_weight.T, preferred_element_type=jnp.float32)
    grad_gain_mlp = lax.optimization_barrier(jnp.sum(grad_norm_mlp * normed_mlp, 0))
    back_first = (upper_grad + norm_back(grad_norm_mlp, normed_mlp, spread_mlp, gain_mlp)).astype(jnp.bfloat16)
    normed_attn, spread_attn = normalize(input_second.astype(jnp.float32))
    input_attn = (normed_attn * gain_attn).astype(jnp.bfloat16)
    qkv_rows = jnp.einsum('td,dcj->tcj', input_attn.astype(jnp.float32), qkv_weight.astype(jnp.float32)).astype(jnp.bfloat16)
    grad_heads = jnp.dot(back_first, proj_weight, preferred_element_type=jnp.float32).astype(jnp.bfloat16)
    shaped = qkv_rows.reshape(IMAGES, SEQ, 3, HEADS, head_dim)
    heads_out, grad_query, grad_key, grad_value = lax.map(image_attention, (shaped[:, :, 0], shaped[:, :, 1], shaped[:, :, 2], grad_heads.reshape(IMAGES, SEQ, HEADS, head_dim)))
    attn_rows = heads_out.reshape(rows_all, D)
    grad_rows = jnp.stack([grad_query, grad_key, grad_value], 2).reshape(rows_all, 3, D)
    attn_out = jnp.dot(attn_rows, proj_weight.T, preferred_element_type=jnp.float32)
    input_first = (first_rows - attn_out).astype(jnp.bfloat16)
    grad_proj = jnp.dot(back_first.T, attn_rows, preferred_element_type=jnp.float32)
    grad_qkv = jnp.einsum('td,tcj->dcj', input_attn.astype(jnp.float32), grad_rows.astype(jnp.float32))
    grad_norm_attn = jnp.einsum('tcj,dcj->td', grad_rows.astype(jnp.float32), qkv_weight.astype(jnp.float32))
    grad_gain_attn = lax.optimization_barrier(jnp.sum(grad_norm_attn * normed_attn, 0))
    back_second = (lower_grad.astype(jnp.float32) + norm_back(grad_norm_attn, normed_attn, spread_attn, gain_attn)).astype(jnp.bfloat16)
    shape_out = (IMAGES, SEQ, D)
    return (input_first.reshape(shape_out), input_second.reshape(shape_out), back_first.reshape(shape_out), back_second.reshape(shape_out), grad_qkv, grad_proj, grad_inner, grad_bias, grad_outer, grad_gain_attn, grad_gain_mlp)
```

```python
import functools

import jax
import jax.numpy as jnp
from jax import lax
from jax.experimental import pallas as pl
from jax.experimental.pallas import tpu as pltpu
from jax.sharding import Mesh
from jax.sharding import PartitionSpec as P

AXES = ("z", "yl", "x", "yh", "c")
DP = ("z", "yl", "x")
TENSOR = ("yh", "c")
MESH = pl.DeviceIdType.MESH
SEQ = 197
R = 208
K = 256
W = 256
NZ, NX = 8, 4
EPS = 1e-06
F32 = jnp.float32
BF16 = jnp.bfloat16
GELU_A = 0.7978845608028654
GELU_B = 0.044715
SEMS = 160


def nn(a, b):
    return lax.dot_general(a, b, (((1,), (0,)), ((), ())), preferred_element_type=F32)


def nt(a, b):
    return lax.dot_general(a, b, (((1,), (1,)), ((), ())), preferred_element_type=F32)


def at_cols(ref, lo, hi):
    return ref.at[(slice(None),) * (len(ref.shape) - 1) + (slice(lo, hi),)]


def add_into(dst, src):
    lead = dst.shape[:-2]
    total = 1
    for n in lead:
        total *= n
    if total == 1:
        where = (0,) * len(lead)
        dst[where] = dst[where] + src[where]
        return

    def body(j, _):
        where = []
        rest = j
        for n in reversed(lead):
            where.append(lax.rem(rest, n))
            rest = lax.div(rest, n)
        where = tuple(reversed(where))
        dst[where] = dst[where] + src[where]
        return 0

    lax.fori_loop(0, total, body, 0)


class Chain:
    def __init__(self, net, chunk, axis, size, recv):
        self.net, self.chunk, self.axis, self.size, self.recv = net, chunk, axis, size, recv
        self.pos = net.pos[axis]
        self.steps = size // 2
        self.flying = None

    def part(self, ref, way, distance):
        if distance == self.steps:
            half = ref.shape[-1] // 2
            return at_cols(ref, way * half, (way + 1) * half)
        return ref

    def owner(self, way, distance):
        return lax.rem(self.pos + (distance if way == 0 else self.size - distance), self.size)

    def send(self, way, step):
        distance = self.steps - step + 1
        src = self.part(self.chunk(self.owner(way, distance)), way, distance)
        dst = self.part(self.recv.at[way, step - 1], way, distance)
        target = self.net.dev(**{self.axis: self.owner(way, 1)})
        return self.net.copy(src, dst, target)

    def start(self):
        self.flying = [self.send(0, 1), self.send(1, 1)]

    def tick(self, step):
        later = [None, None]
        for way in (0, 1):
            distance = self.steps - step + 1
            self.flying[way].wait_recv()
            got = self.part(self.recv.at[way, step - 1], way, distance)
            mine = self.part(self.chunk(self.owner(way, distance - 1)), way, distance)
            add_into(mine, got)
            if step < self.steps:
                later[way] = self.send(way, step + 1)
        self.flying = later


class Scatter:
    def __init__(self, net, buf, first, r1, r2, r3, finish):
        z, x, yl = net.pos["z"], net.pos["x"], net.pos["yl"]
        self.net, self.r3, self.finish = net, r3, finish
        if first == "z":
            one = Chain(net, lambda o: buf.at[o], "z", NZ, r1)
            two = Chain(net, lambda o: buf.at[z, :, o], "x", NX, r2)
            self.last = lambda y: buf.at[z, y, x]
        else:
            one = Chain(net, lambda o: buf.at[o], "x", NX, r1)
            two = Chain(net, lambda o: buf.at[x, o], "z", NZ, r2)
            self.last = lambda y: buf.at[x, z, y]
        self.one, self.two, self.yl = one, two, yl
        self.todo = [one.start]
        for s in range(1, one.steps + 1):
            self.todo.append(functools.partial(one.tick, s))
        self.todo.append(two.start)
        for s in range(1, two.steps + 1):
            self.todo.append(functools.partial(two.tick, s))
        self.todo.append(self.start_last)
        self.todo.append(self.end_last)
        merged, k = [[self.todo[0]]], 1
        for f in self.todo[1:]:
            if f == two.start or f == self.start_last:
                merged[-1].append(f)
            else:
                merged.append([f])
        self.todo = merged

    def start_last(self):
        self.flying = self.net.copy(
            self.last(1 - self.yl), self.r3, self.net.dev(yl=1 - self.yl)
        )

    def end_last(self):
        self.flying.wait_recv()
        self.finish(self.last(self.yl)[...].astype(F32) + self.r3[...].astype(F32))

    def tick(self):
        if self.todo:
            for f in self.todo.pop(0):
                f()


class Everyone:
    def __init__(self, net, slots, finish):
        self.net, self.slots, self.finish = net, slots, finish
        self.stages = [("z", NZ), ("x", NX), ("yl", 2)]
        self.at = 0

    def send(self, block):
        axis, n = self.stages[self.at]
        me = self.net.pos[axis]
        slot = self.slots[self.at]
        slot[me] = block
        self.flying = []
        for k in range(1, n):
            target = self.net.dev(**{axis: lax.rem(me + k, n)})
            self.flying.append(self.net.copy(slot.at[me], slot.at[me], target))

    def tick(self):
        if self.at == 3:
            return
        for c in self.flying:
            c.wait_recv()
        slot = self.slots[self.at]
        total = slot[0]
        for k in range(1, self.stages[self.at][1]):
            total = total + slot[k]
        self.at += 1
        if self.at == 3:
            self.finish(total)
        else:
            self.send(total)


class Net:
    def __init__(self, send_sem, recv_sem):
        self.pos = {a: lax.axis_index(a) for a in AXES}
        self.send_sem, self.recv_sem = send_sem, recv_sem
        self.started = []

    def dev(self, **other):
        where = dict(self.pos)
        where.update(other)
        return tuple(where[a] for a in AXES)

    def copy(self, src, dst, target):
        k = len(self.started)
        assert k < SEMS
        c = pltpu.make_async_remote_copy(
            src_ref=src,
            dst_ref=dst,
            send_sem=self.send_sem.at[k],
            recv_sem=self.recv_sem.at[k],
            device_id=target,
            device_id_type=MESH,
        )
        c.start()
        self.started.append(c)
        return c

    def drain(self):
        for c in self.started:
            c.wait_send()


def kernel(
    of_ref, os_ref, gf_ref, gs_ref, gain_attn_ref, gain_mlp_ref, wq_hbm, wp_hbm, wi_hbm, bias_ref, wo_hbm,
    o_first, o_second, o_bfirst, o_bsecond, o_qkv, o_proj, o_inner, o_bias, o_outer, o_gattn, o_gmlp,
    wq, wp, wi, wo, w_sem, send_sem, recv_sem,
    xg, gg, xs, xb, nm, im, act, dg, gh, lhs_a, lhs_b,
    pair_a, pair_b, pair_c, pair_d, mine_a, mine_b, out_a, out_b, out_c, out_d, in_a, in_b, in_c, in_d,
    stat_a, stat_b, qs, ks, vs, hs, rows_s, g3,
    ga, gb, ra1, ra2, ra3, rb1, rb2, rb3,
    ha, hb, sa1, sa2, sa3, sb1, sb2, sb3,
    t1z, t1x, t1y, t2z, t2x, t2y,
):
    net = Net(send_sem, recv_sem)
    pos = net.pos
    yh, c = pos["yh"], pos["c"]
    me, sib = 2 * yh + c, 2 * yh + 1 - c
    far, diag = 2 * (1 - yh) + c, 2 * (1 - yh) + 1 - c
    d_sib, d_far, d_diag = net.dev(c=1 - c), net.dev(yh=1 - yh), net.dev(yh=1 - yh, c=1 - c)

    barrier = pltpu.get_barrier_semaphore()
    others = [d_sib, d_far, d_diag, net.dev(yl=1 - pos["yl"])]
    others += [net.dev(z=lax.rem(pos["z"] + k, NZ)) for k in range(1, NZ)]
    others += [net.dev(x=lax.rem(pos["x"] + k, NX)) for k in range(1, NX)]
    for other in others:
        pl.semaphore_signal(barrier, inc=1, device_id=other, device_id_type=MESH)

    loads = [
        pltpu.make_async_copy(wi_hbm, wi, w_sem.at[0]),
        pltpu.make_async_copy(wo_hbm, wo, w_sem.at[1]),
        pltpu.make_async_copy(wq_hbm, wq, w_sem.at[2]),
        pltpu.make_async_copy(wp_hbm, wp, w_sem.at[3]),
    ]
    for load in loads:
        load.start()

    zero_rows = jnp.zeros((K - R, W), BF16)
    xg[me] = jnp.zeros((R, W), BF16)
    xg[me, 0:SEQ] = of_ref[...]
    gg[me, 0:R] = jnp.zeros((R, W), BF16)
    gg[me, 0:SEQ] = gs_ref[...]
    pl.semaphore_wait(barrier, len(others))

    def gather_start(ref, block=None):
        own = ref.at[me, 0:R]
        return [net.copy(own, own, d_far), net.copy(own, own, d_sib)]

    def gather_forward(ref, two):
        two[0].wait_recv()
        got = ref.at[far, 0:R]
        two.append(net.copy(got, got, d_sib))

    def gather_end(two):
        two[1].wait_recv()
        two[2].wait_recv()

    x_all = gather_start(xg)
    g_all = gather_start(gg)
    for b in range(4):
        gg[b, R:K] = zero_rows
        xb[b, R:K] = zero_rows
        for ref in (im, act, gh):
            ref[R:K, b * W : (b + 1) * W] = zero_rows
    for ref in (qs, ks, vs, hs):
        ref[R:K] = zero_rows
    gather_forward(xg, x_all)
    gather_end(x_all)

    def gain_of(ref, b):
        return ref[0:1, b * W : (b + 1) * W]

    def gain_at(ref, b):
        return ref[0:1, pl.ds(pl.multiple_of(b * W, W), W)]

    def normalize(block, gain_ref):
        total = jnp.zeros((R, 1), F32)
        for b in range(4):
            total = total + jnp.sum(block(b), 1, keepdims=True)
        mean = total * (1.0 / 1024)
        square = jnp.zeros((R, 1), F32)
        for b in range(4):
            centre = block(b) - mean
            nm[b] = centre
            square = square + jnp.sum(centre * centre, 1, keepdims=True)
        spread = lax.rsqrt(square * (1.0 / 1024) + EPS)
        for b in range(4):
            normed = nm[b] * spread
            nm[b] = normed
            im[0:R, b * W : (b + 1) * W] = (normed * gain_of(gain_ref, b)).astype(BF16)
        return spread

    spread_mlp = normalize(lambda b: xg[b].astype(F32), gain_mlp_ref)

    loads[0].wait()
    for n in range(4):
        cols = slice(n * W, (n + 1) * W)
        u = nn(im[0:R], wi[:, cols]) + bias_ref[0:1, cols]
        square = u * u
        t = jnp.tanh(GELU_A * (u + GELU_B * (square * u)))
        half = 0.5 * (1.0 + t)
        act[0:R, cols] = (u * half).astype(BF16)
        slope = 0.5 * GELU_A * (1.0 - t * t) * (1.0 + 3.0 * GELU_B * square)
        dg[0:R, cols] = half + u * slope
        if n == 1:
            gather_forward(gg, g_all)

    loads[1].wait()

    def rows_at(ref, q):
        return ref[pl.ds(pl.multiple_of(q * W, W), W), :]

    pair_a[0, 0] = nt(act[0:R], rows_at(wo, sib))
    pair_a[0, 1] = nt(act[0:R], rows_at(wo, diag))
    pair_mlp = net.copy(pair_a.at[0], pair_a.at[1], d_sib)
    mine_a[0] = nt(act[0:R], rows_at(wo, far))
    mine_a[1] = nt(act[0:R], rows_at(wo, me))
    pair_mlp.wait_recv()
    out_a[...] = (mine_a[0] + pair_a[1, 1]).astype(BF16)
    far_mlp = net.copy(out_a, in_a, d_far)
    gather_end(g_all)

    for n in range(4):
        cols = slice(n * W, (n + 1) * W)
        grad_active = nn(gg[0, 0:R], wo[0:W, cols])
        for b in range(1, 4):
            grad_active = grad_active + nn(gg[b, 0:R], wo[b * W : (b + 1) * W, cols])
        low = (grad_active * dg[0:R, cols]).astype(BF16)
        gh[0:R, cols] = low
        o_bias[0:1, cols] = jnp.sum(low.astype(F32), 0, keepdims=True)

    lane = lax.broadcasted_iota(jnp.int32, (R, 128), 1)

    def stats_of(part, q, gain_ref, sums):
        scaled = part * gain_at(gain_ref, q)
        one = sums[0] + jnp.sum(scaled, 1, keepdims=True)
        two = sums[1] + jnp.sum(scaled * nm[q], 1, keepdims=True)
        return (one, two)

    def stats_send(sums, stat):
        both = jnp.where(lane == 0, sums[0], jnp.where(lane == 1, sums[1], 0.0))
        both = jnp.concatenate([both, jnp.zeros((K - R, 128), F32)], 0)
        stat[me] = both.T[0:8, :]
        return [net.copy(stat.at[me], stat.at[me], d) for d in (d_sib, d_far, d_diag)]

    def stats_end(sent, stat):
        for s in sent:
            s.wait_recv()
        total = (stat[0] + stat[1]) + (stat[2] + stat[3])
        wide = jnp.concatenate([total * (1.0 / 1024), jnp.zeros((120, K), F32)], 0).T
        return wide[0:R, 0:1], wide[0:R, 1:2]

    def norm_back(part_of, gain_ref, pair, mine, out, inn, stat, between):
        sums = (jnp.zeros((R, 1), F32), jnp.zeros((R, 1), F32))
        for slot, q in ((0, sib), (1, diag)):
            part = part_of(q)
            pair[0, slot] = part
            sums = stats_of(part, q, gain_ref, sums)
        swap = net.copy(pair.at[0], pair.at[1], d_sib)
        for slot, q in ((0, far), (1, me)):
            part = part_of(q)
            mine[slot] = part
            sums = stats_of(part, q, gain_ref, sums)
        sent = stats_send(sums, stat)
        swap.wait_recv()
        out[...] = (mine[0] + pair[1, 1]).astype(BF16)
        last = net.copy(out, inn, d_far)
        between()
        last.wait_recv()
        first_mean, second_mean = stats_end(sent, stat)
        grad = mine[1] + pair[1, 0] + inn[...].astype(F32)
        return grad, first_mean, second_mean

    ends = {}
    valid = lax.broadcasted_iota(jnp.int32, (R, W), 0) < SEQ

    def outer_term(lhs, rhs, buf, first, col):
        for b in range(4):
            tile = nn(lhs[b * W : (b + 1) * W], rhs).astype(BF16).reshape(2, 2, 4, 16, W)
            if first == "z":
                buf[2 * b : 2 * b + 2, :, :, :, col : col + W] = tile
            else:
                for x in range(4):
                    buf[x, 2 * b : 2 * b + 2, :, :, col : col + W] = tile[:, :, x]

    def finish_outer(total):
        o_outer[...] = total

    def finish_inner(total):
        o_inner[...] = total

    def finish_ha(total):
        o_proj[...] = total[:, 0:W]
        o_qkv[2] = total[:, W : 2 * W]

    def finish_hb(total):
        o_qkv[0] = total[:, 0:W]
        o_qkv[1] = total[:, W : 2 * W]

    def finish_small1(total):
        for n in range(4):
            o_bias[0:1, n * W : (n + 1) * W] = total[n : n + 1]
        o_gmlp[...] = total[4:5]

    def finish_small2(total):
        o_gattn[...] = total[0:1]

    s_outer = Scatter(net, ga, "z", ra1, ra2, ra3, finish_outer)
    s_inner = Scatter(net, gb, "x", rb1, rb2, rb3, finish_inner)
    s_ha = Scatter(net, ha, "z", sa1, sa2, sa3, finish_ha)
    s_hb = Scatter(net, hb, "x", sb1, sb2, sb3, finish_hb)
    small1 = Everyone(net, (t1z, t1x, t1y), finish_small1)
    small2 = Everyone(net, (t2z, t2x, t2y), finish_small2)

    def between_mlp():
        far_mlp.wait_recv()
        mlp = mine_a[1] + pair_a[1, 0] + in_a[...].astype(F32)
        os_wide = os_ref[...].astype(F32)
        second = jnp.where(valid[0:SEQ], os_wide - mlp[0:SEQ], 0.0).astype(BF16)
        o_second[...] = second
        xs[me] = jnp.zeros((R, W), BF16)
        xs[me, 0:SEQ] = second
        ends["second"] = gather_start(xs)
        for b in range(4):
            lhs_a[b * W : (b + 1) * W] = gg[b].T
        for n in range(4):
            outer_term(lhs_a, act[:, n * W : (n + 1) * W], ga, "z", n * W)
        s_outer.tick()

    grad, first_mean, second_mean = norm_back(
        lambda q: nt(gh[0:R], rows_at(wi, q)),
        gain_mlp_ref, pair_b, mine_b, out_b, in_b, stat_a, between_mlp,
    )
    normed_own = nm[me]
    back = spread_mlp * (grad * gain_at(gain_mlp_ref, me) - first_mean - normed_own * second_mean)
    first = (gf_ref[...].astype(F32) + back[0:SEQ]).astype(BF16)
    o_bfirst[...] = first
    xb[me, 0:R] = jnp.zeros((R, W), BF16)
    xb[me, 0:SEQ] = first
    b_all = gather_start(xb)
    gather_forward(xs, ends["second"])
    block = [o_bias[0:1, n * W : (n + 1) * W] for n in range(4)]
    block.append(jnp.sum(grad * normed_own, 0, keepdims=True))
    small1.send(jnp.concatenate(block + [jnp.zeros((3, W), F32)], 0))

    for b in range(4):
        lhs_b[b * W : (b + 1) * W] = im[:, b * W : (b + 1) * W].T
    for n in range(4):
        outer_term(lhs_b, gh[:, n * W : (n + 1) * W], gb, "x", n * W)
    s_inner.tick()
    gather_end(ends["second"])

    spread_attn = normalize(lambda b: xs[b].astype(F32), gain_attn_ref)
    gather_forward(xb, b_all)
    s_outer.tick()
    loads[2].wait()
    for kind, ref in enumerate((qs, ks, vs)):
        ref[0:R] = nn(im[0:R], wq[kind]).astype(BF16)
    for b in range(4):
        lhs_a[b * W : (b + 1) * W] = im[:, b * W : (b + 1) * W].T
    small1.tick()
    gather_end(b_all)
    loads[3].wait()
    heads = nn(xb[0, 0:R], wp[0:W])
    for b in range(1, 4):
        heads = heads + nn(xb[b, 0:R], wp[b * W : (b + 1) * W])
    hs[0:R] = heads.astype(BF16)
    for b in range(4):
        lhs_b[b * W : (b + 1) * W] = xb[b].T
    s_inner.tick()
    s_outer.tick()

    head_lane = lax.broadcasted_iota(jnp.int32, (K, W), 1) // 64
    key_ok = lax.broadcasted_iota(jnp.int32, (K, K), 1) < SEQ
    factor = 0.125

    def only(ref, h):
        return jnp.where(head_lane == h, ref[...], jnp.zeros((), BF16))

    attn = jnp.zeros((K, W), F32)
    grads = [jnp.zeros((K, W), F32) for _ in range(3)]
    for h in range(4):
        q_h, k_h, v_h, g_h = only(qs, h), only(ks, h), only(vs, h), only(hs, h)
        scores = jnp.where(key_ok, nt(q_h, ks[...]) * factor, -1e30)
        e = jnp.exp(scores - jnp.max(scores, 1, keepdims=True))
        probs = e / jnp.sum(e, 1, keepdims=True)
        low = probs.astype(BF16)
        grad_probs = nt(g_h, vs[...])
        row_dot = jnp.sum(grad_probs * probs, 1, keepdims=True)
        grad_scores = (probs * (grad_probs - row_dot)).astype(BF16)
        a_h = nn(low, v_h)
        gv_h = nn(low.T, g_h)
        gq_h = nn(grad_scores, k_h)
        gk_h = nn(grad_scores.T, q_h)
        if h == 0:
            rows_s[0], rows_s[1], rows_s[2], rows_s[3] = a_h, gq_h, gk_h, gv_h
        else:
            rows_s[0] += a_h
            rows_s[1] += gq_h
            rows_s[2] += gk_h
            rows_s[3] += gv_h
        if h == 1:
            small1.tick()
    rows_low = rows_s[0].astype(BF16)
    g3[0] = (rows_s[1] * factor).astype(BF16)
    g3[1] = (rows_s[2] * factor).astype(BF16)
    g3[2] = rows_s[3].astype(BF16)

    for slot, q in ((0, sib), (1, diag)):
        pair_c[0, slot] = nt(rows_low[0:R], rows_at(wp, q))
    pair_out = net.copy(pair_c.at[0], pair_c.at[1], d_sib)
    for slot, q in ((0, far), (1, me)):
        mine_a[slot] = nt(rows_low[0:R], rows_at(wp, q))
    s_outer.tick()
    pair_out.wait_recv()
    out_c[...] = (mine_a[0] + pair_c[1, 1]).astype(BF16)
    far_out = net.copy(out_c, in_c, d_far)

    outer_term(lhs_b, rows_low, ha, "z", 0)
    outer_term(lhs_a, g3[2], ha, "z", W)
    s_ha.tick()
    outer_term(lhs_a, g3[0], hb, "x", 0)
    outer_term(lhs_a, g3[1], hb, "x", W)
    s_hb.tick()
    small1.tick()

    def qkv_part(q):
        at = pl.ds(pl.multiple_of(q * W, W), W)
        part = nt(g3[0, 0:R], wq[0, at, :])
        part = part + nt(g3[1, 0:R], wq[1, at, :])
        return part + nt(g3[2, 0:R], wq[2, at, :])

    def between_attn():
        far_out.wait_recv()
        total = mine_a[1] + pair_c[1, 0] + in_c[...].astype(F32)
        o_first[...] = (of_ref[...].astype(F32) - total[0:SEQ]).astype(BF16)
        s_outer.tick()
        s_inner.tick()

    grad, first_mean, second_mean = norm_back(
        qkv_part, gain_attn_ref, pair_d, mine_b, out_d, in_d, stat_b, between_attn
    )
    normed_own = nm[me]
    small2.send(
        jnp.concatenate([jnp.sum(grad * normed_own, 0, keepdims=True), jnp.zeros((7, W), F32)], 0)
    )
    back = spread_attn * (grad * gain_at(gain_attn_ref, me) - first_mean - normed_own * second_mean)
    o_bsecond[...] = (gs_ref[...].astype(F32) + back[0:SEQ]).astype(BF16)

    for _ in range(8):
        s_ha.tick()
        s_hb.tick()
        small2.tick()
        s_outer.tick()
        s_inner.tick()
    assert not (s_ha.todo or s_hb.todo or s_outer.todo or s_inner.todo)
    assert small1.at == 3 and small2.at == 3
    net.drain()


def on_device(
    out_first, out_second, grad_first, grad_second, gain_attn, gain_mlp,
    qkv_weight, proj_weight, inner_weight, inner_bias, outer_weight,
):
    sds = jax.ShapeDtypeStruct
    vmem = pl.BlockSpec(memory_space=pltpu.VMEM)
    hbm = pl.BlockSpec(memory_space=pl.ANY)

    def v(*shape, dtype=BF16):
        return pltpu.VMEM(shape, dtype)

    def scatter_bufs(cols):
        a = [v(8, 2, 4, 16, cols), v(4, 8, 2, 16, cols)]
        za = [v(2, 4, 2, 4, 16, cols), v(2, 2, 2, 16, cols), v(16, cols)]
        xb = [v(2, 2, 8, 2, 16, cols), v(2, 4, 2, 16, cols), v(16, cols)]
        return a + za + xb

    scratch = [
        v(3, 1024, W), v(1024, W), v(1024, 1024), v(1024, 1024), pltpu.SemaphoreType.DMA((4,)),
        pltpu.SemaphoreType.DMA((SEMS,)), pltpu.SemaphoreType.DMA((SEMS,)),
        v(4, R, W), v(4, K, W), v(4, R, W), v(4, K, W), v(4, R, W, dtype=F32),
        v(K, 1024), v(K, 1024), v(R, 1024, dtype=F32), v(K, 1024), v(1024, K), v(1024, K),
        *[v(2, 2, R, W, dtype=F32) for _ in range(4)],
        *[v(2, R, W, dtype=F32) for _ in range(2)],
        *[v(R, W) for _ in range(8)],
        v(4, 8, K, dtype=F32), v(4, 8, K, dtype=F32),
        *[v(K, W) for _ in range(4)],
        v(4, K, W, dtype=F32), v(3, K, W),
        *scatter_bufs(1024), *scatter_bufs(512),
        *[v(n, 8, W, dtype=F32) for n in (8, 4, 2, 8, 4, 2)],
    ]
    outs = pl.pallas_call(
        kernel,
        out_shape=[
            sds((SEQ, W), BF16), sds((SEQ, W), BF16), sds((SEQ, W), BF16), sds((SEQ, W), BF16),
            sds((3, 16, W), F32), sds((16, W), F32), sds((16, 1024), F32), sds((1, 1024), F32),
            sds((16, 1024), F32), sds((1, W), F32), sds((1, W), F32),
        ],
        in_specs=[vmem] * 6 + [hbm] * 3 + [vmem, hbm],
        out_specs=[vmem] * 11,
        scratch_shapes=scratch,
        compiler_params=pltpu.CompilerParams(
            collective_id=0, has_side_effects=True, vmem_limit_bytes=60 * 1024 * 1024
        ),
        name="block_pair",
    )(
        out_first[0], out_second[0], grad_first[0], grad_second[0],
        gain_attn.reshape(1, -1), gain_mlp.reshape(1, -1),
        jnp.swapaxes(qkv_weight, 0, 1), proj_weight, inner_weight, inner_bias.reshape(1, -1), outer_weight,
    )
    return (
        outs[0][None], outs[1][None], outs[2][None], outs[3][None],
        jnp.swapaxes(outs[4], 0, 1), outs[5], outs[6], outs[7].reshape(-1), outs[8],
        outs[9].reshape(-1), outs[10].reshape(-1),
    )


def solution(mesh):
    split = Mesh(mesh.devices.reshape(NZ, 2, NX, 2, 2), AXES)
    rows = P(DP, None, TENSOR)
    return jax.shard_map(
        on_device,
        mesh=split,
        in_specs=(
            rows, rows, rows, rows, P(), P(),
            P(None, None, TENSOR), P(None, TENSOR), P(None, TENSOR), P(TENSOR), P(None, TENSOR),
        ),
        out_specs=(
            rows, rows, rows, rows,
            P(DP, None, TENSOR), P(DP, TENSOR), P(DP, TENSOR), P(TENSOR), P(DP, TENSOR),
            P(TENSOR), P(TENSOR),
        ),
        check_vma=False,
    )
```

```python
import functools

import jax
import jax.numpy as jnp
from jax import lax
from jax.experimental import pallas as pl
from jax.experimental.pallas import tpu as pltpu
from jax.sharding import Mesh
from jax.sharding import PartitionSpec as P

AXES = ("z", "yl", "x", "yh", "c")
DP = ("z", "yl", "x")
TENSOR = ("yh", "c")
MESH = pl.DeviceIdType.MESH
SEQ = 197
R = 208
K = 256
W = 256
NZ, NX = 8, 4
EPS = 1e-06
F32 = jnp.float32
BF16 = jnp.bfloat16
GELU_A = 0.7978845608028654
GELU_B = 0.044715
SENDS, RECVS = 71, 71
PIECES = (
    ("A1", "outer", "z", 0, 256),
    ("A2", "outer", "z", 256, 512),
    ("B0", "outer", "xz", 512, 1024),
    ("A3", "inner", "z", 0, 256),
    ("B1", "inner", "xz", 256, 1024),
    ("a1", "v", "z", 0, 256),
    ("a2", "proj", "z", 0, 256),
    ("b1", "q", "x", 0, 256),
    ("b2", "k", "x", 0, 256),
)
TICKS = {
    "swap": ("A1", "A2"),
    "inner": ("B0",),
    "back": ("A1", "A2"),
    "forward": ("A3",),
    "qkv": ("B1",),
    "probs": ("A1", "A2"),
    "heads": ("A3", "s1"),
    "attn": ("B0", "A1", "A2"),
    "pair": ("A3", "B0"),
    "last": ("a1", "a2", "s1", "B0", "B1"),
    "tail": (
        "a1", "a2", "b1", "b2", "A3", "A1", "A2", "B0", "B1",
        "a1", "a2", "A3", "B0", "B1", "b1", "b2", "s2",
        "B0", "B1", "a1", "a2", "s2", "B1", "b1", "b2", "B1", "a1", "a2",
    ),
}


def nn(a, b):
    return lax.dot_general(a, b, (((1,), (0,)), ((), ())), preferred_element_type=F32)


def nt(a, b):
    return lax.dot_general(a, b, (((1,), (1,)), ((), ())), preferred_element_type=F32)


def at_cols(ref, lo, hi):
    return ref.at[(slice(None),) * (len(ref.shape) - 1) + (slice(lo, hi),)]


def add_into(dst, src):
    lead = dst.shape[:-2]
    total = 1
    for n in lead:
        total *= n
    if total == 1:
        where = (0,) * len(lead)
        dst[where] = dst[where] + src[where]
        return

    def body(j, _):
        where = []
        rest = j
        for n in reversed(lead):
            where.append(lax.rem(rest, n))
            rest = lax.div(rest, n)
        where = tuple(reversed(where))
        dst[where] = dst[where] + src[where]
        return 0

    lax.fori_loop(0, total, body, 0)


class Phases:
    def __init__(self):
        self.scope = None

    def __call__(self, name):
        if self.scope is not None:
            self.scope.__exit__(None, None, None)
        self.scope = jax.named_scope(name) if name else None
        if name:
            self.scope.__enter__()


class Net:
    def __init__(self, send_sem, recv_sem):
        self.pos = {a: lax.axis_index(a) for a in AXES}
        self.send_sem, self.recv_sem = send_sem, recv_sem
        self.sends, self.recvs = 0, 0
        self.out = []

    def dev(self, **other):
        where = dict(self.pos)
        where.update(other)
        return tuple(where[a] for a in AXES)

    def copies(self, triples, sent, got=None):
        k, m = self.sends, self.recvs
        self.sends, self.recvs = k + 1, m + 1
        assert self.sends <= SENDS and self.recvs <= RECVS

        def describe(src, dst, target):
            return pltpu.make_async_remote_copy(
                src_ref=src,
                dst_ref=dst,
                send_sem=self.send_sem.at[k],
                recv_sem=self.recv_sem.at[m],
                device_id=target,
                device_id_type=MESH,
            )

        for triple in triples:
            describe(*triple).start()
        target = triples[0][2]
        self.out.append(describe(sent, sent, target))
        return describe(sent if got is None else got, sent if got is None else got, target)

    def copy(self, src, dst, target):
        return self.copies([(src, dst, target)], src, dst)

    def drain(self):
        for c in self.out:
            c.wait_send()


class Chain:
    def __init__(self, net, chunk, axis, size, recv):
        self.net, self.chunk, self.axis, self.size, self.recv = net, chunk, axis, size, recv
        self.pos = net.pos[axis]
        self.steps = size // 2

    def part(self, ref, way, distance):
        if distance == self.steps:
            half = ref.shape[-1] // 2
            return at_cols(ref, way * half, (way + 1) * half)
        return ref

    def owner(self, way, distance):
        return lax.rem(self.pos + (distance if way == 0 else self.size - distance), self.size)

    def send(self, step):
        distance = self.steps - step + 1
        triples = []
        for way in (0, 1):
            src = self.part(self.chunk(self.owner(way, distance)), way, distance)
            dst = self.part(self.recv.at[way, step - 1], way, distance)
            triples.append((src, dst, self.net.dev(**{self.axis: self.owner(way, 1)})))
        both = self.recv.at[0, 0] if step == 1 else self.recv.at[:, step - 1]
        self.flying = self.net.copies(triples, both)

    def tick(self, step):
        self.flying.wait_recv()
        distance = self.steps - step + 1
        for way in (0, 1):
            got = self.part(self.recv.at[way, step - 1], way, distance)
            mine = self.part(self.chunk(self.owner(way, distance - 1)), way, distance)
            add_into(mine, got)
        if step < self.steps:
            self.send(step + 1)


class Spread:
    def __init__(self, net, ring, size, recv):
        self.net, self.ring, self.size, self.recv = net, ring, size, recv

    def start(self, piece):
        net, ring, size = self.net, self.ring, self.size
        triples = []
        for j in range(1, 2 * size):
            there = lax.rem(net.pos[ring] + j % size, size)
            y = lax.rem(net.pos["yl"] + j // size, 2)
            triples.append((piece(there, y), self.recv.at[j], net.dev(**{ring: there, "yl": y})))
        self.flying = net.copies(triples, self.recv.at[1 : 2 * size])

    def end(self, own):
        self.flying.wait_recv()
        total = own
        for j in range(1, 2 * self.size):
            total = total + self.recv[j].astype(F32)
        return total


class Scatter:
    def __init__(self, net, first, bufs, finish):
        z, x, yl = net.pos["z"], net.pos["x"], net.pos["yl"]
        buf = bufs[0]
        self.todo = []
        if first == "z":
            one = Chain(net, lambda o: buf.at[o], "z", NZ, bufs[1])
            last = Spread(net, "x", NX, bufs[2])
            piece = lambda there, y: buf.at[z, y, there]
            own = lambda: buf[z, yl, x].astype(F32)
        else:
            one = Chain(net, lambda o: buf.at[o], "x", NX, bufs[1])
            piece = lambda there, y: buf.at[x, there, y]
            own = lambda: buf[x, z, yl].astype(F32)
            if first == "xz":
                two = Chain(net, lambda o: buf.at[x, o], "z", NZ, bufs[2])
            else:
                last = Spread(net, "z", NZ, bufs[2])
        self.todo.append(functools.partial(one.send, 1))
        for k in range(1, one.steps):
            self.todo.append(functools.partial(one.tick, k))
        if first == "xz":

            def turn():
                one.tick(one.steps)
                two.send(1)

            self.todo.append(turn)
            for k in range(1, two.steps):
                self.todo.append(functools.partial(two.tick, k))

            def across():
                two.tick(two.steps)
                self.flying = net.copy(buf.at[x, z, 1 - yl], bufs[3], net.dev(yl=1 - yl))

            def end():
                self.flying.wait_recv()
                finish(own() + bufs[3][...].astype(F32))

            self.todo += [across, end]
        else:

            def turn():
                one.tick(one.steps)
                last.start(piece)

            self.todo += [turn, lambda: finish(last.end(own()))]

    def tick(self):
        self.todo.pop(0)()


class Everyone:
    def __init__(self, net, slots, finish):
        self.net, self.slots, self.finish = net, slots, finish
        self.todo = [self.turn, self.end]

    def send(self, block):
        self.slots[0][0] = block
        self.one = Spread(self.net, "z", NZ, self.slots[0])
        self.one.start(lambda there, y: self.slots[0].at[0])

    def turn(self):
        net, slot = self.net, self.slots[1]
        slot[0] = self.one.end(self.slots[0][0])
        triples = []
        for k in range(1, NX):
            target = net.dev(x=lax.rem(net.pos["x"] + k, NX))
            triples.append((slot.at[0], slot.at[k], target))
        self.flying = net.copies(triples, slot.at[1:NX])

    def end(self):
        self.flying.wait_recv()
        slot = self.slots[1]
        self.finish(((slot[0] + slot[1]) + slot[2]) + slot[3])

    def tick(self):
        self.todo.pop(0)()


def kernel(
    of_hbm, os_hbm, gf_hbm, gs_hbm, gain_attn_hbm, gain_mlp_hbm, wq_hbm, wp_hbm, wi_hbm, bias_hbm, wo_hbm,
    o_first, o_second, o_bfirst, o_bsecond, o_qkv, o_proj, o_inner, o_bias, o_outer, o_gattn, o_gmlp,
    of_ref, os_ref, gf_ref, gs_ref, gain_attn_ref, gain_mlp_ref, wq, wp, wi, bias_ref, wo,
    load_sem, send_sem, recv_sem,
    xg, gg, xs, xb, nm, im, act, dg, gh, lhs_a, lhs_b,
    pair_a, pair_b, pair_c, pair_d, mine_a, mine_b, out_a, out_b, out_c, out_d, in_a, in_b, in_c, in_d,
    stat_a, stat_b, qs, ks, vs, hs, rows_s, probs_s, g3,
    *rest,
):
    phase = Phases()
    phase("entry")
    net = Net(send_sem, recv_sem)
    pos = net.pos
    yh, c = pos["yh"], pos["c"]
    me, sib = 2 * yh + c, 2 * yh + 1 - c
    far, diag = 2 * (1 - yh) + c, 2 * (1 - yh) + 1 - c
    d_sib, d_far, d_diag = net.dev(c=1 - c), net.dev(yh=1 - yh), net.dev(yh=1 - yh, c=1 - c)

    loads = {}
    for k, (name, src, dst) in enumerate(
        (
            ("of", of_hbm, of_ref), ("gs", gs_hbm, gs_ref), ("gm", gain_mlp_hbm, gain_mlp_ref),
            ("bias", bias_hbm, bias_ref), ("wi", wi_hbm, wi), ("wo", wo_hbm, wo), ("os", os_hbm, os_ref),
            ("gf", gf_hbm, gf_ref), ("ga", gain_attn_hbm, gain_attn_ref), ("wq", wq_hbm, wq), ("wp", wp_hbm, wp),
        )
    ):
        loads[name] = pltpu.make_async_copy(src, dst, load_sem.at[k])
        loads[name].start()

    barrier = pltpu.get_barrier_semaphore()
    others = [d_sib, d_far, d_diag]
    for dy in range(2):
        y = lax.rem(pos["yl"] + dy, 2)
        others += [net.dev(z=lax.rem(pos["z"] + k, NZ), yl=y) for k in range(1 - dy, NZ)]
        others += [net.dev(x=lax.rem(pos["x"] + k, NX), yl=y) for k in range(1, NX)]
    for other in others:
        pl.semaphore_signal(barrier, inc=1, device_id=other, device_id_type=MESH)

    zero_rows = jnp.zeros((K - R, W), BF16)
    loads["of"].wait()
    xg[me] = jnp.zeros((R, W), BF16)
    xg[me, 0:SEQ] = of_ref[...]
    loads["gs"].wait()
    gg[me, 0:R] = jnp.zeros((R, W), BF16)
    gg[me, 0:SEQ] = gs_ref[...]
    for b in range(4):
        gg[b, R:K] = zero_rows
        xb[b, R:K] = zero_rows
        for ref in (im, act, gh):
            ref[R:K, b * W : (b + 1) * W] = zero_rows
    for ref in (qs, ks, vs, hs):
        ref[R:K] = zero_rows
    pl.semaphore_wait(barrier, len(others))

    def gather_start(ref):
        own = ref.at[me, 0:R]
        return [net.copy(own, own, d_far), net.copy(own, own, d_sib)]

    def gather_forward(ref, two):
        two[0].wait_recv()
        got = ref.at[far, 0:R]
        two.append(net.copy(got, got, d_sib))

    def gather_end(two):
        two[1].wait_recv()
        two[2].wait_recv()

    def gain_of(ref, b):
        return ref[0:1, b * W : (b + 1) * W]

    def gain_at(ref, b):
        return ref[0:1, pl.ds(pl.multiple_of(b * W, W), W)]

    def rows_at(ref, q):
        return ref[pl.ds(pl.multiple_of(q * W, W), W), :]

    def normalize(block, gain_ref):
        total = jnp.zeros((R, 1), F32)
        for b in range(4):
            total = total + jnp.sum(block(b), 1, keepdims=True)
        mean = total * (1.0 / 1024)
        square = jnp.zeros((R, 1), F32)
        for b in range(4):
            centre = block(b) - mean
            nm[b] = centre
            square = square + jnp.sum(centre * centre, 1, keepdims=True)
        spread = lax.rsqrt(square * (1.0 / 1024) + EPS)
        for b in range(4):
            normed = nm[b] * spread
            nm[b] = normed
            im[0:R, b * W : (b + 1) * W] = (normed * gain_of(gain_ref, b)).astype(BF16)
        return spread

    def turn(lhs, block):
        for b in range(4):
            lhs[b * W : (b + 1) * W] = block(b).T

    lane = lax.broadcasted_iota(jnp.int32, (R, 128), 1)

    def stats_of(part, q, gain_ref, sums):
        scaled = part * gain_at(gain_ref, q)
        one = sums[0] + jnp.sum(scaled, 1, keepdims=True)
        two = sums[1] + jnp.sum(scaled * nm[q], 1, keepdims=True)
        return (one, two)

    def stats_send(sums, stat):
        both = jnp.where(lane == 0, sums[0], jnp.where(lane == 1, sums[1], 0.0))
        both = jnp.concatenate([both, jnp.zeros((K - R, 128), F32)], 0)
        stat[0] = both.T[0:8, :]
        triples = [(stat.at[0], stat.at[k + 1], d) for k, d in enumerate((d_sib, d_far, d_diag))]
        return net.copies(triples, stat.at[1:4])

    def stats_end(sent, stat):
        sent.wait_recv()
        total = (stat[0] + stat[1]) + (stat[2] + stat[3])
        wide = jnp.concatenate([total * (1.0 / 1024), jnp.zeros((120, K), F32)], 0).T
        return wide[0:R, 0:1], wide[0:R, 1:2]

    def norm_back(part_of, gain_ref, pair, mine, out, inn, stat, stop, between):
        phase("nb_parts")
        sums = (jnp.zeros((R, 1), F32), jnp.zeros((R, 1), F32))
        for slot, q in ((0, sib), (1, diag)):
            part = part_of(q)
            pair[0, slot] = part
            sums = stats_of(part, q, gain_ref, sums)
        swap = net.copy(pair.at[0], pair.at[1], d_sib)
        for slot, q in ((0, far), (1, me)):
            part = part_of(q)
            mine[slot] = part
            sums = stats_of(part, q, gain_ref, sums)
        sent = stats_send(sums, stat)
        phase("nb_swap_wait")
        swap.wait_recv()
        out[...] = (mine[0] + pair[1, 1]).astype(BF16)
        last = net.copy(out, inn, d_far)
        tick(*TICKS[stop])
        between()
        phase("nb_last_wait")
        last.wait_recv()
        first_mean, second_mean = stats_end(sent, stat)
        grad = mine[1] + pair[1, 0] + inn[...].astype(F32)
        return grad, first_mean, second_mean

    def outer_term(lhs, rhs, scatter, col):
        first, buf = scatter
        for b in range(4):
            tile = nn(lhs[b * W : (b + 1) * W], rhs).astype(BF16).reshape(2, 2, 4, 16, W)
            if first == "z":
                buf[2 * b : 2 * b + 2, :, :, :, col : col + W] = tile
            else:
                for x in range(4):
                    buf[x, 2 * b : 2 * b + 2, :, :, col : col + W] = tile[:, :, x]

    def writer(ref, lo, hi):
        def finish(total):
            ref[:, lo:hi] = total

        return finish

    def kind_writer(k):
        def finish(total):
            o_qkv[k] = total

        return finish

    targets = {
        "outer": lambda lo, hi: writer(o_outer, lo, hi),
        "inner": lambda lo, hi: writer(o_inner, lo, hi),
        "proj": lambda lo, hi: writer(o_proj, lo, hi),
        "q": lambda lo, hi: kind_writer(0),
        "k": lambda lo, hi: kind_writer(1),
        "v": lambda lo, hi: kind_writer(2),
    }
    scatters, at = {}, 0
    for name, what, first, lo, hi in PIECES:
        bufs = rest[at : at + 4]
        at += 4
        scatters[name] = (Scatter(net, first, bufs, targets[what](lo, hi)), (first, bufs[0]))

    def finish_small1(total):
        for n in range(4):
            o_bias[0:1, n * W : (n + 1) * W] = total[n : n + 1]
        o_gmlp[...] = total[4:5]

    def finish_small2(total):
        o_gattn[...] = total[0:1]

    small1 = Everyone(net, rest[at : at + 2], finish_small1)
    small2 = Everyone(net, rest[at + 2 : at + 4], finish_small2)

    def make(what, lhs, tile_of):
        for name, kind, first, lo, hi in PIECES:
            if kind == what:
                for col in range(lo, hi, W):
                    outer_term(lhs, tile_of(col), scatters[name][1], col - lo)
                scatters[name][0].tick()

    def tick(*names):
        for name in names:
            phase("tick_" + name)
            if name == "s1":
                small1.tick()
            elif name == "s2":
                small2.tick()
            else:
                scatters[name][0].tick()

    x_all = gather_start(xg)
    g_all = gather_start(gg)
    phase("gather_x_wait")
    gather_forward(xg, x_all)
    gather_end(x_all)
    phase("norm_mlp")
    loads["gm"].wait()
    spread_mlp = normalize(lambda b: xg[b].astype(F32), gain_mlp_ref)
    phase("hidden")
    loads["bias"].wait()
    loads["wi"].wait()
    for n in range(4):
        cols = slice(n * W, (n + 1) * W)
        u = nn(im[0:R], wi[:, cols]) + bias_ref[0:1, cols]
        square = u * u
        t = jnp.tanh(GELU_A * (u + GELU_B * (square * u)))
        half = 0.5 * (1.0 + t)
        act[0:R, cols] = (u * half).astype(BF16)
        slope = 0.5 * GELU_A * (1.0 - t * t) * (1.0 + 3.0 * GELU_B * square)
        dg[0:R, cols] = half + u * slope
        if n == 1:
            gather_forward(gg, g_all)
    phase("mlp_out")
    loads["wo"].wait()
    pair_a[0, 0] = nt(act[0:R], rows_at(wo, sib))
    pair_a[0, 1] = nt(act[0:R], rows_at(wo, diag))
    pair_mlp = net.copy(pair_a.at[0], pair_a.at[1], d_sib)
    mine_a[0] = nt(act[0:R], rows_at(wo, far))
    mine_a[1] = nt(act[0:R], rows_at(wo, me))
    phase("g_wait")
    gather_end(g_all)
    phase("turn_g")
    turn(lhs_a, lambda b: gg[b])
    phase("pair_mlp_wait")
    pair_mlp.wait_recv()
    out_a[...] = (mine_a[0] + pair_a[1, 1]).astype(BF16)
    far_mlp = net.copy(out_a, in_a, d_far)
    phase("outer_grad")
    make("outer", lhs_a, lambda col: act[:, col : col + W])

    phase("grad_active")
    bias_rows = []
    for n in range(4):
        cols = slice(n * W, (n + 1) * W)
        grad_active = nn(gg[0, 0:R], wo[0:W, cols])
        for b in range(1, 4):
            grad_active = grad_active + nn(gg[b, 0:R], wo[b * W : (b + 1) * W, cols])
        low = (grad_active * dg[0:R, cols]).astype(BF16)
        gh[0:R, cols] = low
        bias_rows.append(jnp.sum(low.astype(F32), 0, keepdims=True))

    valid = lax.broadcasted_iota(jnp.int32, (SEQ, W), 0) < SEQ
    ends = {}

    def between_mlp():
        phase("turn_im")
        turn(lhs_b, lambda b: im[:, b * W : (b + 1) * W])
        phase("far_mlp_wait")
        far_mlp.wait_recv()
        phase("input_second")
        loads["os"].wait()
        mlp = mine_a[1] + pair_a[1, 0] + in_a[...].astype(F32)
        second = (os_ref[...].astype(F32) - mlp[0:SEQ]).astype(BF16)
        o_second[...] = second
        xs[me] = jnp.zeros((R, W), BF16)
        xs[me, 0:SEQ] = second
        ends["second"] = gather_start(xs)
        phase("inner_grad")
        make("inner", lhs_b, lambda col: gh[:, col : col + W])
        tick(*TICKS["inner"])

    grad, first_mean, second_mean = norm_back(
        lambda q: nt(gh[0:R], rows_at(wi, q)),
        gain_mlp_ref, pair_b, mine_b, out_b, in_b, stat_a, "swap", between_mlp,
    )
    phase("back_first")
    loads["gf"].wait()
    normed_own = nm[me]
    back = spread_mlp * (grad * gain_at(gain_mlp_ref, me) - first_mean - normed_own * second_mean)
    first = (gf_ref[...].astype(F32) + back[0:SEQ]).astype(BF16)
    o_bfirst[...] = first
    xb[me, 0:R] = jnp.zeros((R, W), BF16)
    xb[me, 0:SEQ] = first
    b_all = gather_start(xb)
    block = bias_rows + [jnp.sum(grad * normed_own, 0, keepdims=True), jnp.zeros((3, W), F32)]
    small1.send(jnp.concatenate(block, 0))
    tick(*TICKS["back"])
    phase("xs_forward")
    gather_forward(xs, ends["second"])
    tick(*TICKS["forward"])
    phase("xs_wait")
    gather_end(ends["second"])

    phase("norm_attn")
    loads["ga"].wait()
    spread_attn = normalize(lambda b: xs[b].astype(F32), gain_attn_ref)
    phase("qkv")
    loads["wq"].wait()
    for kind, ref in enumerate((qs, ks, vs)):
        ref[0:R] = nn(im[0:R], wq[kind]).astype(BF16)
    phase("turn_attn")
    turn(lhs_a, lambda b: im[:, b * W : (b + 1) * W])
    tick(*TICKS["qkv"])

    head_lane = lax.broadcasted_iota(jnp.int32, (K, W), 1) // 64
    key_ok = lax.broadcasted_iota(jnp.int32, (K, K), 1) < SEQ
    factor = 0.125

    def only(ref, h):
        return jnp.where(head_lane == h, ref[...], jnp.zeros((), BF16))

    for h in range(4):
        phase(f"probs_{h}")
        scores = jnp.where(key_ok, nt(only(qs, h), ks[...]) * factor, -1e30)
        e = jnp.exp(scores - jnp.max(scores, 1, keepdims=True))
        probs = e / jnp.sum(e, 1, keepdims=True)
        probs_s[h] = probs
        a_h = nn(probs.astype(BF16), only(vs, h))
        if h == 0:
            rows_s[0] = a_h
        else:
            rows_s[0] += a_h
        if h == 1:
            phase("xb_forward")
            gather_forward(xb, b_all)
    tick(*TICKS["probs"])
    phase("attn_out")
    rows_low = rows_s[0].astype(BF16)
    loads["wp"].wait()
    for slot, q in ((0, sib), (1, diag)):
        pair_c[0, slot] = nt(rows_low[0:R], rows_at(wp, q))
    pair_out = net.copy(pair_c.at[0], pair_c.at[1], d_sib)
    for slot, q in ((0, far), (1, me)):
        mine_a[slot] = nt(rows_low[0:R], rows_at(wp, q))
    phase("xb_wait")
    gather_end(b_all)
    phase("grad_heads")
    heads = nn(xb[0, 0:R], wp[0:W])
    for b in range(1, 4):
        heads = heads + nn(xb[b, 0:R], wp[b * W : (b + 1) * W])
    hs[0:R] = heads.astype(BF16)
    phase("pair_out_wait")
    pair_out.wait_recv()
    out_c[...] = (mine_a[0] + pair_c[1, 1]).astype(BF16)
    far_out = net.copy(out_c, in_c, d_far)
    phase("proj_grad")
    turn(lhs_b, lambda b: xb[b])
    make("proj", lhs_b, lambda col: rows_low)
    tick(*TICKS["heads"])

    for h in range(4):
        phase(f"head_{h}")
        q_h, k_h, g_h = only(qs, h), only(ks, h), only(hs, h)
        probs = probs_s[h]
        grad_probs = nt(g_h, vs[...])
        row_dot = jnp.sum(grad_probs * probs, 1, keepdims=True)
        grad_scores = (probs * (grad_probs - row_dot)).astype(BF16)
        gv_h = nn(probs.astype(BF16).T, g_h)
        gq_h = nn(grad_scores, k_h)
        gk_h = nn(grad_scores.T, q_h)
        if h == 0:
            rows_s[1], rows_s[2], rows_s[3] = gq_h, gk_h, gv_h
        else:
            rows_s[1] += gq_h
            rows_s[2] += gk_h
            rows_s[3] += gv_h
    phase("attn_grads")
    g3[0] = (rows_s[1] * factor).astype(BF16)
    g3[1] = (rows_s[2] * factor).astype(BF16)
    g3[2] = rows_s[3].astype(BF16)
    make("v", lhs_a, lambda col: g3[2])
    make("q", lhs_a, lambda col: g3[0])
    make("k", lhs_a, lambda col: g3[1])
    tick(*TICKS["attn"])

    def qkv_part(q):
        cols = pl.ds(pl.multiple_of(q * W, W), W)
        part = nt(g3[0, 0:R], wq[0, cols, :])
        part = part + nt(g3[1, 0:R], wq[1, cols, :])
        return part + nt(g3[2, 0:R], wq[2, cols, :])

    def between_attn():
        phase("far_out_wait")
        far_out.wait_recv()
        total = mine_a[1] + pair_c[1, 0] + in_c[...].astype(F32)
        o_first[...] = (of_ref[...].astype(F32) - total[0:SEQ]).astype(BF16)
        tick(*TICKS["last"])

    grad, first_mean, second_mean = norm_back(
        qkv_part, gain_attn_ref, pair_d, mine_b, out_d, in_d, stat_b, "pair", between_attn
    )
    phase("back_second")
    normed_own = nm[me]
    small2.send(
        jnp.concatenate([jnp.sum(grad * normed_own, 0, keepdims=True), jnp.zeros((7, W), F32)], 0)
    )
    back = spread_attn * (grad * gain_at(gain_attn_ref, me) - first_mean - normed_own * second_mean)
    o_bsecond[...] = (gs_ref[...].astype(F32) + back[0:SEQ]).astype(BF16)
    tick(*TICKS["tail"])
    assert not (small1.todo or small2.todo or any(one.todo for one, _ in scatters.values()))
    phase("drain")
    assert (net.sends, net.recvs) == (SENDS, RECVS), (net.sends, net.recvs)
    net.drain()
    phase(None)


def hand_over(*refs):
    half = len(refs) // 2
    for src, dst in zip(refs[:half], refs[half:]):
        dst[...] = src[...]


def on_device(
    out_first, out_second, grad_first, grad_second, gain_attn, gain_mlp,
    qkv_weight, proj_weight, inner_weight, inner_bias, outer_weight,
):
    sds = jax.ShapeDtypeStruct
    vmem = pl.BlockSpec(memory_space=pltpu.VMEM)
    hbm = pl.BlockSpec(memory_space=pltpu.HBM)

    def v(*shape, dtype=BF16):
        return pltpu.VMEM(shape, dtype)

    def piece_bufs(first, cols):
        if first == "z":
            return [v(8, 2, 4, 16, cols), v(2, 4, 2, 4, 16, cols), v(8, 16, cols), v(16, 128)]
        bufs = [v(4, 8, 2, 16, cols), v(2, 2, 8, 2, 16, cols)]
        if first == "x":
            return bufs + [v(16, 16, cols), v(16, 128)]
        return bufs + [v(2, 4, 2, 16, cols), v(16, cols)]

    pieces = []
    for _, _, first, lo, hi in PIECES:
        pieces += piece_bufs(first, hi - lo)
    scratch = [
        *[v(SEQ, W) for _ in range(4)], v(1, 1024, dtype=F32), v(1, 1024, dtype=F32),
        v(3, 1024, W), v(1024, W), v(1024, 1024), v(1, 1024, dtype=F32), v(1024, 1024),
        pltpu.SemaphoreType.DMA((11,)),
        pltpu.SemaphoreType.DMA((SENDS,)), pltpu.SemaphoreType.DMA((RECVS,)),
        v(4, R, W), v(4, K, W), v(4, R, W), v(4, K, W), v(4, R, W, dtype=F32),
        v(K, 1024), v(K, 1024), v(R, 1024, dtype=F32), v(K, 1024), v(1024, K), v(1024, K),
        *[v(2, 2, R, W, dtype=F32) for _ in range(4)],
        *[v(2, R, W, dtype=F32) for _ in range(2)],
        *[v(R, W) for _ in range(8)],
        v(4, 8, K, dtype=F32), v(4, 8, K, dtype=F32),
        *[v(K, W) for _ in range(4)],
        v(4, K, W, dtype=F32), v(4, K, K, dtype=F32), v(3, K, W),
        *pieces,
        *[v(n, 8, W, dtype=F32) for n in (16, 4, 16, 4)],
    ]
    shapes = [
        sds((SEQ, W), BF16), sds((SEQ, W), BF16), sds((SEQ, W), BF16), sds((SEQ, W), BF16),
        sds((3, 16, W), F32), sds((16, W), F32), sds((16, 1024), F32), sds((1, 1024), F32),
        sds((16, 1024), F32), sds((1, W), F32), sds((1, W), F32),
    ]
    outs = pl.pallas_call(
        kernel,
        out_shape=[pltpu.VMEM(o.shape, o.dtype) for o in shapes],
        in_specs=[hbm] * 11,
        out_specs=[vmem] * 11,
        scratch_shapes=scratch,
        compiler_params=pltpu.CompilerParams(
            collective_id=0, has_side_effects=True, vmem_limit_bytes=56 * 1024 * 1024
        ),
        name="block_pair",
    )(
        out_first[0], out_second[0], grad_first[0], grad_second[0],
        gain_attn.reshape(1, -1), gain_mlp.reshape(1, -1),
        jnp.swapaxes(qkv_weight, 0, 1), proj_weight, inner_weight, inner_bias.reshape(1, -1), outer_weight,
    )
    outs = pl.pallas_call(
        hand_over,
        out_shape=shapes,
        in_specs=[vmem] * 11,
        out_specs=[vmem] * 11,
        compiler_params=pltpu.CompilerParams(vmem_limit_bytes=8 * 1024 * 1024),
        name="hand_over",
    )(*outs)
    return (
        outs[0][None], outs[1][None], outs[2][None], outs[3][None],
        jnp.swapaxes(outs[4], 0, 1), outs[5], outs[6], outs[7].reshape(-1), outs[8],
        outs[9].reshape(-1), outs[10].reshape(-1),
    )


def solution(mesh):
    split = Mesh(mesh.devices.reshape(NZ, 2, NX, 2, 2), AXES)
    rows = P(DP, None, TENSOR)
    return jax.shard_map(
        on_device,
        mesh=split,
        in_specs=(
            rows, rows, rows, rows, P(), P(),
            P(None, None, TENSOR), P(None, TENSOR), P(None, TENSOR), P(TENSOR), P(None, TENSOR),
        ),
        out_specs=(
            rows, rows, rows, rows,
            P(DP, None, TENSOR), P(DP, TENSOR), P(DP, TENSOR), P(TENSOR), P(DP, TENSOR),
            P(TENSOR), P(TENSOR),
        ),
        check_vma=False,
    )
```

```python
import functools

import jax
import jax.numpy as jnp
from jax import lax
from jax.experimental import pallas as pl
from jax.experimental.pallas import tpu as pltpu
from jax.sharding import Mesh
from jax.sharding import PartitionSpec as P

AXES = ("z", "yl", "x", "yh", "c")
DP = ("z", "yl", "x")
TENSOR = ("yh", "c")
MESH = pl.DeviceIdType.MESH
SEQ = 197
R = 208
K = 256
W = 256
NZ, NX = 8, 4
SIZE = {"z": NZ, "x": NX, "yl": 2}
EPS = 1e-06
F32 = jnp.float32
BF16 = jnp.bfloat16
GELU_A = 0.7978845608028654
GELU_B = 0.044715
SENDS, RECVS = 78, 78
KINDS = {
    "a": (("ring", "x"), ("swap", "yl"), ("spread", "z")),
    "b": (("ring", "x"), ("swap", "yl"), ("ring", "z")),
    "c": (("ring", "z"), ("swap", "yl"), ("spread", "x")),
    "d": (("ring", "x"), ("ring", "z"), ("swap", "yl")),
    "e": (("ring", "z"), ("spread", "x"), ("swap", "yl")),
    "f": (("ring", "z"), ("spread", "x", "yl")),
    "g": (("swap", "yl"), ("ring", "x"), ("spread", "z")),
}
PIECES = (
    ("O0", "outer", "a", 0, 256),
    ("O1", "outer", "b", 256, 512),
    ("O2", "outer", "c", 512, 1024),
    ("I0", "inner", "d", 0, 256),
    ("I1", "inner", "e", 256, 768),
    ("I2", "inner", "a", 768, 1024),
    ("v", "v", "a", 0, 256),
    ("proj", "proj", "f", 0, 256),
    ("q", "q", "a", 0, 256),
    ("k", "k", "g", 0, 256),
)
TICKS = {
    "ga": (),
    "swap": (),
    "inner": (
        "O0", "O2",
    ),
    "back": (
        "O1",
    ),
    "forward": (
        "I0", "I1",
    ),
    "qkv": (
        "I2", "O2",
    ),
    "probs_half": (
        "O0",
    ),
    "probs": (
        "s1",
    ),
    "grad_heads": (),
    "heads": (
        "I1", "O1",
    ),
    "heads_half": (
        "O0",
    ),
    "attn": (
        "O2", "I0", "proj",
    ),
    "pair": (
        "I2", "s1", "O1", "I1",
    ),
    "last": (
        "v", "q", "O0", "O2", "I0", "k", "proj", "O1", "v",
    ),
    "tail": (
        "I1", "I0", "s1", "I2", "q", "proj", "k", "O1", "O2", "v", "I0", "I1", "q", "k", "s2", "proj", "O1",
        "I2", "O2", "I0", "I1", "s2", "v", "O1", "I0", "proj", "q", "k",
    ),
}

def nn(a, b):
    return lax.dot_general(a, b, (((1,), (0,)), ((), ())), preferred_element_type=F32)


def nt(a, b):
    return lax.dot_general(a, b, (((1,), (1,)), ((), ())), preferred_element_type=F32)


def at_cols(ref, lo, hi):
    return ref.at[(slice(None),) * (len(ref.shape) - 1) + (slice(lo, hi),)]


def add_into(dst, src):
    lead = dst.shape[:-2]
    total = 1
    for n in lead:
        total *= n
    if total == 1:
        where = (0,) * len(lead)
        dst[where] = dst[where] + src[where]
        return

    def body(j, _):
        where = []
        rest = j
        for n in reversed(lead):
            where.append(lax.rem(rest, n))
            rest = lax.div(rest, n)
        where = tuple(reversed(where))
        dst[where] = dst[where] + src[where]
        return 0

    lax.fori_loop(0, total, body, 0)


class Phases:
    def __init__(self):
        self.scope = None

    def __call__(self, name):
        if self.scope is not None:
            self.scope.__exit__(None, None, None)
        self.scope = jax.named_scope(name) if name else None
        if name:
            self.scope.__enter__()


class Net:
    def __init__(self, send_sem, recv_sem):
        self.pos = {a: lax.axis_index(a) for a in AXES}
        self.send_sem, self.recv_sem = send_sem, recv_sem
        self.sends, self.recvs = 0, 0
        self.out = []

    def dev(self, **other):
        where = dict(self.pos)
        where.update(other)
        return tuple(where[a] for a in AXES)

    def copies(self, triples, sent, got=None):
        k, m = self.sends, self.recvs
        self.sends, self.recvs = k + 1, m + 1
        assert self.sends <= SENDS and self.recvs <= RECVS

        def describe(src, dst, target):
            return pltpu.make_async_remote_copy(
                src_ref=src,
                dst_ref=dst,
                send_sem=self.send_sem.at[k],
                recv_sem=self.recv_sem.at[m],
                device_id=target,
                device_id_type=MESH,
            )

        for triple in triples:
            describe(*triple).start()
        target = triples[0][2]
        self.out.append(describe(sent, sent, target))
        return describe(sent if got is None else got, sent if got is None else got, target)

    def copy(self, src, dst, target):
        return self.copies([(src, dst, target)], src, dst)

    def drain(self):
        for c in self.out:
            c.wait_send()


class Chain:
    def __init__(self, net, chunk, axis, size, recv):
        self.net, self.chunk, self.axis, self.size, self.recv = net, chunk, axis, size, recv
        self.pos = net.pos[axis]
        self.steps = size // 2

    def part(self, ref, way, distance):
        if distance == self.steps:
            half = ref.shape[-1] // 2
            return at_cols(ref, way * half, (way + 1) * half)
        return ref

    def owner(self, way, distance):
        return lax.rem(self.pos + (distance if way == 0 else self.size - distance), self.size)

    def send(self, step):
        distance = self.steps - step + 1
        triples = []
        for way in (0, 1):
            src = self.part(self.chunk(self.owner(way, distance)), way, distance)
            dst = self.part(self.recv.at[way, step - 1], way, distance)
            triples.append((src, dst, self.net.dev(**{self.axis: self.owner(way, 1)})))
        both = self.recv.at[0, 0] if step == 1 else self.recv.at[:, step - 1]
        self.flying = self.net.copies(triples, both)

    def tick(self, step, finish):
        self.flying.wait_recv()
        distance = self.steps - step + 1
        if step == self.steps and finish:
            mine = self.chunk(self.owner(0, 0))
            finish(mine[...].astype(F32) + self.recv[0, step - 1].astype(F32) + self.recv[1, step - 1].astype(F32))
            return
        for way in (0, 1):
            got = self.part(self.recv.at[way, step - 1], way, distance)
            mine = self.part(self.chunk(self.owner(way, distance - 1)), way, distance)
            add_into(mine, got)
        if step < self.steps:
            self.send(step + 1)


class Swap:
    def __init__(self, net, part, recv):
        self.net, self.part, self.recv = net, part, recv
        self.yl = net.pos["yl"]
        self.steps = 1

    def send(self, step):
        target = self.net.dev(yl=1 - self.yl)
        self.flying = self.net.copy(self.part((1 - self.yl,)), self.recv, target)

    def tick(self, step, finish):
        self.flying.wait_recv()
        mine = self.part((self.yl,))
        if finish:
            finish(mine[...].astype(F32) + self.recv[...].astype(F32))
        else:
            add_into(mine, self.recv)


class Spread:
    def __init__(self, net, axes, part, recv):
        self.net, self.axes, self.part, self.recv = net, axes, part, recv
        self.steps = 1

    def send(self, step):
        net, triples = self.net, []
        count = self.recv.shape[0]
        for j in range(1, count):
            there, rest = {}, j
            for axis in self.axes:
                n = SIZE[axis]
                there[axis] = lax.rem(net.pos[axis] + rest % n, n)
                rest //= n
            src = self.part(tuple(there[a] for a in self.axes))
            triples.append((src, self.recv.at[j], net.dev(**there)))
        self.flying = net.copies(triples, self.recv.at[1:count])

    def tick(self, step, finish):
        self.flying.wait_recv()
        mine = self.part(tuple(self.net.pos[a] for a in self.axes))
        total = mine[...].astype(F32)
        for j in range(1, self.recv.shape[0]):
            total = total + self.recv[j].astype(F32)
        if finish:
            finish(total)
        else:
            mine[...] = total.astype(BF16)


class Scatter:
    def __init__(self, net, stages, bufs, finish):
        buf, before, steps = bufs[0], (), []
        for k, (how, *axes) in enumerate(stages):
            part = functools.partial(lambda before, here: buf.at[before + here], before)
            if how == "ring":
                chunk = functools.partial(lambda part, o: part((o,)), part)
                stage = Chain(net, chunk, axes[0], SIZE[axes[0]], bufs[k + 1])
            elif how == "swap":
                stage = Swap(net, part, bufs[k + 1])
            else:
                stage = Spread(net, axes, part, bufs[k + 1])
            before = before + tuple(net.pos[a] for a in axes)
            steps.append(stage)
        self.todo = [functools.partial(steps[0].send, 1)]
        for k, stage in enumerate(steps):
            last = k + 1 == len(steps)
            for step in range(1, stage.steps + 1):
                turn = last and step == stage.steps
                follow = steps[k + 1] if not last and step == stage.steps else None
                self.todo.append(functools.partial(self.advance, stage, step, finish if turn else None, follow))

    def advance(self, stage, step, finish, follow):
        stage.tick(step, finish)
        if follow is not None:
            follow.send(1)

    def tick(self):
        self.todo.pop(0)()


class Everyone:
    def __init__(self, net, stages, slots, finish):
        self.net, self.slots, self.finish = net, slots, finish
        self.stages = stages
        self.todo = [functools.partial(self.turn, k) for k in range(len(stages))]

    def send(self, block, k=0):
        net, slot = self.net, self.slots[k]
        slot[0] = block
        triples = []
        for j in range(1, slot.shape[0]):
            there, rest = {}, j
            for axis in self.stages[k]:
                n = SIZE[axis]
                there[axis] = lax.rem(net.pos[axis] + rest % n, n)
                rest //= n
            triples.append((slot.at[0], slot.at[j], net.dev(**there)))
        self.flying = net.copies(triples, slot.at[1 : slot.shape[0]])

    def turn(self, k):
        self.flying.wait_recv()
        slot = self.slots[k]
        total = slot[0]
        for j in range(1, slot.shape[0]):
            total = total + slot[j]
        if k + 1 < len(self.stages):
            self.send(total, k + 1)
        else:
            self.finish(total)

    def tick(self):
        self.todo.pop(0)()


def kernel(
    of_hbm, os_hbm, gf_hbm, gs_hbm, gain_attn_hbm, gain_mlp_hbm, wq_hbm, wp_hbm, wi_hbm, bias_hbm, wo_hbm,
    o_first, o_second, o_bfirst, o_bsecond, o_qkv, o_proj, o_inner, o_bias, o_outer, o_gattn, o_gmlp,
    of_ref, os_ref, gf_ref, gs_ref, gain_attn_ref, gain_mlp_ref, wq, wp, wi, bias_ref, wo,
    load_sem, send_sem, recv_sem,
    xg, gg, xs, xb, nm, im, act, dg, gh, lhs_a, lhs_b,
    pair_a, pair_b, pair_c, pair_d, mine_a, mine_b, out_a, out_b, out_c, out_d, in_a, in_b, in_c, in_d,
    stat_a, stat_b, qs, ks, vs, hs, rows_s, probs_s, g3,
    *rest,
):
    phase = Phases()
    phase("entry")
    net = Net(send_sem, recv_sem)
    pos = net.pos
    yh, c = pos["yh"], pos["c"]
    me, sib = 2 * yh + c, 2 * yh + 1 - c
    far, diag = 2 * (1 - yh) + c, 2 * (1 - yh) + 1 - c
    d_sib, d_far, d_diag = net.dev(c=1 - c), net.dev(yh=1 - yh), net.dev(yh=1 - yh, c=1 - c)

    loads = {}
    for k, (name, src, dst) in enumerate(
        (
            ("of", of_hbm, of_ref), ("gs", gs_hbm, gs_ref), ("gm", gain_mlp_hbm, gain_mlp_ref),
            ("bias", bias_hbm, bias_ref), ("wi", wi_hbm, wi), ("wo", wo_hbm, wo), ("os", os_hbm, os_ref),
            ("gf", gf_hbm, gf_ref), ("ga", gain_attn_hbm, gain_attn_ref), ("wq", wq_hbm, wq), ("wp", wp_hbm, wp),
        )
    ):
        loads[name] = pltpu.make_async_copy(src, dst, load_sem.at[k])
        loads[name].start()

    barrier = pltpu.get_barrier_semaphore()
    others = [d_sib, d_far, d_diag]
    for dy in range(2):
        y = lax.rem(pos["yl"] + dy, 2)
        others += [net.dev(z=lax.rem(pos["z"] + k, NZ), yl=y) for k in range(1 - dy, NZ)]
        others += [net.dev(x=lax.rem(pos["x"] + k, NX), yl=y) for k in range(1, NX)]
    for other in others:
        pl.semaphore_signal(barrier, inc=1, device_id=other, device_id_type=MESH)

    zero_rows = jnp.zeros((K - R, W), BF16)
    loads["of"].wait()
    xg[me] = jnp.zeros((R, W), BF16)
    xg[me, 0:SEQ] = of_ref[...]
    loads["gs"].wait()
    gg[me, 0:R] = jnp.zeros((R, W), BF16)
    gg[me, 0:SEQ] = gs_ref[...]
    for b in range(4):
        gg[b, R:K] = zero_rows
        xb[b, R:K] = zero_rows
        for ref in (im, act, gh):
            ref[R:K, b * W : (b + 1) * W] = zero_rows
    for ref in (qs, ks, vs, hs):
        ref[R:K] = zero_rows
    pl.semaphore_wait(barrier, len(others))

    def gather_start(ref):
        own = ref.at[me, 0:R]
        return [net.copy(own, own, d_far), net.copy(own, own, d_sib)]

    def gather_forward(ref, two):
        two[0].wait_recv()
        got = ref.at[far, 0:R]
        two.append(net.copy(got, got, d_sib))

    def gather_end(two):
        two[1].wait_recv()
        two[2].wait_recv()

    def gain_of(ref, b):
        return ref[0:1, b * W : (b + 1) * W]

    def gain_at(ref, b):
        return ref[0:1, pl.ds(pl.multiple_of(b * W, W), W)]

    def rows_at(ref, q):
        return ref[pl.ds(pl.multiple_of(q * W, W), W), :]

    def normalize(block, gain_ref):
        total = jnp.zeros((R, 1), F32)
        for b in range(4):
            total = total + jnp.sum(block(b), 1, keepdims=True)
        mean = total * (1.0 / 1024)
        square = jnp.zeros((R, 1), F32)
        for b in range(4):
            centre = block(b) - mean
            nm[b] = centre
            square = square + jnp.sum(centre * centre, 1, keepdims=True)
        spread = lax.rsqrt(square * (1.0 / 1024) + EPS)
        for b in range(4):
            normed = nm[b] * spread
            nm[b] = normed
            im[0:R, b * W : (b + 1) * W] = (normed * gain_of(gain_ref, b)).astype(BF16)
        return spread

    def turn(lhs, block):
        for b in range(4):
            lhs[b * W : (b + 1) * W] = block(b).T

    lane = lax.broadcasted_iota(jnp.int32, (R, 128), 1)

    def stats_of(part, q, gain_ref, sums):
        scaled = part * gain_at(gain_ref, q)
        one = sums[0] + jnp.sum(scaled, 1, keepdims=True)
        two = sums[1] + jnp.sum(scaled * nm[q], 1, keepdims=True)
        return (one, two)

    def stats_send(sums, stat):
        both = jnp.where(lane == 0, sums[0], jnp.where(lane == 1, sums[1], 0.0))
        both = jnp.concatenate([both, jnp.zeros((K - R, 128), F32)], 0)
        stat[0] = both.T[0:8, :]
        triples = [(stat.at[0], stat.at[k + 1], d) for k, d in enumerate((d_sib, d_far, d_diag))]
        return net.copies(triples, stat.at[1:4])

    def stats_end(sent, stat):
        sent.wait_recv()
        total = (stat[0] + stat[1]) + (stat[2] + stat[3])
        wide = jnp.concatenate([total * (1.0 / 1024), jnp.zeros((120, K), F32)], 0).T
        return wide[0:R, 0:1], wide[0:R, 1:2]

    def norm_back(part_of, gain_ref, pair, mine, out, inn, stat, stop, between):
        phase("nb_parts")
        sums = (jnp.zeros((R, 1), F32), jnp.zeros((R, 1), F32))
        for slot, q in ((0, sib), (1, diag)):
            part = part_of(q)
            pair[0, slot] = part
            sums = stats_of(part, q, gain_ref, sums)
        swap = net.copy(pair.at[0], pair.at[1], d_sib)
        for slot, q in ((0, far), (1, me)):
            part = part_of(q)
            mine[slot] = part
            sums = stats_of(part, q, gain_ref, sums)
        sent = stats_send(sums, stat)
        phase("nb_swap_wait")
        swap.wait_recv()
        out[...] = (mine[0] + pair[1, 1]).astype(BF16)
        last = net.copy(out, inn, d_far)
        tick(*TICKS[stop])
        between()
        phase("nb_last_wait")
        last.wait_recv()
        first_mean, second_mean = stats_end(sent, stat)
        grad = mine[1] + pair[1, 0] + inn[...].astype(F32)
        return grad, first_mean, second_mean

    def outer_term(lhs, rhs, scatter, col):
        order, buf = scatter
        for b in range(4):
            tile = nn(lhs[b * W : (b + 1) * W], rhs).astype(BF16).reshape(2, 2, 4, 16, W)
            for z in range(2):
                for y in range(2):
                    for x in range(4):
                        at = {"z": 2 * b + z, "yl": y, "x": x}
                        where = tuple(at[a] for a in order)
                        buf[where + (slice(None), slice(col, col + W))] = tile[z, y, x]

    def writer(ref, lo, hi):
        def finish(total):
            ref[:, lo:hi] = total

        return finish

    def kind_writer(k):
        def finish(total):
            o_qkv[k] = total

        return finish

    targets = {
        "outer": lambda lo, hi: writer(o_outer, lo, hi),
        "inner": lambda lo, hi: writer(o_inner, lo, hi),
        "proj": lambda lo, hi: writer(o_proj, lo, hi),
        "q": lambda lo, hi: kind_writer(0),
        "k": lambda lo, hi: kind_writer(1),
        "v": lambda lo, hi: kind_writer(2),
    }
    scatters, at = {}, 0
    for name, what, kind, lo, hi in PIECES:
        stages = KINDS[kind]
        bufs = rest[at : at + len(stages) + 1]
        at += len(stages) + 1
        order = [a for stage in stages for a in stage[1:]]
        scatters[name] = (Scatter(net, stages, bufs, targets[what](lo, hi)), (order, bufs[0]))

    def finish_small1(total):
        for n in range(4):
            o_bias[0:1, n * W : (n + 1) * W] = total[n : n + 1]
        o_gmlp[...] = total[4:5]

    def finish_small2(total):
        o_gattn[0:1, 0:128] = total[0:1]
        o_gattn[0:1, 128:256] = total[1:2]

    small1 = Everyone(net, (("x",), ("z",), ("yl",)), rest[at : at + 3], finish_small1)
    small2 = Everyone(net, (("z", "yl"), ("x",)), rest[at + 3 : at + 5], finish_small2)

    def make(what, lhs, tile_of):
        for name, kind, first, lo, hi in PIECES:
            if kind == what:
                for col in range(lo, hi, W):
                    outer_term(lhs, tile_of(col), scatters[name][1], col - lo)
                scatters[name][0].tick()

    def tick(*names):
        for name in names:
            phase("tick_" + name)
            if name == "s1":
                small1.tick()
            elif name == "s2":
                small2.tick()
            else:
                scatters[name][0].tick()

    x_all = gather_start(xg)
    g_all = gather_start(gg)
    phase("gather_x_wait")
    gather_forward(xg, x_all)
    gather_end(x_all)
    phase("norm_mlp")
    loads["gm"].wait()
    spread_mlp = normalize(lambda b: xg[b].astype(F32), gain_mlp_ref)
    phase("hidden")
    loads["bias"].wait()
    loads["wi"].wait()
    for n in range(4):
        cols = slice(n * W, (n + 1) * W)
        u = nn(im[0:R], wi[:, cols]) + bias_ref[0:1, cols]
        square = u * u
        t = jnp.tanh(GELU_A * (u + GELU_B * (square * u)))
        half = 0.5 * (1.0 + t)
        act[0:R, cols] = (u * half).astype(BF16)
        slope = 0.5 * GELU_A * (1.0 - t * t) * (1.0 + 3.0 * GELU_B * square)
        dg[0:R, cols] = half + u * slope
        if n == 1:
            gather_forward(gg, g_all)
    phase("mlp_out")
    loads["wo"].wait()
    pair_a[0, 0] = nt(act[0:R], rows_at(wo, sib))
    pair_a[0, 1] = nt(act[0:R], rows_at(wo, diag))
    pair_mlp = net.copy(pair_a.at[0], pair_a.at[1], d_sib)
    mine_a[0] = nt(act[0:R], rows_at(wo, far))
    mine_a[1] = nt(act[0:R], rows_at(wo, me))
    phase("g_wait")
    gather_end(g_all)
    phase("turn_g")
    turn(lhs_a, lambda b: gg[b])
    phase("pair_mlp_wait")
    pair_mlp.wait_recv()
    out_a[...] = (mine_a[0] + pair_a[1, 1]).astype(BF16)
    far_mlp = net.copy(out_a, in_a, d_far)
    phase("outer_grad")
    make("outer", lhs_a, lambda col: act[:, col : col + W])

    phase("grad_active")
    bias_rows = []
    for n in range(4):
        cols = slice(n * W, (n + 1) * W)
        grad_active = nn(gg[0, 0:R], wo[0:W, cols])
        for b in range(1, 4):
            grad_active = grad_active + nn(gg[b, 0:R], wo[b * W : (b + 1) * W, cols])
        low = (grad_active * dg[0:R, cols]).astype(BF16)
        gh[0:R, cols] = low
        bias_rows.append(jnp.sum(low.astype(F32), 0, keepdims=True))
    tick(*TICKS["ga"])

    valid = lax.broadcasted_iota(jnp.int32, (SEQ, W), 0) < SEQ
    ends = {}

    def between_mlp():
        phase("turn_im")
        turn(lhs_b, lambda b: im[:, b * W : (b + 1) * W])
        phase("far_mlp_wait")
        far_mlp.wait_recv()
        phase("input_second")
        loads["os"].wait()
        mlp = mine_a[1] + pair_a[1, 0] + in_a[...].astype(F32)
        second = (os_ref[...].astype(F32) - mlp[0:SEQ]).astype(BF16)
        o_second[...] = second
        xs[me] = jnp.zeros((R, W), BF16)
        xs[me, 0:SEQ] = second
        ends["second"] = gather_start(xs)
        phase("inner_grad")
        make("inner", lhs_b, lambda col: gh[:, col : col + W])
        tick(*TICKS["inner"])

    grad, first_mean, second_mean = norm_back(
        lambda q: nt(gh[0:R], rows_at(wi, q)),
        gain_mlp_ref, pair_b, mine_b, out_b, in_b, stat_a, "swap", between_mlp,
    )
    phase("back_first")
    loads["gf"].wait()
    normed_own = nm[me]
    back = spread_mlp * (grad * gain_at(gain_mlp_ref, me) - first_mean - normed_own * second_mean)
    first = (gf_ref[...].astype(F32) + back[0:SEQ]).astype(BF16)
    o_bfirst[...] = first
    xb[me, 0:R] = jnp.zeros((R, W), BF16)
    xb[me, 0:SEQ] = first
    b_all = gather_start(xb)
    block = bias_rows + [jnp.sum(grad * normed_own, 0, keepdims=True), jnp.zeros((3, W), F32)]
    small1.send(jnp.concatenate(block, 0))
    tick(*TICKS["back"])
    phase("xs_forward")
    gather_forward(xs, ends["second"])
    tick(*TICKS["forward"])
    phase("xs_wait")
    gather_end(ends["second"])

    phase("norm_attn")
    loads["ga"].wait()
    spread_attn = normalize(lambda b: xs[b].astype(F32), gain_attn_ref)
    phase("qkv")
    loads["wq"].wait()
    for kind, ref in enumerate((qs, ks, vs)):
        ref[0:R] = nn(im[0:R], wq[kind]).astype(BF16)
    phase("turn_attn")
    turn(lhs_a, lambda b: im[:, b * W : (b + 1) * W])
    tick(*TICKS["qkv"])

    head_lane = lax.broadcasted_iota(jnp.int32, (K, W), 1) // 64
    key_ok = lax.broadcasted_iota(jnp.int32, (K, K), 1) < SEQ
    factor = 0.125

    def only(ref, h):
        return jnp.where(head_lane == h, ref[...], jnp.zeros((), BF16))

    for h in range(4):
        phase(f"probs_{h}")
        scores = jnp.where(key_ok, nt(only(qs, h), ks[...]) * factor, -1e30)
        e = jnp.exp(scores - jnp.max(scores, 1, keepdims=True))
        probs = e / jnp.sum(e, 1, keepdims=True)
        probs_s[h] = probs
        a_h = nn(probs.astype(BF16), only(vs, h))
        if h == 0:
            rows_s[0] = a_h
        else:
            rows_s[0] += a_h
        if h == 1:
            phase("xb_forward")
            gather_forward(xb, b_all)
            tick(*TICKS["probs_half"])
    tick(*TICKS["probs"])
    phase("attn_out")
    rows_low = rows_s[0].astype(BF16)
    loads["wp"].wait()
    for slot, q in ((0, sib), (1, diag)):
        pair_c[0, slot] = nt(rows_low[0:R], rows_at(wp, q))
    pair_out = net.copy(pair_c.at[0], pair_c.at[1], d_sib)
    for slot, q in ((0, far), (1, me)):
        mine_a[slot] = nt(rows_low[0:R], rows_at(wp, q))
    phase("xb_wait")
    gather_end(b_all)
    phase("grad_heads")
    heads = nn(xb[0, 0:R], wp[0:W])
    for b in range(1, 4):
        heads = heads + nn(xb[b, 0:R], wp[b * W : (b + 1) * W])
    hs[0:R] = heads.astype(BF16)
    tick(*TICKS["grad_heads"])
    phase("pair_out_wait")
    pair_out.wait_recv()
    out_c[...] = (mine_a[0] + pair_c[1, 1]).astype(BF16)
    far_out = net.copy(out_c, in_c, d_far)
    phase("proj_grad")
    turn(lhs_b, lambda b: xb[b])
    make("proj", lhs_b, lambda col: rows_low)
    tick(*TICKS["heads"])

    for h in range(4):
        phase(f"head_{h}")
        q_h, k_h, g_h = only(qs, h), only(ks, h), only(hs, h)
        probs = probs_s[h]
        grad_probs = nt(g_h, vs[...])
        row_dot = jnp.sum(grad_probs * probs, 1, keepdims=True)
        grad_scores = (probs * (grad_probs - row_dot)).astype(BF16)
        gv_h = nn(probs.astype(BF16).T, g_h)
        gq_h = nn(grad_scores, k_h)
        gk_h = nn(grad_scores.T, q_h)
        if h == 0:
            rows_s[1], rows_s[2], rows_s[3] = gq_h, gk_h, gv_h
        else:
            rows_s[1] += gq_h
            rows_s[2] += gk_h
            rows_s[3] += gv_h
        if h == 1:
            tick(*TICKS["heads_half"])
    phase("attn_grads")
    g3[0] = (rows_s[1] * factor).astype(BF16)
    g3[1] = (rows_s[2] * factor).astype(BF16)
    g3[2] = rows_s[3].astype(BF16)
    make("v", lhs_a, lambda col: g3[2])
    make("q", lhs_a, lambda col: g3[0])
    make("k", lhs_a, lambda col: g3[1])
    tick(*TICKS["attn"])

    def qkv_part(q):
        cols = pl.ds(pl.multiple_of(q * W, W), W)
        part = nt(g3[0, 0:R], wq[0, cols, :])
        part = part + nt(g3[1, 0:R], wq[1, cols, :])
        return part + nt(g3[2, 0:R], wq[2, cols, :])

    def between_attn():
        phase("far_out_wait")
        far_out.wait_recv()
        total = mine_a[1] + pair_c[1, 0] + in_c[...].astype(F32)
        o_first[...] = (of_ref[...].astype(F32) - total[0:SEQ]).astype(BF16)
        tick(*TICKS["last"])

    grad, first_mean, second_mean = norm_back(
        qkv_part, gain_attn_ref, pair_d, mine_b, out_d, in_d, stat_b, "pair", between_attn
    )
    phase("back_second")
    normed_own = nm[me]
    gain_row = jnp.sum(grad * normed_own, 0, keepdims=True)
    small2.send(
        jnp.concatenate([gain_row[:, 0:128], gain_row[:, 128:256], jnp.zeros((6, 128), F32)], 0)
    )
    back = spread_attn * (grad * gain_at(gain_attn_ref, me) - first_mean - normed_own * second_mean)
    o_bsecond[...] = (gs_ref[...].astype(F32) + back[0:SEQ]).astype(BF16)
    tick(*TICKS["tail"])
    assert not (small1.todo or small2.todo or any(one.todo for one, _ in scatters.values()))
    phase("drain")
    assert (net.sends, net.recvs) == (SENDS, RECVS), (net.sends, net.recvs)
    net.drain()
    phase(None)


def hand_over(*refs):
    half = len(refs) // 2
    for src, dst in zip(refs[:half], refs[half:]):
        dst[...] = src[...]


def on_device(
    out_first, out_second, grad_first, grad_second, gain_attn, gain_mlp,
    qkv_weight, proj_weight, inner_weight, inner_bias, outer_weight,
):
    sds = jax.ShapeDtypeStruct
    vmem = pl.BlockSpec(memory_space=pltpu.VMEM)
    hbm = pl.BlockSpec(memory_space=pltpu.HBM)

    def v(*shape, dtype=BF16):
        return pltpu.VMEM(shape, dtype)

    def piece_bufs(stages, cols):
        left = [a for stage in stages for a in stage[1:]]
        bufs = [v(*[SIZE[a] for a in left], 16, cols)]
        for how, *axes in stages:
            left = left[len(axes) :]
            shape = [SIZE[a] for a in left] + [16, cols]
            if how == "ring":
                shape = [2, SIZE[axes[0]] // 2] + shape
            elif how == "spread":
                count = 1
                for a in axes:
                    count *= SIZE[a]
                shape = [count] + shape
            bufs.append(v(*shape))
        return bufs

    pieces = []
    for _, _, kind, lo, hi in PIECES:
        pieces += piece_bufs(KINDS[kind], hi - lo)
    scratch = [
        *[v(SEQ, W) for _ in range(4)], v(1, 1024, dtype=F32), v(1, 1024, dtype=F32),
        v(3, 1024, W), v(1024, W), v(1024, 1024), v(1, 1024, dtype=F32), v(1024, 1024),
        pltpu.SemaphoreType.DMA((11,)),
        pltpu.SemaphoreType.DMA((SENDS,)), pltpu.SemaphoreType.DMA((RECVS,)),
        v(4, R, W), v(4, K, W), v(4, R, W), v(4, K, W), v(4, R, W, dtype=F32),
        v(K, 1024), v(K, 1024), v(R, 1024, dtype=F32), v(K, 1024), v(1024, K), v(1024, K),
        *[v(2, 2, R, W, dtype=F32) for _ in range(4)],
        *[v(2, R, W, dtype=F32) for _ in range(2)],
        *[v(R, W) for _ in range(8)],
        v(4, 8, K, dtype=F32), v(4, 8, K, dtype=F32),
        *[v(K, W) for _ in range(4)],
        v(4, K, W, dtype=F32), v(4, K, K, dtype=F32), v(3, K, W),
        *pieces,
        *[v(n, 8, W, dtype=F32) for n in (4, 8, 2)], *[v(n, 8, 128, dtype=F32) for n in (16, 4)],
    ]
    shapes = [
        sds((SEQ, W), BF16), sds((SEQ, W), BF16), sds((SEQ, W), BF16), sds((SEQ, W), BF16),
        sds((3, 16, W), F32), sds((16, W), F32), sds((16, 1024), F32), sds((1, 1024), F32),
        sds((16, 1024), F32), sds((1, W), F32), sds((1, W), F32),
    ]
    outs = pl.pallas_call(
        kernel,
        out_shape=[pltpu.VMEM(o.shape, o.dtype) for o in shapes],
        in_specs=[hbm] * 11,
        out_specs=[vmem] * 11,
        scratch_shapes=scratch,
        compiler_params=pltpu.CompilerParams(
            collective_id=0, has_side_effects=True, vmem_limit_bytes=56 * 1024 * 1024
        ),
        name="block_pair",
    )(
        out_first[0], out_second[0], grad_first[0], grad_second[0],
        gain_attn.reshape(1, -1), gain_mlp.reshape(1, -1),
        jnp.swapaxes(qkv_weight, 0, 1), proj_weight, inner_weight, inner_bias.reshape(1, -1), outer_weight,
    )
    outs = pl.pallas_call(
        hand_over,
        out_shape=shapes,
        in_specs=[vmem] * 11,
        out_specs=[vmem] * 11,
        compiler_params=pltpu.CompilerParams(vmem_limit_bytes=8 * 1024 * 1024),
        name="hand_over",
    )(*outs)
    return (
        outs[0][None], outs[1][None], outs[2][None], outs[3][None],
        jnp.swapaxes(outs[4], 0, 1), outs[5], outs[6], outs[7].reshape(-1), outs[8],
        outs[9].reshape(-1), outs[10].reshape(-1),
    )


def solution(mesh):
    split = Mesh(mesh.devices.reshape(NZ, 2, NX, 2, 2), AXES)
    rows = P(DP, None, TENSOR)
    return jax.shard_map(
        on_device,
        mesh=split,
        in_specs=(
            rows, rows, rows, rows, P(), P(),
            P(None, None, TENSOR), P(None, TENSOR), P(None, TENSOR), P(TENSOR), P(None, TENSOR),
        ),
        out_specs=(
            rows, rows, rows, rows,
            P(DP, None, TENSOR), P(DP, TENSOR), P(DP, TENSOR), P(TENSOR), P(DP, TENSOR),
            P(TENSOR), P(TENSOR),
        ),
        check_vma=False,
    )
```

```python
import functools

import jax
import jax.numpy as jnp
from jax import lax
from jax.experimental import pallas as pl
from jax.experimental.pallas import tpu as pltpu
from jax.sharding import Mesh
from jax.sharding import PartitionSpec as P

AXES = ("z", "yl", "x", "yh", "c")
DP = ("z", "yl", "x")
TENSOR = ("yh", "c")
MESH = pl.DeviceIdType.MESH
SEQ = 197
R = 208
K = 256
W = 256
NZ, NX = 8, 4
SIZE = {"z": NZ, "x": NX, "yl": 2}
EPS = 1e-06
F32 = jnp.float32
BF16 = jnp.bfloat16
GELU_A = 0.7978845608028654
GELU_B = 0.044715
ORDER = ("k", "q")
SENDS, RECVS = 77, 77
KINDS = {
    "a": (("ring", "x"), ("swap", "yl"), ("spread", "z")),
    "b": (("ring", "z"), ("spread", "x", "yl")),
    "c": (("ring", "x"), ("swap", "yl"), ("ring", "z")),
    "d": (("ring", "z"), ("swap", "yl"), ("spread", "x")),
    "e": (("swap", "yl"), ("ring", "x"), ("spread", "z")),
}
PIECES = (
    ("O0", "outer0", "a", 0, 256),
    ("O1", "outer", "b", 256, 768),
    ("O2", "outer", "b", 768, 1024),
    ("I0", "inner", "c", 0, 256),
    ("I1", "inner", "d", 256, 768),
    ("I2", "inner", "c", 768, 1024),
    ("v", "v", "a", 0, 256),
    ("proj", "proj", "e", 0, 256),
    ("q", "q", "a", 0, 256),
    ("k", "k", "a", 0, 256),
)
TICKS = {
    "ga": (),
    "swap": (),
    "inner": (
        "O0",
    ),
    "back": (
        "O1", "O2",
    ),
    "forward": (
        "I0", "I1", "I2",
    ),
    "qkv": (),
    "probs_half": (
        "O0",
    ),
    "probs": (
        "s1", "O1",
    ),
    "grad_heads": (),
    "heads": (),
    "value": (
        "O2", "I0",
    ),
    "heads_half": (),
    "attn": (
        "O0", "I1", "I2",
    ),
    "pair": (
        "v",
    ),
    "tail": (
        "s1", "O1", "k", "O2", "proj", "q", "I0", "I2", "v", "O0", "I1", "first", "k", "O1", "proj",
        "second", "s1", "O2", "I0", "I2", "v", "q", "k", "I1", "I0", "I2", "proj", "O1", "q", "s2", "O2",
        "I0", "I2", "I1", "v", "k", "I0", "I2", "s2", "proj", "I1", "q",
    ),
}

def nn(a, b):
    return lax.dot_general(a, b, (((1,), (0,)), ((), ())), preferred_element_type=F32)


def nt(a, b):
    return lax.dot_general(a, b, (((1,), (1,)), ((), ())), preferred_element_type=F32)


def at_cols(ref, lo, hi):
    return ref.at[(slice(None),) * (len(ref.shape) - 1) + (slice(lo, hi),)]


def add_into(dst, src):
    dst[...] = dst[...] + src[...]


class Phases:
    def __init__(self):
        self.scope = None

    def __call__(self, name):
        if self.scope is not None:
            self.scope.__exit__(None, None, None)
        self.scope = jax.named_scope(name) if name else None
        if name:
            self.scope.__enter__()


class Net:
    def __init__(self, send_sem, recv_sem):
        self.pos = {a: lax.axis_index(a) for a in AXES}
        self.send_sem, self.recv_sem = send_sem, recv_sem
        self.sends, self.recvs = 0, 0
        self.out = []

    def dev(self, **other):
        where = dict(self.pos)
        where.update(other)
        return tuple(where[a] for a in AXES)

    def copies(self, triples, sent, got=None):
        k, m = self.sends, self.recvs
        self.sends, self.recvs = k + 1, m + 1
        assert self.sends <= SENDS and self.recvs <= RECVS

        def describe(src, dst, target):
            return pltpu.make_async_remote_copy(
                src_ref=src,
                dst_ref=dst,
                send_sem=self.send_sem.at[k],
                recv_sem=self.recv_sem.at[m],
                device_id=target,
                device_id_type=MESH,
            )

        for triple in triples:
            describe(*triple).start()
        target = triples[0][2]
        self.out.append(describe(sent, sent, target))
        return describe(sent if got is None else got, sent if got is None else got, target)

    def copy(self, src, dst, target):
        return self.copies([(src, dst, target)], src, dst)

    def drain(self):
        for c in self.out:
            c.wait_send()


class Chain:
    def __init__(self, net, chunk, axis, size, recv):
        self.net, self.chunk, self.axis, self.size, self.recv = net, chunk, axis, size, recv
        self.pos = net.pos[axis]
        self.steps = size // 2

    def part(self, ref, way, distance):
        if distance == self.steps:
            half = ref.shape[-1] // 2
            return at_cols(ref, way * half, (way + 1) * half)
        return ref

    def owner(self, way, distance):
        return lax.rem(self.pos + (distance if way == 0 else self.size - distance), self.size)

    def send(self, step):
        distance = self.steps - step + 1
        triples = []
        for way in (0, 1):
            src = self.part(self.chunk(self.owner(way, distance)), way, distance)
            dst = self.part(self.recv.at[way, step - 1], way, distance)
            triples.append((src, dst, self.net.dev(**{self.axis: self.owner(way, 1)})))
        both = self.recv.at[0, 0] if step == 1 else self.recv.at[:, step - 1]
        self.flying = self.net.copies(triples, both)

    def tick(self, step, finish):
        self.flying.wait_recv()
        distance = self.steps - step + 1
        if step == self.steps and finish:
            mine = self.chunk(self.owner(0, 0))
            finish(mine[...].astype(F32) + self.recv[0, step - 1].astype(F32) + self.recv[1, step - 1].astype(F32))
            return
        for way in (0, 1):
            got = self.part(self.recv.at[way, step - 1], way, distance)
            mine = self.part(self.chunk(self.owner(way, distance - 1)), way, distance)
            add_into(mine, got)
        if step < self.steps:
            self.send(step + 1)


class Swap:
    def __init__(self, net, part, recv):
        self.net, self.part, self.recv = net, part, recv
        self.yl = net.pos["yl"]
        self.steps = 1

    def send(self, step):
        target = self.net.dev(yl=1 - self.yl)
        self.flying = self.net.copy(self.part((1 - self.yl,)), self.recv, target)

    def tick(self, step, finish):
        self.flying.wait_recv()
        mine = self.part((self.yl,))
        if finish:
            finish(mine[...].astype(F32) + self.recv[...].astype(F32))
        else:
            add_into(mine, self.recv)


class Spread:
    def __init__(self, net, axes, part, recv):
        self.net, self.axes, self.part, self.recv = net, axes, part, recv
        self.steps = 1

    def send(self, step):
        net, triples = self.net, []
        count = self.recv.shape[0]
        for j in range(1, count):
            there, rest = {}, j
            for axis in self.axes:
                n = SIZE[axis]
                there[axis] = lax.rem(net.pos[axis] + rest % n, n)
                rest //= n
            src = self.part(tuple(there[a] for a in self.axes))
            triples.append((src, self.recv.at[j], net.dev(**there)))
        self.flying = net.copies(triples, self.recv.at[1:count])

    def tick(self, step, finish):
        self.flying.wait_recv()
        mine = self.part(tuple(self.net.pos[a] for a in self.axes))
        total = mine[...].astype(F32)
        for j in range(1, self.recv.shape[0]):
            total = total + self.recv[j].astype(F32)
        if finish:
            finish(total)
        else:
            mine[...] = total.astype(BF16)


class Scatter:
    def __init__(self, net, stages, bufs, finish):
        buf, before, steps = bufs[0], (), []
        for k, (how, *axes) in enumerate(stages):
            part = functools.partial(lambda before, here: buf.at[before + here], before)
            if how == "ring":
                chunk = functools.partial(lambda part, o: part((o,)), part)
                stage = Chain(net, chunk, axes[0], SIZE[axes[0]], bufs[k + 1])
            elif how == "swap":
                stage = Swap(net, part, bufs[k + 1])
            else:
                stage = Spread(net, axes, part, bufs[k + 1])
            before = before + tuple(net.pos[a] for a in axes)
            steps.append(stage)
        self.todo = [functools.partial(steps[0].send, 1)]
        for k, stage in enumerate(steps):
            last = k + 1 == len(steps)
            for step in range(1, stage.steps + 1):
                turn = last and step == stage.steps
                follow = steps[k + 1] if not last and step == stage.steps else None
                self.todo.append(functools.partial(self.advance, stage, step, finish if turn else None, follow))

    def advance(self, stage, step, finish, follow):
        stage.tick(step, finish)
        if follow is not None:
            follow.send(1)

    def tick(self):
        self.todo.pop(0)()


class Everyone:
    def __init__(self, net, stages, slots, finish):
        self.net, self.slots, self.finish = net, slots, finish
        self.stages = stages
        self.todo = [functools.partial(self.turn, k) for k in range(len(stages))]

    def send(self, block, k=0):
        net, slot = self.net, self.slots[k]
        slot[0] = block
        triples = []
        for j in range(1, slot.shape[0]):
            there, rest = {}, j
            for axis in self.stages[k]:
                n = SIZE[axis]
                there[axis] = lax.rem(net.pos[axis] + rest % n, n)
                rest //= n
            triples.append((slot.at[0], slot.at[j], net.dev(**there)))
        self.flying = net.copies(triples, slot.at[1 : slot.shape[0]])

    def turn(self, k):
        self.flying.wait_recv()
        slot = self.slots[k]
        total = slot[0]
        for j in range(1, slot.shape[0]):
            total = total + slot[j]
        if k + 1 < len(self.stages):
            self.send(total, k + 1)
        else:
            self.finish(total)

    def tick(self):
        self.todo.pop(0)()


def kernel(
    of_hbm, os_hbm, gf_hbm, gs_hbm, gain_attn_hbm, gain_mlp_hbm, wq_hbm, wp_hbm, wi_hbm, bias_hbm, wo_hbm,
    o_first, o_second, o_bfirst, o_bsecond, o_qkv, o_proj, o_inner, o_bias, o_outer, o_gattn, o_gmlp,
    of_ref, os_ref, gf_ref, gs_ref, gain_attn_ref, gain_mlp_ref, wq, wp, wi, bias_ref, wo,
    load_sem, send_sem, recv_sem,
    xg, gg, xs, xb, nm, im, act, us, dg, gh, lhs_a, lhs_b,
    pair_a, pair_b, pair_c, pair_d, mine_a, mine_b, out_a, out_b, out_c, out_d, in_a, in_b, in_c, in_d,
    stat_a, stat_b, qs, ks, vs, hs, rows_s, probs_s, g3,
    *rest,
):
    phase = Phases()
    phase("entry")
    net = Net(send_sem, recv_sem)
    pos = net.pos
    yh, c = pos["yh"], pos["c"]
    me, sib = 2 * yh + c, 2 * yh + 1 - c
    far, diag = 2 * (1 - yh) + c, 2 * (1 - yh) + 1 - c
    d_sib, d_far, d_diag = net.dev(c=1 - c), net.dev(yh=1 - yh), net.dev(yh=1 - yh, c=1 - c)

    loads = {}
    for k, (name, src, dst) in enumerate(
        (
            ("of", of_hbm, of_ref), ("gs", gs_hbm, gs_ref), ("gm", gain_mlp_hbm, gain_mlp_ref),
            ("bias", bias_hbm, bias_ref), ("wi", wi_hbm, wi), ("wo", wo_hbm, wo), ("os", os_hbm, os_ref),
            ("gf", gf_hbm, gf_ref), ("ga", gain_attn_hbm, gain_attn_ref), ("wq", wq_hbm, wq), ("wp", wp_hbm, wp),
        )
    ):
        loads[name] = pltpu.make_async_copy(src, dst, load_sem.at[k])
        loads[name].start()

    barrier = pltpu.get_barrier_semaphore()
    others = [d_sib, d_far, d_diag]
    for dy in range(2):
        y = lax.rem(pos["yl"] + dy, 2)
        others += [net.dev(z=lax.rem(pos["z"] + k, NZ), yl=y) for k in range(1 - dy, NZ)]
        others += [net.dev(x=lax.rem(pos["x"] + k, NX), yl=y) for k in range(1, NX)]
    for other in others:
        pl.semaphore_signal(barrier, inc=1, device_id=other, device_id_type=MESH)

    zero_rows = jnp.zeros((K - R, W), BF16)
    loads["of"].wait()
    xg[me] = jnp.zeros((R, W), BF16)
    xg[me, 0:SEQ] = of_ref[...]
    loads["gs"].wait()
    gg[me, 0:R] = jnp.zeros((R, W), BF16)
    gg[me, 0:SEQ] = gs_ref[...]
    for b in range(4):
        gg[b, R:K] = zero_rows
        xb[b, R:K] = zero_rows
        for ref in (im, act, gh):
            ref[R:K, b * W : (b + 1) * W] = zero_rows
    for ref in (qs, ks, vs, hs):
        ref[R:K] = zero_rows
    pl.semaphore_wait(barrier, len(others))

    def gather_start(ref):
        own = ref.at[me, 0:R]
        return [net.copy(own, own, d_far), net.copy(own, own, d_sib)]

    def gather_forward(ref, two):
        two[0].wait_recv()
        got = ref.at[far, 0:R]
        two.append(net.copy(got, got, d_sib))

    def gather_end(two):
        two[1].wait_recv()
        two[2].wait_recv()

    def gain_of(ref, b):
        return ref[0:1, b * W : (b + 1) * W]

    def gain_at(ref, b):
        return ref[0:1, pl.ds(pl.multiple_of(b * W, W), W)]

    def rows_at(ref, q):
        return ref[pl.ds(pl.multiple_of(q * W, W), W), :]

    def normalize(block, gain_ref):
        total = jnp.zeros((R, 1), F32)
        for b in range(4):
            total = total + jnp.sum(block(b), 1, keepdims=True)
        mean = total * (1.0 / 1024)
        square = jnp.zeros((R, 1), F32)
        for b in range(4):
            centre = block(b) - mean
            nm[b] = centre
            square = square + jnp.sum(centre * centre, 1, keepdims=True)
        spread = lax.rsqrt(square * (1.0 / 1024) + EPS)
        for b in range(4):
            normed = nm[b] * spread
            nm[b] = normed
            im[0:R, b * W : (b + 1) * W] = (normed * gain_of(gain_ref, b)).astype(BF16)
        return spread

    def turn(lhs, block):
        for b in range(4):
            lhs[b * W : (b + 1) * W] = block(b).T

    lane = lax.broadcasted_iota(jnp.int32, (R, 128), 1)

    def stats_of(part, q, gain_ref, sums):
        scaled = part * gain_at(gain_ref, q)
        one = sums[0] + jnp.sum(scaled, 1, keepdims=True)
        two = sums[1] + jnp.sum(scaled * nm[q], 1, keepdims=True)
        return (one, two)

    def stats_send(sums, stat):
        both = jnp.where(lane == 0, sums[0], jnp.where(lane == 1, sums[1], 0.0))
        both = jnp.concatenate([both, jnp.zeros((K - R, 128), F32)], 0)
        stat[0] = both.T[0:8, :]
        triples = [(stat.at[0], stat.at[k + 1], d) for k, d in enumerate((d_sib, d_far, d_diag))]
        return net.copies(triples, stat.at[1:4])

    def stats_end(sent, stat):
        sent.wait_recv()
        total = (stat[0] + stat[1]) + (stat[2] + stat[3])
        wide = jnp.concatenate([total * (1.0 / 1024), jnp.zeros((120, K), F32)], 0).T
        return wide[0:R, 0:1], wide[0:R, 1:2]

    def norm_back(part_of, gain_ref, pair, mine, out, inn, stat, stop, early):
        phase("nb_parts")
        sums = (jnp.zeros((R, 1), F32), jnp.zeros((R, 1), F32))
        for slot, q in ((0, sib), (1, diag)):
            part = part_of(q)
            pair[0, slot] = part
            sums = stats_of(part, q, gain_ref, sums)
        swap = net.copy(pair.at[0], pair.at[1], d_sib)
        for slot, q in ((0, far), (1, me)):
            part = part_of(q)
            mine[slot] = part
            sums = stats_of(part, q, gain_ref, sums)
        sent = stats_send(sums, stat)
        early()
        phase("nb_swap_wait")
        swap.wait_recv()
        out[...] = (mine[0] + pair[1, 1]).astype(BF16)
        last = net.copy(out, inn, d_far)
        tick(*TICKS[stop])

        def end():
            phase("nb_last_wait")
            last.wait_recv()
            first_mean, second_mean = stats_end(sent, stat)
            grad = mine[1] + pair[1, 0] + inn[...].astype(F32)
            return grad, first_mean, second_mean

        return end

    def outer_term(lhs, rhs, scatter, col):
        order, buf = scatter
        for b in range(4):
            tile = nn(lhs[b * W : (b + 1) * W], rhs).astype(BF16).reshape(2, 2, 4, 16, W)
            for z in range(2):
                for y in range(2):
                    for x in range(4):
                        at = {"z": 2 * b + z, "yl": y, "x": x}
                        where = tuple(at[a] for a in order)
                        buf[where + (slice(None), slice(col, col + W))] = tile[z, y, x]

    def writer(ref, lo, hi):
        def finish(total):
            ref[:, lo:hi] = total

        return finish

    def kind_writer(k):
        def finish(total):
            o_qkv[k] = total

        return finish

    targets = {
        "outer": lambda lo, hi: writer(o_outer, lo, hi),
        "outer0": lambda lo, hi: writer(o_outer, lo, hi),
        "inner": lambda lo, hi: writer(o_inner, lo, hi),
        "proj": lambda lo, hi: writer(o_proj, lo, hi),
        "q": lambda lo, hi: kind_writer(0),
        "k": lambda lo, hi: kind_writer(1),
        "v": lambda lo, hi: kind_writer(2),
    }
    scatters, at = {}, 0
    for name, what, kind, lo, hi in PIECES:
        stages = KINDS[kind]
        bufs = rest[at : at + len(stages) + 1]
        at += len(stages) + 1
        order = [a for stage in stages for a in stage[1:]]
        scatters[name] = (Scatter(net, stages, bufs, targets[what](lo, hi)), (order, bufs[0]))

    def finish_small1(total):
        for n in range(4):
            o_bias[0:1, n * W : (n + 1) * W] = total[n : n + 1]
        o_gmlp[...] = total[4:5]

    def finish_small2(total):
        o_gattn[0:1, 0:128] = total[0:1]
        o_gattn[0:1, 128:256] = total[1:2]

    small1 = Everyone(net, (("x",), ("z",), ("yl",)), rest[at : at + 3], finish_small1)
    small2 = Everyone(net, (("z",), ("x", "yl")), rest[at + 3 : at + 5], finish_small2)

    def make(what, lhs, tile_of):
        for name, kind, first, lo, hi in PIECES:
            if kind == what:
                for col in range(lo, hi, W):
                    outer_term(lhs, tile_of(col), scatters[name][1], col - lo)
                scatters[name][0].tick()

    def tick(*names):
        for name in names:
            phase("tick_" + name)
            if name == "s1":
                small1.tick()
            elif name == "s2":
                small2.tick()
            else:
                scatters[name][0].tick()

    x_all = gather_start(xg)
    g_all = gather_start(gg)
    phase("gather_x_wait")
    gather_forward(xg, x_all)
    gather_end(x_all)
    phase("norm_mlp")
    loads["gm"].wait()
    spread_mlp = normalize(lambda b: xg[b].astype(F32), gain_mlp_ref)
    phase("hidden")
    loads["bias"].wait()
    loads["wi"].wait()
    for n in range(4):
        cols = slice(n * W, (n + 1) * W)
        u = nn(im[0:R], wi[:, cols]) + bias_ref[0:1, cols]
        square = u * u
        t = jnp.tanh(GELU_A * (u + GELU_B * (square * u)))
        half = 0.5 * (1.0 + t)
        act[0:R, cols] = (u * half).astype(BF16)
        us[:, cols] = u
        dg[:, cols] = half
        if n == 1:
            gather_forward(gg, g_all)
    phase("mlp_out")
    loads["wo"].wait()
    pair_a[0, 0] = nt(act[0:R], rows_at(wo, sib))
    pair_a[0, 1] = nt(act[0:R], rows_at(wo, diag))
    pair_mlp = net.copy(pair_a.at[0], pair_a.at[1], d_sib)
    mine_a[0] = nt(act[0:R], rows_at(wo, far))
    mine_a[1] = nt(act[0:R], rows_at(wo, me))
    phase("g_wait")
    gather_end(g_all)
    phase("slope")
    for n in range(4):
        cols = slice(n * W, (n + 1) * W)
        u, half = us[:, cols], dg[:, cols]
        t = 2.0 * half - 1.0
        slope = 0.5 * GELU_A * (1.0 - t * t) * (1.0 + 3.0 * GELU_B * (u * u))
        dg[:, cols] = half + u * slope
    turn(lhs_a, lambda b: gg[b])
    phase("pair_mlp_wait")
    pair_mlp.wait_recv()
    out_a[...] = (mine_a[0] + pair_a[1, 1]).astype(BF16)
    far_mlp = net.copy(out_a, in_a, d_far)
    phase("outer_first")
    make("outer0", lhs_a, lambda col: act[:, col : col + W])

    def outer_grad():
        phase("outer_grad")
        make("outer", lhs_a, lambda col: act[:, col : col + W])

    phase("grad_active")
    bias_rows = []
    for n in range(4):
        cols = slice(n * W, (n + 1) * W)
        grad_active = nn(gg[0, 0:R], wo[0:W, cols])
        for b in range(1, 4):
            grad_active = grad_active + nn(gg[b, 0:R], wo[b * W : (b + 1) * W, cols])
        low = (grad_active * dg[0:R, cols]).astype(BF16)
        gh[0:R, cols] = low
        bias_rows.append(jnp.sum(low.astype(F32), 0, keepdims=True))
    tick(*TICKS["ga"])

    valid = lax.broadcasted_iota(jnp.int32, (SEQ, W), 0) < SEQ
    ends = {}

    def between_mlp():
        phase("turn_im")
        turn(lhs_b, lambda b: im[:, b * W : (b + 1) * W])
        phase("inner_grad")
        make("inner", lhs_b, lambda col: gh[:, col : col + W])
        phase("far_mlp_wait")
        far_mlp.wait_recv()
        phase("input_second")
        loads["os"].wait()
        mlp = mine_a[1] + pair_a[1, 0] + in_a[...].astype(F32)
        second = (os_ref[...].astype(F32) - mlp[0:SEQ]).astype(BF16)
        o_second[...] = second
        xs[me] = jnp.zeros((R, W), BF16)
        xs[me, 0:SEQ] = second
        ends["second"] = gather_start(xs)
        tick(*TICKS["inner"])

    end_mlp = norm_back(
        lambda q: nt(gh[0:R], rows_at(wi, q)),
        gain_mlp_ref, pair_b, mine_b, out_b, in_b, stat_a, "swap", outer_grad,
    )
    between_mlp()
    grad, first_mean, second_mean = end_mlp()
    phase("back_first")
    loads["gf"].wait()
    normed_own = nm[me]
    back = spread_mlp * (grad * gain_at(gain_mlp_ref, me) - first_mean - normed_own * second_mean)
    first = (gf_ref[...].astype(F32) + back[0:SEQ]).astype(BF16)
    o_bfirst[...] = first
    xb[me, 0:R] = jnp.zeros((R, W), BF16)
    xb[me, 0:SEQ] = first
    b_all = gather_start(xb)
    block = bias_rows + [jnp.sum(grad * normed_own, 0, keepdims=True), jnp.zeros((3, W), F32)]
    small1.send(jnp.concatenate(block, 0))
    tick(*TICKS["back"])
    phase("xs_forward")
    gather_forward(xs, ends["second"])
    tick(*TICKS["forward"])
    phase("xs_wait")
    gather_end(ends["second"])

    phase("norm_attn")
    loads["ga"].wait()
    spread_attn = normalize(lambda b: xs[b].astype(F32), gain_attn_ref)
    phase("qkv")
    loads["wq"].wait()
    for kind, ref in enumerate((qs, ks, vs)):
        ref[0:R] = nn(im[0:R], wq[kind]).astype(BF16)
    phase("turn_attn")
    turn(lhs_a, lambda b: im[:, b * W : (b + 1) * W])
    tick(*TICKS["qkv"])

    head_lane = lax.broadcasted_iota(jnp.int32, (K, W), 1) // 64
    key_ok = lax.broadcasted_iota(jnp.int32, (K, K), 1) < SEQ
    factor = 0.125

    def only(ref, h):
        return jnp.where(head_lane == h, ref[...], jnp.zeros((), BF16))

    for h in range(4):
        phase(f"probs_{h}")
        scores = jnp.where(key_ok, nt(only(qs, h), ks[...]) * factor, -1e30)
        e = jnp.exp(scores - jnp.max(scores, 1, keepdims=True))
        probs = e / jnp.sum(e, 1, keepdims=True)
        probs_s[h] = probs
        a_h = nn(probs.astype(BF16), only(vs, h))
        if h == 0:
            rows_s[0] = a_h
        else:
            rows_s[0] += a_h
        if h == 1:
            phase("xb_forward")
            gather_forward(xb, b_all)
            tick(*TICKS["probs_half"])
    tick(*TICKS["probs"])
    rows_low = rows_s[0].astype(BF16)
    phase("xb_wait")
    gather_end(b_all)
    phase("grad_heads")
    loads["wp"].wait()
    heads = nn(xb[0, 0:R], wp[0:W])
    for b in range(1, 4):
        heads = heads + nn(xb[b, 0:R], wp[b * W : (b + 1) * W])
    hs[0:R] = heads.astype(BF16)
    tick(*TICKS["grad_heads"])
    phase("proj_grad")
    turn(lhs_b, lambda b: xb[b])
    make("proj", lhs_b, lambda col: rows_low)
    tick(*TICKS["heads"])

    for h in range(4):
        phase(f"value_{h}")
        gv_h = nn(probs_s[h].astype(BF16).T, only(hs, h))
        if h == 0:
            rows_s[3] = gv_h
        else:
            rows_s[3] += gv_h
    phase("v_grad")
    g3[2] = rows_s[3].astype(BF16)
    make("v", lhs_a, lambda col: g3[2])
    tick(*TICKS["value"])
    for h in range(4):
        phase(f"head_{h}")
        q_h, k_h, g_h = only(qs, h), only(ks, h), only(hs, h)
        probs = probs_s[h]
        grad_probs = nt(g_h, vs[...])
        row_dot = jnp.sum(grad_probs * probs, 1, keepdims=True)
        grad_scores = (probs * (grad_probs - row_dot)).astype(BF16)
        gq_h = nn(grad_scores, k_h)
        gk_h = nn(grad_scores.T, q_h)
        if h == 0:
            rows_s[1], rows_s[2] = gq_h, gk_h
        else:
            rows_s[1] += gq_h
            rows_s[2] += gk_h
        if h == 1:
            tick(*TICKS["heads_half"])
    phase("attn_grads")
    g3[0] = (rows_s[1] * factor).astype(BF16)
    g3[1] = (rows_s[2] * factor).astype(BF16)
    for name in ORDER:
        make(name, lhs_a, lambda col: g3["qkv".index(name)])
    phase("attn_out")
    for slot, q in ((0, sib), (1, diag)):
        pair_c[0, slot] = nt(rows_low[0:R], rows_at(wp, q))
    pair_out = net.copy(pair_c.at[0], pair_c.at[1], d_sib)
    for slot, q in ((0, far), (1, me)):
        mine_a[slot] = nt(rows_low[0:R], rows_at(wp, q))
    tick(*TICKS["attn"])

    def qkv_part(q):
        cols = pl.ds(pl.multiple_of(q * W, W), W)
        part = nt(g3[0, 0:R], wq[0, cols, :])
        part = part + nt(g3[1, 0:R], wq[1, cols, :])
        return part + nt(g3[2, 0:R], wq[2, cols, :])

    sent = {}

    def attn_far():
        phase("pair_out_wait")
        pair_out.wait_recv()
        out_c[...] = (mine_a[0] + pair_c[1, 1]).astype(BF16)
        sent["out"] = net.copy(out_c, in_c, d_far)

    end_attn = norm_back(
        qkv_part, gain_attn_ref, pair_d, mine_b, out_d, in_d, stat_b, "pair", attn_far
    )

    def end_first():
        phase("far_out_wait")
        sent["out"].wait_recv()
        total = mine_a[1] + pair_c[1, 0] + in_c[...].astype(F32)
        o_first[...] = (of_ref[...].astype(F32) - total[0:SEQ]).astype(BF16)

    def end_second():
        grad, first_mean, second_mean = end_attn()
        phase("back_second")
        normed_own = nm[me]
        gain_row = jnp.sum(grad * normed_own, 0, keepdims=True)
        small2.send(
            jnp.concatenate([gain_row[:, 0:128], gain_row[:, 128:256], jnp.zeros((6, 128), F32)], 0)
        )
        back = spread_attn * (grad * gain_at(gain_attn_ref, me) - first_mean - normed_own * second_mean)
        o_bsecond[...] = (gs_ref[...].astype(F32) + back[0:SEQ]).astype(BF16)

    for name in TICKS["tail"]:
        if name == "first":
            end_first()
        elif name == "second":
            end_second()
        else:
            tick(name)
    assert not (small1.todo or small2.todo or any(one.todo for one, _ in scatters.values()))
    phase("drain")
    assert (net.sends, net.recvs) == (SENDS, RECVS), (net.sends, net.recvs)
    net.drain()
    phase(None)


def hand_over(*refs):
    half = len(refs) // 2
    for src, dst in zip(refs[:half], refs[half:]):
        dst[...] = src[...]


def on_device(
    out_first, out_second, grad_first, grad_second, gain_attn, gain_mlp,
    qkv_weight, proj_weight, inner_weight, inner_bias, outer_weight,
):
    sds = jax.ShapeDtypeStruct
    vmem = pl.BlockSpec(memory_space=pltpu.VMEM)
    hbm = pl.BlockSpec(memory_space=pltpu.HBM)

    def v(*shape, dtype=BF16):
        return pltpu.VMEM(shape, dtype)

    def piece_bufs(stages, cols):
        left = [a for stage in stages for a in stage[1:]]
        bufs = [v(*[SIZE[a] for a in left], 16, cols)]
        for how, *axes in stages:
            left = left[len(axes) :]
            shape = [SIZE[a] for a in left] + [16, cols]
            if how == "ring":
                shape = [2, SIZE[axes[0]] // 2] + shape
            elif how == "spread":
                count = 1
                for a in axes:
                    count *= SIZE[a]
                shape = [count] + shape
            bufs.append(v(*shape))
        return bufs

    pieces = []
    for _, _, kind, lo, hi in PIECES:
        pieces += piece_bufs(KINDS[kind], hi - lo)
    scratch = [
        *[v(SEQ, W) for _ in range(4)], v(1, 1024, dtype=F32), v(1, 1024, dtype=F32),
        v(3, 1024, W), v(1024, W), v(1024, 1024), v(1, 1024, dtype=F32), v(1024, 1024),
        pltpu.SemaphoreType.DMA((11,)),
        pltpu.SemaphoreType.DMA((SENDS,)), pltpu.SemaphoreType.DMA((RECVS,)),
        v(4, R, W), v(4, K, W), v(4, R, W), v(4, K, W), v(4, R, W, dtype=F32),
        v(K, 1024), v(K, 1024), v(R, 1024, dtype=F32), v(R, 1024, dtype=F32), v(K, 1024), v(1024, K), v(1024, K),
        *[v(2, 2, R, W, dtype=F32) for _ in range(4)],
        *[v(2, R, W, dtype=F32) for _ in range(2)],
        *[v(R, W) for _ in range(8)],
        v(4, 8, K, dtype=F32), v(4, 8, K, dtype=F32),
        *[v(K, W) for _ in range(4)],
        v(4, K, W, dtype=F32), v(4, K, K, dtype=F32), v(3, K, W),
        *pieces,
        *[v(n, 8, W, dtype=F32) for n in (4, 8, 2)], *[v(n, 8, 128, dtype=F32) for n in (8, 8)],
    ]
    shapes = [
        sds((SEQ, W), BF16), sds((SEQ, W), BF16), sds((SEQ, W), BF16), sds((SEQ, W), BF16),
        sds((3, 16, W), F32), sds((16, W), F32), sds((16, 1024), F32), sds((1, 1024), F32),
        sds((16, 1024), F32), sds((1, W), F32), sds((1, W), F32),
    ]
    outs = pl.pallas_call(
        kernel,
        out_shape=[pltpu.VMEM(o.shape, o.dtype) for o in shapes],
        in_specs=[hbm] * 11,
        out_specs=[vmem] * 11,
        scratch_shapes=scratch,
        compiler_params=pltpu.CompilerParams(
            collective_id=0, has_side_effects=True, vmem_limit_bytes=56 * 1024 * 1024
        ),
        name="block_pair",
    )(
        out_first[0], out_second[0], grad_first[0], grad_second[0],
        gain_attn.reshape(1, -1), gain_mlp.reshape(1, -1),
        jnp.swapaxes(qkv_weight, 0, 1), proj_weight, inner_weight, inner_bias.reshape(1, -1), outer_weight,
    )
    outs = pl.pallas_call(
        hand_over,
        out_shape=shapes,
        in_specs=[vmem] * 11,
        out_specs=[vmem] * 11,
        compiler_params=pltpu.CompilerParams(vmem_limit_bytes=8 * 1024 * 1024),
        name="hand_over",
    )(*outs)
    return (
        outs[0][None], outs[1][None], outs[2][None], outs[3][None],
        jnp.swapaxes(outs[4], 0, 1), outs[5], outs[6], outs[7].reshape(-1), outs[8],
        outs[9].reshape(-1), outs[10].reshape(-1),
    )


def solution(mesh):
    split = Mesh(mesh.devices.reshape(NZ, 2, NX, 2, 2), AXES)
    rows = P(DP, None, TENSOR)
    return jax.shard_map(
        on_device,
        mesh=split,
        in_specs=(
            rows, rows, rows, rows, P(), P(),
            P(None, None, TENSOR), P(None, TENSOR), P(None, TENSOR), P(TENSOR), P(None, TENSOR),
        ),
        out_specs=(
            rows, rows, rows, rows,
            P(DP, None, TENSOR), P(DP, TENSOR), P(DP, TENSOR), P(TENSOR), P(DP, TENSOR),
            P(TENSOR), P(TENSOR),
        ),
        check_vma=False,
    )
```

```python
import functools

import jax
import jax.numpy as jnp
from jax import lax
from jax.experimental import pallas as pl
from jax.experimental.pallas import tpu as pltpu
from jax.sharding import Mesh
from jax.sharding import PartitionSpec as P

AXES = ("z", "yl", "x", "yh", "c")
DP = ("z", "yl", "x")
TENSOR = ("yh", "c")
MESH = pl.DeviceIdType.MESH
SEQ = 197
R = 208
K = 256
W = 256
NZ, NX = 8, 4
SIZE = {"z": NZ, "x": NX, "yl": 2}
EPS = 1e-06
F32 = jnp.float32
BF16 = jnp.bfloat16
GELU_A = 0.7978845608028654
GELU_B = 0.044715
ORDER = ("q", "k")
SENDS, RECVS = 62, 62
KINDS = {
    "a": (("ring", "x"), ("swap", "yl"), ("ring", "z")),
    "b": (("ring", "z"), ("spread", "x", "yl")),
    "c": (("spread", "x"), ("swap", "yl"), ("spread", "z")),
    "d": (("ring", "x"), ("swap", "yl"), ("spread", "z")),
    "e": (("swap", "yl"), ("spread", "x"), ("spread", "z")),
}
PIECES = (
    ("O0", "outer0", "a", 0, 512),
    ("O1", "outer", "b", 512, 1024),
    ("I0", "inner", "b", 0, 768),
    ("I1", "inner", "c", 768, 1024),
    ("v", "v", "d", 0, 256),
    ("proj", "proj", "e", 0, 256),
    ("q", "q", "d", 0, 256),
    ("k", "k", "d", 0, 256),
)
TICKS = {
    "ga": (),
    "swap": (),
    "inner": (),
    "back": (
        "O0", "O1",
    ),
    "forward": (
        "I0",
    ),
    "qkv": (),
    "probs_half": (
        "I1",
    ),
    "probs": (
        "s1", "O1",
    ),
    "grad_heads": (),
    "heads": (),
    "value": (),
    "heads_half": (),
    "attn": (
        "I1", "I0", "O0",
    ),
    "pair": (
        "v",
    ),
    "tail": (
        "s1", "O1", "q", "k", "proj", "I1", "O0", "v", "I0", "q", "first", "O1", "O0", "s1", "second", "k",
        "v", "q", "I0", "O0", "proj", "k", "s2", "O1", "O0", "v", "q", "I0", "O0", "proj", "s2", "k",
    ),
}

def nn(a, b):
    return lax.dot_general(a, b, (((1,), (0,)), ((), ())), preferred_element_type=F32)


def nt(a, b):
    return lax.dot_general(a, b, (((1,), (1,)), ((), ())), preferred_element_type=F32)


def at_cols(ref, lo, hi):
    return ref.at[(slice(None),) * (len(ref.shape) - 1) + (slice(lo, hi),)]


def add_into(dst, src):
    dst[...] = dst[...] + src[...]


class Phases:
    def __init__(self):
        self.scope = None

    def __call__(self, name):
        if self.scope is not None:
            self.scope.__exit__(None, None, None)
        self.scope = jax.named_scope(name) if name else None
        if name:
            self.scope.__enter__()


class Net:
    def __init__(self, send_sem, recv_sem):
        self.pos = {a: lax.axis_index(a) for a in AXES}
        self.send_sem, self.recv_sem = send_sem, recv_sem
        self.sends, self.recvs = 0, 0
        self.out = []

    def dev(self, **other):
        where = dict(self.pos)
        where.update(other)
        return tuple(where[a] for a in AXES)

    def copies(self, triples, sent, got=None):
        k, m = self.sends, self.recvs
        self.sends, self.recvs = k + 1, m + 1
        assert self.sends <= SENDS and self.recvs <= RECVS

        def describe(src, dst, target):
            return pltpu.make_async_remote_copy(
                src_ref=src,
                dst_ref=dst,
                send_sem=self.send_sem.at[k],
                recv_sem=self.recv_sem.at[m],
                device_id=target,
                device_id_type=MESH,
            )

        for triple in triples:
            describe(*triple).start()
        target = triples[0][2]
        self.out.append(describe(sent, sent, target))
        return describe(sent if got is None else got, sent if got is None else got, target)

    def copy(self, src, dst, target):
        return self.copies([(src, dst, target)], src, dst)

    def drain(self):
        for c in self.out:
            c.wait_send()


class Chain:
    def __init__(self, net, chunk, axis, size, recv):
        self.net, self.chunk, self.axis, self.size, self.recv = net, chunk, axis, size, recv
        self.pos = net.pos[axis]
        self.steps = size // 2

    def part(self, ref, way, distance):
        if distance == self.steps:
            half = ref.shape[-1] // 2
            return at_cols(ref, way * half, (way + 1) * half)
        return ref

    def owner(self, way, distance):
        return lax.rem(self.pos + (distance if way == 0 else self.size - distance), self.size)

    def send(self, step):
        distance = self.steps - step + 1
        triples = []
        for way in (0, 1):
            src = self.part(self.chunk(self.owner(way, distance)), way, distance)
            dst = self.part(self.recv.at[way, step - 1], way, distance)
            triples.append((src, dst, self.net.dev(**{self.axis: self.owner(way, 1)})))
        both = self.recv.at[0, 0] if step == 1 else self.recv.at[:, step - 1]
        self.flying = self.net.copies(triples, both)

    def tick(self, step, finish):
        self.flying.wait_recv()
        distance = self.steps - step + 1
        if step == self.steps and finish:
            mine = self.chunk(self.owner(0, 0))
            finish(mine[...].astype(F32) + self.recv[0, step - 1].astype(F32) + self.recv[1, step - 1].astype(F32))
            return
        for way in (0, 1):
            got = self.part(self.recv.at[way, step - 1], way, distance)
            mine = self.part(self.chunk(self.owner(way, distance - 1)), way, distance)
            add_into(mine, got)
        if step < self.steps:
            self.send(step + 1)


class Swap:
    def __init__(self, net, part, recv):
        self.net, self.part, self.recv = net, part, recv
        self.yl = net.pos["yl"]
        self.steps = 1

    def send(self, step):
        target = self.net.dev(yl=1 - self.yl)
        self.flying = self.net.copy(self.part((1 - self.yl,)), self.recv, target)

    def tick(self, step, finish):
        self.flying.wait_recv()
        mine = self.part((self.yl,))
        if finish:
            finish(mine[...].astype(F32) + self.recv[...].astype(F32))
        else:
            add_into(mine, self.recv)


class Spread:
    def __init__(self, net, axes, part, recv):
        self.net, self.axes, self.part, self.recv = net, axes, part, recv
        self.steps = 1

    def send(self, step):
        net, triples = self.net, []
        count = self.recv.shape[0]
        for j in range(1, count):
            there, rest = {}, j
            for axis in self.axes:
                n = SIZE[axis]
                there[axis] = lax.rem(net.pos[axis] + rest % n, n)
                rest //= n
            src = self.part(tuple(there[a] for a in self.axes))
            triples.append((src, self.recv.at[j], net.dev(**there)))
        self.flying = net.copies(triples, self.recv.at[1:count])

    def tick(self, step, finish):
        self.flying.wait_recv()
        mine = self.part(tuple(self.net.pos[a] for a in self.axes))
        total = mine[...].astype(F32)
        for j in range(1, self.recv.shape[0]):
            total = total + self.recv[j].astype(F32)
        if finish:
            finish(total)
        else:
            mine[...] = total.astype(BF16)


class Scatter:
    def __init__(self, net, stages, bufs, finish):
        buf, before, steps = bufs[0], (), []
        for k, (how, *axes) in enumerate(stages):
            part = functools.partial(lambda before, here: buf.at[before + here], before)
            if how == "ring":
                chunk = functools.partial(lambda part, o: part((o,)), part)
                stage = Chain(net, chunk, axes[0], SIZE[axes[0]], bufs[k + 1])
            elif how == "swap":
                stage = Swap(net, part, bufs[k + 1])
            else:
                stage = Spread(net, axes, part, bufs[k + 1])
            before = before + tuple(net.pos[a] for a in axes)
            steps.append(stage)
        self.todo = [functools.partial(steps[0].send, 1)]
        for k, stage in enumerate(steps):
            last = k + 1 == len(steps)
            for step in range(1, stage.steps + 1):
                turn = last and step == stage.steps
                follow = steps[k + 1] if not last and step == stage.steps else None
                self.todo.append(functools.partial(self.advance, stage, step, finish if turn else None, follow))

    def advance(self, stage, step, finish, follow):
        stage.tick(step, finish)
        if follow is not None:
            follow.send(1)

    def tick(self):
        self.todo.pop(0)()


class Everyone:
    def __init__(self, net, stages, slots, finish):
        self.net, self.slots, self.finish = net, slots, finish
        self.stages = stages
        self.todo = [functools.partial(self.turn, k) for k in range(len(stages))]

    def send(self, block, k=0):
        net, slot = self.net, self.slots[k]
        slot[0] = block
        triples = []
        for j in range(1, slot.shape[0]):
            there, rest = {}, j
            for axis in self.stages[k]:
                n = SIZE[axis]
                there[axis] = lax.rem(net.pos[axis] + rest % n, n)
                rest //= n
            triples.append((slot.at[0], slot.at[j], net.dev(**there)))
        self.flying = net.copies(triples, slot.at[1 : slot.shape[0]])

    def turn(self, k):
        self.flying.wait_recv()
        slot = self.slots[k]
        total = slot[0]
        for j in range(1, slot.shape[0]):
            total = total + slot[j]
        if k + 1 < len(self.stages):
            self.send(total, k + 1)
        else:
            self.finish(total)

    def tick(self):
        self.todo.pop(0)()


def kernel(
    of_hbm, os_hbm, gf_hbm, gs_hbm, gain_attn_hbm, gain_mlp_hbm, wq_hbm, wp_hbm, wi_hbm, bias_hbm, wo_hbm,
    o_first, o_second, o_bfirst, o_bsecond, o_qkv, o_proj, o_inner, o_bias, o_outer, o_gattn, o_gmlp,
    of_ref, os_ref, gf_ref, gs_ref, gain_attn_ref, gain_mlp_ref, wq, wp, wi, bias_ref, wo,
    load_sem, send_sem, recv_sem,
    xg, gg, xs, xb, nm, im, act, us, dg, gh, lhs_a, lhs_b,
    pair_a, pair_b, pair_c, pair_d, mine_a, mine_b, out_a, out_b, out_c, out_d, in_a, in_b, in_c, in_d,
    stat_a, stat_b, qs, ks, vs, hs, rows_s, probs_s, g3,
    *rest,
):
    phase = Phases()
    phase("entry")
    net = Net(send_sem, recv_sem)
    pos = net.pos
    yh, c = pos["yh"], pos["c"]
    me, sib = 2 * yh + c, 2 * yh + 1 - c
    far, diag = 2 * (1 - yh) + c, 2 * (1 - yh) + 1 - c
    d_sib, d_far, d_diag = net.dev(c=1 - c), net.dev(yh=1 - yh), net.dev(yh=1 - yh, c=1 - c)

    loads = {}
    for k, (name, src, dst) in enumerate(
        (
            ("of", of_hbm, of_ref), ("gs", gs_hbm, gs_ref), ("gm", gain_mlp_hbm, gain_mlp_ref),
            ("bias", bias_hbm, bias_ref), ("wi", wi_hbm, wi), ("wo", wo_hbm, wo), ("os", os_hbm, os_ref),
            ("gf", gf_hbm, gf_ref), ("ga", gain_attn_hbm, gain_attn_ref), ("wq", wq_hbm, wq), ("wp", wp_hbm, wp),
        )
    ):
        loads[name] = pltpu.make_async_copy(src, dst, load_sem.at[k])
        loads[name].start()

    barrier = pltpu.get_barrier_semaphore()
    others = [d_sib, d_far, d_diag]
    for dy in range(2):
        y = lax.rem(pos["yl"] + dy, 2)
        others += [net.dev(z=lax.rem(pos["z"] + k, NZ), yl=y) for k in range(1 - dy, NZ)]
        others += [net.dev(x=lax.rem(pos["x"] + k, NX), yl=y) for k in range(1, NX)]
    for other in others:
        pl.semaphore_signal(barrier, inc=1, device_id=other, device_id_type=MESH)

    zero_rows = jnp.zeros((K - R, W), BF16)
    loads["of"].wait()
    xg[me] = jnp.zeros((R, W), BF16)
    xg[me, 0:SEQ] = of_ref[...]
    pl.semaphore_wait(barrier, len(others))

    def gather_start(ref):
        own = ref.at[me, 0:R]
        return [net.copy(own, own, d_far), net.copy(own, own, d_sib)]

    def gather_forward(ref, two):
        two[0].wait_recv()
        got = ref.at[far, 0:R]
        two.append(net.copy(got, got, d_sib))

    def gather_end(two):
        two[1].wait_recv()
        two[2].wait_recv()

    def gain_of(ref, b):
        return ref[0:1, b * W : (b + 1) * W]

    def gain_at(ref, b):
        return ref[0:1, pl.ds(pl.multiple_of(b * W, W), W)]

    def rows_at(ref, q):
        return ref[pl.ds(pl.multiple_of(q * W, W), W), :]

    def normalize(block, gain_ref):
        total = jnp.zeros((R, 1), F32)
        for b in range(4):
            total = total + jnp.sum(block(b), 1, keepdims=True)
        mean = total * (1.0 / 1024)
        square = jnp.zeros((R, 1), F32)
        for b in range(4):
            centre = block(b) - mean
            nm[b] = centre
            square = square + jnp.sum(centre * centre, 1, keepdims=True)
        spread = lax.rsqrt(square * (1.0 / 1024) + EPS)
        for b in range(4):
            normed = nm[b] * spread
            nm[b] = normed
            im[0:R, b * W : (b + 1) * W] = (normed * gain_of(gain_ref, b)).astype(BF16)
        return spread

    def turn(lhs, block):
        for b in range(4):
            lhs[b * W : (b + 1) * W] = block(b).T

    lane = lax.broadcasted_iota(jnp.int32, (R, 128), 1)

    def stats_of(part, q, gain_ref, sums):
        scaled = part * gain_at(gain_ref, q)
        one = sums[0] + jnp.sum(scaled, 1, keepdims=True)
        two = sums[1] + jnp.sum(scaled * nm[q], 1, keepdims=True)
        return (one, two)

    def stats_send(sums, stat):
        both = jnp.where(lane == 0, sums[0], jnp.where(lane == 1, sums[1], 0.0))
        both = jnp.concatenate([both, jnp.zeros((K - R, 128), F32)], 0)
        stat[0] = both.T[0:8, :]
        triples = [(stat.at[0], stat.at[k + 1], d) for k, d in enumerate((d_sib, d_far, d_diag))]
        return net.copies(triples, stat.at[1:4])

    def stats_end(sent, stat):
        sent.wait_recv()
        total = (stat[0] + stat[1]) + (stat[2] + stat[3])
        wide = jnp.concatenate([total * (1.0 / 1024), jnp.zeros((120, K), F32)], 0).T
        return wide[0:R, 0:1], wide[0:R, 1:2]

    def norm_back(part_of, gain_ref, pair, mine, out, inn, stat, stop, early):
        phase("nb_parts")
        sums = (jnp.zeros((R, 1), F32), jnp.zeros((R, 1), F32))
        for slot, q in ((0, sib), (1, diag)):
            part = part_of(q)
            pair[0, slot] = part
            sums = stats_of(part, q, gain_ref, sums)
        swap = net.copy(pair.at[0], pair.at[1], d_sib)
        for slot, q in ((0, far), (1, me)):
            part = part_of(q)
            mine[slot] = part
            sums = stats_of(part, q, gain_ref, sums)
        sent = stats_send(sums, stat)
        early()
        phase("nb_swap_wait")
        swap.wait_recv()
        out[...] = (mine[0] + pair[1, 1]).astype(BF16)
        last = net.copy(out, inn, d_far)
        tick(*TICKS[stop])

        def end():
            phase("nb_last_wait")
            last.wait_recv()
            first_mean, second_mean = stats_end(sent, stat)
            grad = mine[1] + pair[1, 0] + inn[...].astype(F32)
            return grad, first_mean, second_mean

        return end

    def outer_term(lhs, rhs, scatter, col):
        order, buf = scatter
        for b in range(4):
            tile = nn(lhs[b * W : (b + 1) * W], rhs).astype(BF16).reshape(2, 2, 4, 16, W)
            for z in range(2):
                for y in range(2):
                    for x in range(4):
                        at = {"z": 2 * b + z, "yl": y, "x": x}
                        where = tuple(at[a] for a in order)
                        buf[where + (slice(None), slice(col, col + W))] = tile[z, y, x]

    def writer(ref, lo, hi):
        def finish(total):
            ref[:, lo:hi] = total

        return finish

    def kind_writer(k):
        def finish(total):
            o_qkv[k] = total

        return finish

    targets = {
        "outer": lambda lo, hi: writer(o_outer, lo, hi),
        "outer0": lambda lo, hi: writer(o_outer, lo, hi),
        "inner": lambda lo, hi: writer(o_inner, lo, hi),
        "proj": lambda lo, hi: writer(o_proj, lo, hi),
        "q": lambda lo, hi: kind_writer(0),
        "k": lambda lo, hi: kind_writer(1),
        "v": lambda lo, hi: kind_writer(2),
    }
    scatters, at = {}, 0
    for name, what, kind, lo, hi in PIECES:
        stages = KINDS[kind]
        bufs = rest[at : at + len(stages) + 1]
        at += len(stages) + 1
        order = [a for stage in stages for a in stage[1:]]
        scatters[name] = (Scatter(net, stages, bufs, targets[what](lo, hi)), (order, bufs[0]))

    def finish_small1(total):
        for n in range(4):
            o_bias[0:1, n * W : (n + 1) * W] = total[n : n + 1]
        o_gmlp[...] = total[4:5]

    def finish_small2(total):
        o_gattn[0:1, 0:128] = total[0:1]
        o_gattn[0:1, 128:256] = total[1:2]

    small1 = Everyone(net, (("x",), ("z",), ("yl",)), rest[at : at + 3], finish_small1)
    small2 = Everyone(net, (("z",), ("x", "yl")), rest[at + 3 : at + 5], finish_small2)

    def make(what, lhs, tile_of):
        for name, kind, first, lo, hi in PIECES:
            if kind == what:
                for col in range(lo, hi, W):
                    outer_term(lhs, tile_of(col), scatters[name][1], col - lo)
                scatters[name][0].tick()

    def tick(*names):
        for name in names:
            phase("tick_" + name)
            if name == "s1":
                small1.tick()
            elif name == "s2":
                small2.tick()
            else:
                scatters[name][0].tick()

    x_all = gather_start(xg)
    loads["gs"].wait()
    gg[me, 0:R] = jnp.zeros((R, W), BF16)
    gg[me, 0:SEQ] = gs_ref[...]
    g_all = gather_start(gg)
    for b in range(4):
        gg[b, R:K] = zero_rows
        xb[b, R:K] = zero_rows
        for ref in (im, act, gh):
            ref[R:K, b * W : (b + 1) * W] = zero_rows
    for ref in (qs, ks, vs, hs):
        ref[R:K] = zero_rows
    phase("gather_x_wait")
    gather_forward(xg, x_all)
    gather_end(x_all)
    phase("norm_mlp")
    loads["gm"].wait()
    spread_mlp = normalize(lambda b: xg[b].astype(F32), gain_mlp_ref)
    phase("hidden")
    loads["bias"].wait()
    loads["wi"].wait()
    for n in range(4):
        cols = slice(n * W, (n + 1) * W)
        u = nn(im[0:R], wi[:, cols]) + bias_ref[0:1, cols]
        square = u * u
        t = jnp.tanh(GELU_A * (u + GELU_B * (square * u)))
        half = 0.5 * (1.0 + t)
        act[0:R, cols] = (u * half).astype(BF16)
        us[:, cols] = u
        dg[:, cols] = half
        if n == 1:
            gather_forward(gg, g_all)
    phase("mlp_out")
    loads["wo"].wait()
    pair_a[0, 0] = nt(act[0:R], rows_at(wo, sib))
    pair_a[0, 1] = nt(act[0:R], rows_at(wo, diag))
    pair_mlp = net.copy(pair_a.at[0], pair_a.at[1], d_sib)
    mine_a[0] = nt(act[0:R], rows_at(wo, far))
    mine_a[1] = nt(act[0:R], rows_at(wo, me))
    phase("g_wait")
    gather_end(g_all)
    phase("slope")
    for n in range(4):
        cols = slice(n * W, (n + 1) * W)
        u, half = us[:, cols], dg[:, cols]
        t = 2.0 * half - 1.0
        slope = 0.5 * GELU_A * (1.0 - t * t) * (1.0 + 3.0 * GELU_B * (u * u))
        dg[:, cols] = half + u * slope
    turn(lhs_a, lambda b: gg[b])
    phase("pair_mlp_wait")
    pair_mlp.wait_recv()
    out_a[...] = (mine_a[0] + pair_a[1, 1]).astype(BF16)
    far_mlp = net.copy(out_a, in_a, d_far)
    phase("outer_first")
    make("outer0", lhs_a, lambda col: act[:, col : col + W])

    def outer_grad():
        phase("outer_grad")
        make("outer", lhs_a, lambda col: act[:, col : col + W])

    phase("grad_active")
    bias_rows = []
    for n in range(4):
        cols = slice(n * W, (n + 1) * W)
        grad_active = nn(gg[0, 0:R], wo[0:W, cols])
        for b in range(1, 4):
            grad_active = grad_active + nn(gg[b, 0:R], wo[b * W : (b + 1) * W, cols])
        low = (grad_active * dg[0:R, cols]).astype(BF16)
        gh[0:R, cols] = low
        bias_rows.append(jnp.sum(low.astype(F32), 0, keepdims=True))
    tick(*TICKS["ga"])

    valid = lax.broadcasted_iota(jnp.int32, (SEQ, W), 0) < SEQ
    ends = {}

    def between_mlp():
        phase("turn_im")
        turn(lhs_b, lambda b: im[:, b * W : (b + 1) * W])
        phase("inner_grad")
        make("inner", lhs_b, lambda col: gh[:, col : col + W])
        phase("far_mlp_wait")
        far_mlp.wait_recv()
        phase("input_second")
        loads["os"].wait()
        mlp = mine_a[1] + pair_a[1, 0] + in_a[...].astype(F32)
        second = (os_ref[...].astype(F32) - mlp[0:SEQ]).astype(BF16)
        o_second[...] = second
        xs[me] = jnp.zeros((R, W), BF16)
        xs[me, 0:SEQ] = second
        ends["second"] = gather_start(xs)
        tick(*TICKS["inner"])

    end_mlp = norm_back(
        lambda q: nt(gh[0:R], rows_at(wi, q)),
        gain_mlp_ref, pair_b, mine_b, out_b, in_b, stat_a, "swap", outer_grad,
    )
    between_mlp()
    grad, first_mean, second_mean = end_mlp()
    phase("back_first")
    loads["gf"].wait()
    normed_own = nm[me]
    back = spread_mlp * (grad * gain_at(gain_mlp_ref, me) - first_mean - normed_own * second_mean)
    first = (gf_ref[...].astype(F32) + back[0:SEQ]).astype(BF16)
    o_bfirst[...] = first
    xb[me, 0:R] = jnp.zeros((R, W), BF16)
    xb[me, 0:SEQ] = first
    b_all = gather_start(xb)
    block = bias_rows + [jnp.sum(grad * normed_own, 0, keepdims=True), jnp.zeros((3, W), F32)]
    small1.send(jnp.concatenate(block, 0))
    tick(*TICKS["back"])
    phase("xs_forward")
    gather_forward(xs, ends["second"])
    tick(*TICKS["forward"])
    phase("xs_wait")
    gather_end(ends["second"])

    phase("norm_attn")
    loads["ga"].wait()
    spread_attn = normalize(lambda b: xs[b].astype(F32), gain_attn_ref)
    phase("qkv")
    loads["wq"].wait()
    for kind, ref in enumerate((qs, ks, vs)):
        ref[0:R] = nn(im[0:R], wq[kind]).astype(BF16)
    phase("turn_attn")
    turn(lhs_a, lambda b: im[:, b * W : (b + 1) * W])
    tick(*TICKS["qkv"])

    head_lane = lax.broadcasted_iota(jnp.int32, (K, W), 1) // 64
    key_ok = lax.broadcasted_iota(jnp.int32, (K, K), 1) < SEQ
    factor = 0.125

    def only(ref, h):
        return jnp.where(head_lane == h, ref[...], jnp.zeros((), BF16))

    for h in range(4):
        phase(f"probs_{h}")
        scores = jnp.where(key_ok, nt(only(qs, h), ks[...]) * factor, -1e30)
        e = jnp.exp(scores - jnp.max(scores, 1, keepdims=True))
        probs = e / jnp.sum(e, 1, keepdims=True)
        probs_s[h] = probs
        a_h = nn(probs.astype(BF16), only(vs, h))
        if h == 0:
            rows_s[0] = a_h
        else:
            rows_s[0] += a_h
        if h == 1:
            phase("xb_forward")
            gather_forward(xb, b_all)
            tick(*TICKS["probs_half"])
    tick(*TICKS["probs"])
    rows_low = rows_s[0].astype(BF16)
    phase("xb_wait")
    gather_end(b_all)
    phase("grad_heads")
    loads["wp"].wait()
    heads = nn(xb[0, 0:R], wp[0:W])
    for b in range(1, 4):
        heads = heads + nn(xb[b, 0:R], wp[b * W : (b + 1) * W])
    hs[0:R] = heads.astype(BF16)
    tick(*TICKS["grad_heads"])
    phase("proj_grad")
    turn(lhs_b, lambda b: xb[b])
    make("proj", lhs_b, lambda col: rows_low)
    tick(*TICKS["heads"])

    for h in range(4):
        phase(f"value_{h}")
        gv_h = nn(probs_s[h].astype(BF16).T, only(hs, h))
        if h == 0:
            rows_s[3] = gv_h
        else:
            rows_s[3] += gv_h
    phase("v_grad")
    g3[2] = rows_s[3].astype(BF16)
    make("v", lhs_a, lambda col: g3[2])
    tick(*TICKS["value"])
    for h in range(4):
        phase(f"head_{h}")
        q_h, k_h, g_h = only(qs, h), only(ks, h), only(hs, h)
        probs = probs_s[h]
        grad_probs = nt(g_h, vs[...])
        row_dot = jnp.sum(grad_probs * probs, 1, keepdims=True)
        grad_scores = (probs * (grad_probs - row_dot)).astype(BF16)
        gq_h = nn(grad_scores, k_h)
        gk_h = nn(grad_scores.T, q_h)
        if h == 0:
            rows_s[1], rows_s[2] = gq_h, gk_h
        else:
            rows_s[1] += gq_h
            rows_s[2] += gk_h
        if h == 1:
            tick(*TICKS["heads_half"])
    phase("attn_grads")
    g3[0] = (rows_s[1] * factor).astype(BF16)
    g3[1] = (rows_s[2] * factor).astype(BF16)
    for name in ORDER:
        make(name, lhs_a, lambda col: g3["qkv".index(name)])
    phase("attn_out")
    for slot, q in ((0, sib), (1, diag)):
        pair_c[0, slot] = nt(rows_low[0:R], rows_at(wp, q))
    pair_out = net.copy(pair_c.at[0], pair_c.at[1], d_sib)
    for slot, q in ((0, far), (1, me)):
        mine_a[slot] = nt(rows_low[0:R], rows_at(wp, q))
    tick(*TICKS["attn"])

    def qkv_part(q):
        cols = pl.ds(pl.multiple_of(q * W, W), W)
        part = nt(g3[0, 0:R], wq[0, cols, :])
        part = part + nt(g3[1, 0:R], wq[1, cols, :])
        return part + nt(g3[2, 0:R], wq[2, cols, :])

    sent = {}

    def attn_far():
        phase("pair_out_wait")
        pair_out.wait_recv()
        out_c[...] = (mine_a[0] + pair_c[1, 1]).astype(BF16)
        sent["out"] = net.copy(out_c, in_c, d_far)

    end_attn = norm_back(
        qkv_part, gain_attn_ref, pair_d, mine_b, out_d, in_d, stat_b, "pair", attn_far
    )

    def end_first():
        phase("far_out_wait")
        sent["out"].wait_recv()
        total = mine_a[1] + pair_c[1, 0] + in_c[...].astype(F32)
        o_first[...] = (of_ref[...].astype(F32) - total[0:SEQ]).astype(BF16)

    def end_second():
        grad, first_mean, second_mean = end_attn()
        phase("back_second")
        normed_own = nm[me]
        gain_row = jnp.sum(grad * normed_own, 0, keepdims=True)
        small2.send(
            jnp.concatenate([gain_row[:, 0:128], gain_row[:, 128:256], jnp.zeros((6, 128), F32)], 0)
        )
        back = spread_attn * (grad * gain_at(gain_attn_ref, me) - first_mean - normed_own * second_mean)
        o_bsecond[...] = (gs_ref[...].astype(F32) + back[0:SEQ]).astype(BF16)

    for name in TICKS["tail"]:
        if name == "first":
            end_first()
        elif name == "second":
            end_second()
        else:
            tick(name)
    assert not (small1.todo or small2.todo or any(one.todo for one, _ in scatters.values()))
    phase("drain")
    assert (net.sends, net.recvs) == (SENDS, RECVS), (net.sends, net.recvs)
    net.drain()
    phase(None)


def hand_over(*refs):
    half = len(refs) // 2
    for src, dst in zip(refs[:half], refs[half:]):
        dst[...] = src[...]


def on_device(
    out_first, out_second, grad_first, grad_second, gain_attn, gain_mlp,
    qkv_weight, proj_weight, inner_weight, inner_bias, outer_weight,
):
    sds = jax.ShapeDtypeStruct
    vmem = pl.BlockSpec(memory_space=pltpu.VMEM)
    hbm = pl.BlockSpec(memory_space=pltpu.HBM)

    def v(*shape, dtype=BF16):
        return pltpu.VMEM(shape, dtype)

    def piece_bufs(stages, cols):
        left = [a for stage in stages for a in stage[1:]]
        bufs = [v(*[SIZE[a] for a in left], 16, cols)]
        for how, *axes in stages:
            left = left[len(axes) :]
            shape = [SIZE[a] for a in left] + [16, cols]
            if how == "ring":
                shape = [2, SIZE[axes[0]] // 2] + shape
            elif how == "spread":
                count = 1
                for a in axes:
                    count *= SIZE[a]
                shape = [count] + shape
            bufs.append(v(*shape))
        return bufs

    pieces = []
    for _, _, kind, lo, hi in PIECES:
        pieces += piece_bufs(KINDS[kind], hi - lo)
    scratch = [
        *[v(SEQ, W) for _ in range(4)], v(1, 1024, dtype=F32), v(1, 1024, dtype=F32),
        v(3, 1024, W), v(1024, W), v(1024, 1024), v(1, 1024, dtype=F32), v(1024, 1024),
        pltpu.SemaphoreType.DMA((11,)),
        pltpu.SemaphoreType.DMA((SENDS,)), pltpu.SemaphoreType.DMA((RECVS,)),
        v(4, R, W), v(4, K, W), v(4, R, W), v(4, K, W), v(4, R, W, dtype=F32),
        v(K, 1024), v(K, 1024), v(R, 1024, dtype=F32), v(R, 1024, dtype=F32), v(K, 1024), v(1024, K), v(1024, K),
        *[v(2, 2, R, W, dtype=F32) for _ in range(4)],
        *[v(2, R, W, dtype=F32) for _ in range(2)],
        *[v(R, W) for _ in range(8)],
        v(4, 8, K, dtype=F32), v(4, 8, K, dtype=F32),
        *[v(K, W) for _ in range(4)],
        v(4, K, W, dtype=F32), v(4, K, K, dtype=F32), v(3, K, W),
        *pieces,
        *[v(n, 8, W, dtype=F32) for n in (4, 8, 2)], *[v(n, 8, 128, dtype=F32) for n in (8, 8)],
    ]
    shapes = [
        sds((SEQ, W), BF16), sds((SEQ, W), BF16), sds((SEQ, W), BF16), sds((SEQ, W), BF16),
        sds((3, 16, W), F32), sds((16, W), F32), sds((16, 1024), F32), sds((1, 1024), F32),
        sds((16, 1024), F32), sds((1, W), F32), sds((1, W), F32),
    ]
    outs = pl.pallas_call(
        kernel,
        out_shape=[pltpu.VMEM(o.shape, o.dtype) for o in shapes],
        in_specs=[hbm] * 11,
        out_specs=[vmem] * 11,
        scratch_shapes=scratch,
        compiler_params=pltpu.CompilerParams(
            collective_id=0, has_side_effects=True, vmem_limit_bytes=56 * 1024 * 1024
        ),
        name="block_pair",
    )(
        out_first[0], out_second[0], grad_first[0], grad_second[0],
        gain_attn.reshape(1, -1), gain_mlp.reshape(1, -1),
        jnp.swapaxes(qkv_weight, 0, 1), proj_weight, inner_weight, inner_bias.reshape(1, -1), outer_weight,
    )
    outs = pl.pallas_call(
        hand_over,
        out_shape=shapes,
        in_specs=[vmem] * 11,
        out_specs=[vmem] * 11,
        compiler_params=pltpu.CompilerParams(vmem_limit_bytes=8 * 1024 * 1024),
        name="hand_over",
    )(*outs)
    return (
        outs[0][None], outs[1][None], outs[2][None], outs[3][None],
        jnp.swapaxes(outs[4], 0, 1), outs[5], outs[6], outs[7].reshape(-1), outs[8],
        outs[9].reshape(-1), outs[10].reshape(-1),
    )


def solution(mesh):
    split = Mesh(mesh.devices.reshape(NZ, 2, NX, 2, 2), AXES)
    rows = P(DP, None, TENSOR)
    return jax.shard_map(
        on_device,
        mesh=split,
        in_specs=(
            rows, rows, rows, rows, P(), P(),
            P(None, None, TENSOR), P(None, TENSOR), P(None, TENSOR), P(TENSOR), P(None, TENSOR),
        ),
        out_specs=(
            rows, rows, rows, rows,
            P(DP, None, TENSOR), P(DP, TENSOR), P(DP, TENSOR), P(TENSOR), P(DP, TENSOR),
            P(TENSOR), P(TENSOR),
        ),
        check_vma=False,
    )
```

```python
import functools

import jax
import jax.numpy as jnp
from jax import lax
from jax.experimental import pallas as pl
from jax.experimental.pallas import tpu as pltpu
from jax.sharding import Mesh
from jax.sharding import PartitionSpec as P

AXES = ("z", "yl", "x", "yh", "c")
DP = ("z", "yl", "x")
TENSOR = ("yh", "c")
MESH = pl.DeviceIdType.MESH
SEQ = 197
R = 208
K = 256
W = 256
NZ, NX = 8, 4
SIZE = {"z": NZ, "x": NX, "yl": 2}
EPS = 1e-06
F32 = jnp.float32
BF16 = jnp.bfloat16
GELU_A = 0.7978845608028654
GELU_B = 0.044715
ORDER = ("q", "k")
SENDS, RECVS = 48, 62
KINDS = {
    "a": (("ring", "x"), ("swap", "yl"), ("ring", "z")),
    "b": (("ring", "z"), ("spread", "x", "yl")),
    "c": (("spread", "x"), ("swap", "yl"), ("spread", "z")),
    "d": (("ring", "x"), ("swap", "yl"), ("spread", "z")),
    "e": (("swap", "yl"), ("spread", "x"), ("spread", "z")),
}
PIECES = (
    ("O0", "outer0", "a", 0, 512),
    ("O1", "outer", "b", 512, 1024),
    ("I0", "inner", "b", 0, 768),
    ("I1", "inner", "c", 768, 1024),
    ("v", "v", "d", 0, 256),
    ("proj", "proj", "e", 0, 256),
    ("q", "q", "d", 0, 256),
    ("k", "k", "d", 0, 256),
)
TICKS = {
    "ga": (),
    "swap": (),
    "inner": (),
    "back": (
        "O0", "O1",
    ),
    "forward": (
        "I0",
    ),
    "qkv": (),
    "probs_half": (
        "I1",
    ),
    "probs": (
        "s1", "O1",
    ),
    "grad_heads": (),
    "heads": (),
    "value": (),
    "heads_half": (),
    "attn": (
        "I1", "I0", "O0",
    ),
    "pair": (
        "v",
    ),
    "tail": (
        "s1", "O1", "q", "k", "proj", "I1", "O0", "v", "I0", "q", "first", "O1", "O0", "s1", "second", "k",
        "v", "q", "I0", "O0", "proj", "k", "s2", "O1", "O0", "v", "q", "I0", "O0", "proj", "s2", "k",
    ),
}

def nn(a, b):
    return lax.dot_general(a, b, (((1,), (0,)), ((), ())), preferred_element_type=F32)


def nt(a, b):
    return lax.dot_general(a, b, (((1,), (1,)), ((), ())), preferred_element_type=F32)


def at_cols(ref, lo, hi):
    return ref.at[(slice(None),) * (len(ref.shape) - 1) + (slice(lo, hi),)]


def add_into(dst, src):
    dst[...] = dst[...] + src[...]


class Phases:
    def __init__(self):
        self.scope = None

    def __call__(self, name):
        if self.scope is not None:
            self.scope.__exit__(None, None, None)
        self.scope = jax.named_scope(name) if name else None
        if name:
            self.scope.__enter__()


class Net:
    def __init__(self, send_sem, recv_sem):
        self.pos = {a: lax.axis_index(a) for a in AXES}
        self.send_sem, self.recv_sem = send_sem, recv_sem
        self.sends, self.recvs = 0, 0
        self.out = []

    def dev(self, **other):
        where = dict(self.pos)
        where.update(other)
        return tuple(where[a] for a in AXES)

    def copies(self, triples, sent, got=None, share=None):
        fresh = share is None or len(share) == 1
        k, m = (self.sends if fresh else share[1]), self.recvs
        self.sends, self.recvs = self.sends + fresh, m + 1
        assert self.sends <= SENDS and self.recvs <= RECVS

        def describe(src, dst, target):
            return pltpu.make_async_remote_copy(
                src_ref=src,
                dst_ref=dst,
                send_sem=self.send_sem.at[k],
                recv_sem=self.recv_sem.at[m],
                device_id=target,
                device_id_type=MESH,
            )

        for triple in triples:
            describe(*triple).start()
        target = triples[0][2]
        if fresh:
            whole = sent if share is None else share[0]
            self.out.append(describe(whole, whole, target))
            if share is not None:
                share.append(k)
        return describe(sent if got is None else got, sent if got is None else got, target)

    def copy(self, src, dst, target, share=None):
        return self.copies([(src, dst, target)], src, dst, share)

    def drain(self):
        for c in self.out:
            c.wait_send()


class Chain:
    def __init__(self, net, chunk, axis, size, recv):
        self.net, self.chunk, self.axis, self.size, self.recv = net, chunk, axis, size, recv
        self.pos = net.pos[axis]
        self.steps = size // 2

    def part(self, ref, way, distance):
        if distance == self.steps:
            half = ref.shape[-1] // 2
            return at_cols(ref, way * half, (way + 1) * half)
        return ref

    def owner(self, way, distance):
        return lax.rem(self.pos + (distance if way == 0 else self.size - distance), self.size)

    def send(self, step):
        distance = self.steps - step + 1
        triples = []
        for way in (0, 1):
            src = self.part(self.chunk(self.owner(way, distance)), way, distance)
            dst = self.part(self.recv.at[way, step - 1], way, distance)
            triples.append((src, dst, self.net.dev(**{self.axis: self.owner(way, 1)})))
        both = self.recv.at[0, 0] if step == 1 else self.recv.at[:, step - 1]
        if step == 2:
            self.share = [self.recv.at[:, 1:]]
        self.flying = self.net.copies(triples, both, None, None if step == 1 else self.share)

    def tick(self, step, finish):
        self.flying.wait_recv()
        distance = self.steps - step + 1
        if step == self.steps and finish:
            mine = self.chunk(self.owner(0, 0))
            finish(mine[...].astype(F32) + self.recv[0, step - 1].astype(F32) + self.recv[1, step - 1].astype(F32))
            return
        for way in (0, 1):
            got = self.part(self.recv.at[way, step - 1], way, distance)
            mine = self.part(self.chunk(self.owner(way, distance - 1)), way, distance)
            add_into(mine, got)
        if step < self.steps:
            self.send(step + 1)


class Swap:
    def __init__(self, net, part, recv):
        self.net, self.part, self.recv = net, part, recv
        self.yl = net.pos["yl"]
        self.steps = 1

    def send(self, step):
        target = self.net.dev(yl=1 - self.yl)
        self.flying = self.net.copy(self.part((1 - self.yl,)), self.recv, target)

    def tick(self, step, finish):
        self.flying.wait_recv()
        mine = self.part((self.yl,))
        if finish:
            finish(mine[...].astype(F32) + self.recv[...].astype(F32))
        else:
            add_into(mine, self.recv)


class Spread:
    def __init__(self, net, axes, part, recv):
        self.net, self.axes, self.part, self.recv = net, axes, part, recv
        self.steps = 1

    def send(self, step):
        net, triples = self.net, []
        count = self.recv.shape[0]
        for j in range(1, count):
            there, rest = {}, j
            for axis in self.axes:
                n = SIZE[axis]
                there[axis] = lax.rem(net.pos[axis] + rest % n, n)
                rest //= n
            src = self.part(tuple(there[a] for a in self.axes))
            triples.append((src, self.recv.at[j], net.dev(**there)))
        self.flying = net.copies(triples, self.recv.at[1:count])

    def tick(self, step, finish):
        self.flying.wait_recv()
        mine = self.part(tuple(self.net.pos[a] for a in self.axes))
        total = mine[...].astype(F32)
        for j in range(1, self.recv.shape[0]):
            total = total + self.recv[j].astype(F32)
        if finish:
            finish(total)
        else:
            mine[...] = total.astype(BF16)


class Scatter:
    def __init__(self, net, stages, bufs, finish):
        buf, before, steps = bufs[0], (), []
        for k, (how, *axes) in enumerate(stages):
            part = functools.partial(lambda before, here: buf.at[before + here], before)
            if how == "ring":
                chunk = functools.partial(lambda part, o: part((o,)), part)
                stage = Chain(net, chunk, axes[0], SIZE[axes[0]], bufs[k + 1])
            elif how == "swap":
                stage = Swap(net, part, bufs[k + 1])
            else:
                stage = Spread(net, axes, part, bufs[k + 1])
            before = before + tuple(net.pos[a] for a in axes)
            steps.append(stage)
        self.todo = [functools.partial(steps[0].send, 1)]
        for k, stage in enumerate(steps):
            last = k + 1 == len(steps)
            for step in range(1, stage.steps + 1):
                turn = last and step == stage.steps
                follow = steps[k + 1] if not last and step == stage.steps else None
                self.todo.append(functools.partial(self.advance, stage, step, finish if turn else None, follow))

    def advance(self, stage, step, finish, follow):
        stage.tick(step, finish)
        if follow is not None:
            follow.send(1)

    def tick(self):
        self.todo.pop(0)()


class Everyone:
    def __init__(self, net, stages, slots, finish):
        self.net, self.slots, self.finish = net, slots, finish
        self.stages = stages
        self.todo = [functools.partial(self.turn, k) for k in range(len(stages))]

    def send(self, block, k=0):
        net, slot = self.net, self.slots[k]
        slot[0] = block
        triples = []
        for j in range(1, slot.shape[0]):
            there, rest = {}, j
            for axis in self.stages[k]:
                n = SIZE[axis]
                there[axis] = lax.rem(net.pos[axis] + rest % n, n)
                rest //= n
            triples.append((slot.at[0], slot.at[j], net.dev(**there)))
        self.flying = net.copies(triples, slot.at[1 : slot.shape[0]])

    def turn(self, k):
        self.flying.wait_recv()
        slot = self.slots[k]
        total = slot[0]
        for j in range(1, slot.shape[0]):
            total = total + slot[j]
        if k + 1 < len(self.stages):
            self.send(total, k + 1)
        else:
            self.finish(total)

    def tick(self):
        self.todo.pop(0)()


def kernel(
    of_hbm, os_hbm, gf_hbm, gs_hbm, gain_attn_hbm, gain_mlp_hbm, wq_hbm, wp_hbm, wi_hbm, bias_hbm, wo_hbm,
    o_first, o_second, o_bfirst, o_bsecond, o_qkv, o_proj, o_inner, o_bias, o_outer, o_gattn, o_gmlp,
    of_ref, os_ref, gf_ref, gs_ref, gain_attn_ref, gain_mlp_ref, wq, wp, wi, bias_ref, wo,
    load_sem, send_sem, recv_sem,
    xg, gg, xs, xb, nm, im, act, us, dg, gh, lhs_a, lhs_b,
    pair_a, pair_b, pair_c, pair_d, mine_a, mine_b, out_a, out_b, out_c, out_d, in_a, in_b, in_c, in_d,
    stat_a, stat_b, qs, ks, vs, hs, rows_s, probs_s, g3,
    *rest,
):
    phase = Phases()
    phase("entry")
    net = Net(send_sem, recv_sem)
    pos = net.pos
    yh, c = pos["yh"], pos["c"]
    me, sib = 2 * yh + c, 2 * yh + 1 - c
    far, diag = 2 * (1 - yh) + c, 2 * (1 - yh) + 1 - c
    d_sib, d_far, d_diag = net.dev(c=1 - c), net.dev(yh=1 - yh), net.dev(yh=1 - yh, c=1 - c)

    loads = {}
    for k, (name, src, dst) in enumerate(
        (
            ("of", of_hbm, of_ref), ("gs", gs_hbm, gs_ref), ("gm", gain_mlp_hbm, gain_mlp_ref),
            ("bias", bias_hbm, bias_ref), ("wi", wi_hbm, wi), ("wo", wo_hbm, wo), ("os", os_hbm, os_ref),
            ("gf", gf_hbm, gf_ref), ("ga", gain_attn_hbm, gain_attn_ref), ("wq", wq_hbm, wq), ("wp", wp_hbm, wp),
        )
    ):
        loads[name] = pltpu.make_async_copy(src, dst, load_sem.at[k])
        loads[name].start()

    barrier = pltpu.get_barrier_semaphore()
    others = [d_sib, d_far, d_diag]
    for dy in range(2):
        y = lax.rem(pos["yl"] + dy, 2)
        others += [net.dev(z=lax.rem(pos["z"] + k, NZ), yl=y) for k in range(1 - dy, NZ)]
        others += [net.dev(x=lax.rem(pos["x"] + k, NX), yl=y) for k in range(1, NX)]
    for other in others:
        pl.semaphore_signal(barrier, inc=1, device_id=other, device_id_type=MESH)

    zero_rows = jnp.zeros((K - R, W), BF16)
    loads["of"].wait()
    xg[me] = jnp.zeros((R, W), BF16)
    xg[me, 0:SEQ] = of_ref[...]
    pl.semaphore_wait(barrier, len(others))

    def gather_start(ref):
        own = ref.at[me, 0:R]
        share = [ref.at[0:3, 0:R]]
        return [net.copy(own, own, d_far, share), net.copy(own, own, d_sib, share), share]

    def gather_forward(ref, two):
        two[0].wait_recv()
        got = ref.at[far, 0:R]
        two.append(net.copy(got, got, d_sib, two[2]))

    def gather_end(two):
        two[1].wait_recv()
        two[3].wait_recv()

    def gain_of(ref, b):
        return ref[0:1, b * W : (b + 1) * W]

    def gain_at(ref, b):
        return ref[0:1, pl.ds(pl.multiple_of(b * W, W), W)]

    def rows_at(ref, q):
        return ref[pl.ds(pl.multiple_of(q * W, W), W), :]

    def normalize(block, gain_ref):
        total = jnp.zeros((R, 1), F32)
        for b in range(4):
            total = total + jnp.sum(block(b), 1, keepdims=True)
        mean = total * (1.0 / 1024)
        square = jnp.zeros((R, 1), F32)
        for b in range(4):
            centre = block(b) - mean
            nm[b] = centre
            square = square + jnp.sum(centre * centre, 1, keepdims=True)
        spread = lax.rsqrt(square * (1.0 / 1024) + EPS)
        for b in range(4):
            normed = nm[b] * spread
            nm[b] = normed
            im[0:R, b * W : (b + 1) * W] = (normed * gain_of(gain_ref, b)).astype(BF16)
        return spread

    def turn(lhs, block):
        for b in range(4):
            lhs[b * W : (b + 1) * W] = block(b).T

    lane = lax.broadcasted_iota(jnp.int32, (R, 128), 1)

    def stats_of(part, q, gain_ref, sums):
        scaled = part * gain_at(gain_ref, q)
        one = sums[0] + jnp.sum(scaled, 1, keepdims=True)
        two = sums[1] + jnp.sum(scaled * nm[q], 1, keepdims=True)
        return (one, two)

    def stats_send(sums, stat):
        both = jnp.where(lane == 0, sums[0], jnp.where(lane == 1, sums[1], 0.0))
        both = jnp.concatenate([both, jnp.zeros((K - R, 128), F32)], 0)
        stat[0] = both.T[0:8, :]
        triples = [(stat.at[0], stat.at[k + 1], d) for k, d in enumerate((d_sib, d_far, d_diag))]
        return net.copies(triples, stat.at[1:4])

    def stats_end(sent, stat):
        sent.wait_recv()
        total = (stat[0] + stat[1]) + (stat[2] + stat[3])
        wide = jnp.concatenate([total * (1.0 / 1024), jnp.zeros((120, K), F32)], 0).T
        return wide[0:R, 0:1], wide[0:R, 1:2]

    def norm_back(part_of, gain_ref, pair, mine, out, inn, stat, stop, early):
        phase("nb_parts")
        sums = (jnp.zeros((R, 1), F32), jnp.zeros((R, 1), F32))
        for slot, q in ((0, sib), (1, diag)):
            part = part_of(q)
            pair[0, slot] = part
            sums = stats_of(part, q, gain_ref, sums)
        swap = net.copy(pair.at[0], pair.at[1], d_sib)
        for slot, q in ((0, far), (1, me)):
            part = part_of(q)
            mine[slot] = part
            sums = stats_of(part, q, gain_ref, sums)
        sent = stats_send(sums, stat)
        early()
        phase("nb_swap_wait")
        swap.wait_recv()
        out[...] = (mine[0] + pair[1, 1]).astype(BF16)
        last = net.copy(out, inn, d_far)
        tick(*TICKS[stop])

        def end():
            phase("nb_last_wait")
            last.wait_recv()
            first_mean, second_mean = stats_end(sent, stat)
            grad = mine[1] + pair[1, 0] + inn[...].astype(F32)
            return grad, first_mean, second_mean

        return end

    def outer_term(lhs, rhs, scatter, col):
        order, buf = scatter
        for b in range(4):
            tile = nn(lhs[b * W : (b + 1) * W], rhs).astype(BF16).reshape(2, 2, 4, 16, W)
            for z in range(2):
                for y in range(2):
                    for x in range(4):
                        at = {"z": 2 * b + z, "yl": y, "x": x}
                        where = tuple(at[a] for a in order)
                        buf[where + (slice(None), slice(col, col + W))] = tile[z, y, x]

    def writer(ref, lo, hi):
        def finish(total):
            ref[:, lo:hi] = total

        return finish

    def kind_writer(k):
        def finish(total):
            o_qkv[k] = total

        return finish

    targets = {
        "outer": lambda lo, hi: writer(o_outer, lo, hi),
        "outer0": lambda lo, hi: writer(o_outer, lo, hi),
        "inner": lambda lo, hi: writer(o_inner, lo, hi),
        "proj": lambda lo, hi: writer(o_proj, lo, hi),
        "q": lambda lo, hi: kind_writer(0),
        "k": lambda lo, hi: kind_writer(1),
        "v": lambda lo, hi: kind_writer(2),
    }
    scatters, at = {}, 0
    for name, what, kind, lo, hi in PIECES:
        stages = KINDS[kind]
        bufs = rest[at : at + len(stages) + 1]
        at += len(stages) + 1
        order = [a for stage in stages for a in stage[1:]]
        scatters[name] = (Scatter(net, stages, bufs, targets[what](lo, hi)), (order, bufs[0]))

    def finish_small1(total):
        for n in range(4):
            o_bias[0:1, n * W : (n + 1) * W] = total[n : n + 1]
        o_gmlp[...] = total[4:5]

    def finish_small2(total):
        o_gattn[0:1, 0:128] = total[0:1]
        o_gattn[0:1, 128:256] = total[1:2]

    small1 = Everyone(net, (("x",), ("z",), ("yl",)), rest[at : at + 3], finish_small1)
    small2 = Everyone(net, (("z",), ("x", "yl")), rest[at + 3 : at + 5], finish_small2)

    def make(what, lhs, tile_of):
        for name, kind, first, lo, hi in PIECES:
            if kind == what:
                for col in range(lo, hi, W):
                    outer_term(lhs, tile_of(col), scatters[name][1], col - lo)
                scatters[name][0].tick()

    def tick(*names):
        for name in names:
            phase("tick_" + name)
            if name == "s1":
                small1.tick()
            elif name == "s2":
                small2.tick()
            else:
                scatters[name][0].tick()

    x_all = gather_start(xg)
    loads["gs"].wait()
    gg[me, 0:R] = jnp.zeros((R, W), BF16)
    gg[me, 0:SEQ] = gs_ref[...]
    g_all = gather_start(gg)
    for b in range(4):
        gg[b, R:K] = zero_rows
        xb[b, R:K] = zero_rows
        for ref in (im, act, gh):
            ref[R:K, b * W : (b + 1) * W] = zero_rows
    for ref in (qs, ks, vs, hs):
        ref[R:K] = zero_rows
    phase("gather_x_wait")
    gather_forward(xg, x_all)
    gather_end(x_all)
    phase("norm_mlp")
    loads["gm"].wait()
    spread_mlp = normalize(lambda b: xg[b].astype(F32), gain_mlp_ref)
    phase("hidden")
    loads["bias"].wait()
    loads["wi"].wait()
    for n in range(4):
        cols = slice(n * W, (n + 1) * W)
        u = nn(im[0:R], wi[:, cols]) + bias_ref[0:1, cols]
        square = u * u
        t = jnp.tanh(GELU_A * (u + GELU_B * (square * u)))
        half = 0.5 * (1.0 + t)
        act[0:R, cols] = (u * half).astype(BF16)
        us[:, cols] = u
        dg[:, cols] = half
        if n == 1:
            gather_forward(gg, g_all)
    phase("mlp_out")
    loads["wo"].wait()
    pair_a[0, 0] = nt(act[0:R], rows_at(wo, sib))
    pair_a[0, 1] = nt(act[0:R], rows_at(wo, diag))
    pair_mlp = net.copy(pair_a.at[0], pair_a.at[1], d_sib)
    mine_a[0] = nt(act[0:R], rows_at(wo, far))
    mine_a[1] = nt(act[0:R], rows_at(wo, me))
    phase("g_wait")
    gather_end(g_all)
    phase("slope")
    for n in range(4):
        cols = slice(n * W, (n + 1) * W)
        u, half = us[:, cols], dg[:, cols]
        t = 2.0 * half - 1.0
        slope = 0.5 * GELU_A * (1.0 - t * t) * (1.0 + 3.0 * GELU_B * (u * u))
        dg[:, cols] = half + u * slope
    turn(lhs_a, lambda b: gg[b])
    phase("pair_mlp_wait")
    pair_mlp.wait_recv()
    out_a[...] = (mine_a[0] + pair_a[1, 1]).astype(BF16)
    far_mlp = net.copy(out_a, in_a, d_far)
    phase("outer_first")
    make("outer0", lhs_a, lambda col: act[:, col : col + W])

    def outer_grad():
        phase("outer_grad")
        make("outer", lhs_a, lambda col: act[:, col : col + W])

    phase("grad_active")
    bias_rows = []
    for n in range(4):
        cols = slice(n * W, (n + 1) * W)
        grad_active = nn(gg[0, 0:R], wo[0:W, cols])
        for b in range(1, 4):
            grad_active = grad_active + nn(gg[b, 0:R], wo[b * W : (b + 1) * W, cols])
        low = (grad_active * dg[0:R, cols]).astype(BF16)
        gh[0:R, cols] = low
        bias_rows.append(jnp.sum(low.astype(F32), 0, keepdims=True))
    tick(*TICKS["ga"])

    valid = lax.broadcasted_iota(jnp.int32, (SEQ, W), 0) < SEQ
    ends = {}

    def between_mlp():
        phase("turn_im")
        turn(lhs_b, lambda b: im[:, b * W : (b + 1) * W])
        phase("inner_grad")
        make("inner", lhs_b, lambda col: gh[:, col : col + W])
        phase("far_mlp_wait")
        far_mlp.wait_recv()
        phase("input_second")
        loads["os"].wait()
        mlp = mine_a[1] + pair_a[1, 0] + in_a[...].astype(F32)
        second = (os_ref[...].astype(F32) - mlp[0:SEQ]).astype(BF16)
        o_second[...] = second
        xs[me] = jnp.zeros((R, W), BF16)
        xs[me, 0:SEQ] = second
        ends["second"] = gather_start(xs)
        tick(*TICKS["inner"])

    end_mlp = norm_back(
        lambda q: nt(gh[0:R], rows_at(wi, q)),
        gain_mlp_ref, pair_b, mine_b, out_b, in_b, stat_a, "swap", outer_grad,
    )
    between_mlp()
    grad, first_mean, second_mean = end_mlp()
    phase("back_first")
    loads["gf"].wait()
    normed_own = nm[me]
    back = spread_mlp * (grad * gain_at(gain_mlp_ref, me) - first_mean - normed_own * second_mean)
    first = (gf_ref[...].astype(F32) + back[0:SEQ]).astype(BF16)
    o_bfirst[...] = first
    xb[me, 0:R] = jnp.zeros((R, W), BF16)
    xb[me, 0:SEQ] = first
    b_all = gather_start(xb)
    block = bias_rows + [jnp.sum(grad * normed_own, 0, keepdims=True), jnp.zeros((3, W), F32)]
    small1.send(jnp.concatenate(block, 0))
    tick(*TICKS["back"])
    phase("xs_forward")
    gather_forward(xs, ends["second"])
    tick(*TICKS["forward"])
    phase("xs_wait")
    gather_end(ends["second"])

    phase("norm_attn")
    loads["ga"].wait()
    spread_attn = normalize(lambda b: xs[b].astype(F32), gain_attn_ref)
    phase("qkv")
    loads["wq"].wait()
    for kind, ref in enumerate((qs, ks, vs)):
        ref[0:R] = nn(im[0:R], wq[kind]).astype(BF16)
    phase("turn_attn")
    turn(lhs_a, lambda b: im[:, b * W : (b + 1) * W])
    tick(*TICKS["qkv"])

    head_lane = lax.broadcasted_iota(jnp.int32, (K, W), 1) // 64
    key_ok = lax.broadcasted_iota(jnp.int32, (K, K), 1) < SEQ
    factor = 0.125

    def only(ref, h):
        return jnp.where(head_lane == h, ref[...], jnp.zeros((), BF16))

    for h in range(4):
        phase(f"probs_{h}")
        scores = jnp.where(key_ok, nt(only(qs, h), ks[...]) * factor, -1e30)
        e = jnp.exp(scores - jnp.max(scores, 1, keepdims=True))
        probs = e * (1.0 / jnp.sum(e, 1, keepdims=True))
        probs_s[h] = probs
        a_h = nn(probs.astype(BF16), only(vs, h))
        if h == 0:
            rows_s[0] = a_h
        else:
            rows_s[0] += a_h
        if h == 1:
            phase("xb_forward")
            gather_forward(xb, b_all)
            tick(*TICKS["probs_half"])
    tick(*TICKS["probs"])
    rows_low = rows_s[0].astype(BF16)
    phase("xb_wait")
    gather_end(b_all)
    phase("grad_heads")
    loads["wp"].wait()
    heads = nn(xb[0, 0:R], wp[0:W])
    for b in range(1, 4):
        heads = heads + nn(xb[b, 0:R], wp[b * W : (b + 1) * W])
    hs[0:R] = heads.astype(BF16)
    tick(*TICKS["grad_heads"])
    phase("proj_grad")
    turn(lhs_b, lambda b: xb[b])
    make("proj", lhs_b, lambda col: rows_low)
    tick(*TICKS["heads"])

    for h in range(4):
        phase(f"value_{h}")
        gv_h = nn(probs_s[h].astype(BF16).T, only(hs, h))
        if h == 0:
            rows_s[3] = gv_h
        else:
            rows_s[3] += gv_h
    phase("v_grad")
    g3[2] = rows_s[3].astype(BF16)
    make("v", lhs_a, lambda col: g3[2])
    tick(*TICKS["value"])
    for h in range(4):
        phase(f"head_{h}")
        q_h, k_h, g_h = only(qs, h), only(ks, h), only(hs, h)
        probs = probs_s[h]
        grad_probs = nt(g_h, vs[...])
        row_dot = jnp.sum(grad_probs * probs, 1, keepdims=True)
        grad_scores = (probs * (grad_probs - row_dot)).astype(BF16)
        gq_h = nn(grad_scores, k_h)
        gk_h = nn(grad_scores.T, q_h)
        if h == 0:
            rows_s[1], rows_s[2] = gq_h, gk_h
        else:
            rows_s[1] += gq_h
            rows_s[2] += gk_h
        if h == 1:
            tick(*TICKS["heads_half"])
    phase("attn_grads")
    g3[0] = (rows_s[1] * factor).astype(BF16)
    g3[1] = (rows_s[2] * factor).astype(BF16)
    for name in ORDER:
        make(name, lhs_a, lambda col: g3["qkv".index(name)])
    phase("attn_out")
    for slot, q in ((0, sib), (1, diag)):
        pair_c[0, slot] = nt(rows_low[0:R], rows_at(wp, q))
    pair_out = net.copy(pair_c.at[0], pair_c.at[1], d_sib)
    for slot, q in ((0, far), (1, me)):
        mine_a[slot] = nt(rows_low[0:R], rows_at(wp, q))
    tick(*TICKS["attn"])

    def qkv_part(q):
        cols = pl.ds(pl.multiple_of(q * W, W), W)
        part = nt(g3[0, 0:R], wq[0, cols, :])
        part = part + nt(g3[1, 0:R], wq[1, cols, :])
        return part + nt(g3[2, 0:R], wq[2, cols, :])

    sent = {}

    def attn_far():
        phase("pair_out_wait")
        pair_out.wait_recv()
        out_c[...] = (mine_a[0] + pair_c[1, 1]).astype(BF16)
        sent["out"] = net.copy(out_c, in_c, d_far)

    end_attn = norm_back(
        qkv_part, gain_attn_ref, pair_d, mine_b, out_d, in_d, stat_b, "pair", attn_far
    )

    def end_first():
        phase("far_out_wait")
        sent["out"].wait_recv()
        total = mine_a[1] + pair_c[1, 0] + in_c[...].astype(F32)
        o_first[...] = (of_ref[...].astype(F32) - total[0:SEQ]).astype(BF16)

    def end_second():
        grad, first_mean, second_mean = end_attn()
        phase("back_second")
        normed_own = nm[me]
        gain_row = jnp.sum(grad * normed_own, 0, keepdims=True)
        small2.send(
            jnp.concatenate([gain_row[:, 0:128], gain_row[:, 128:256], jnp.zeros((6, 128), F32)], 0)
        )
        back = spread_attn * (grad * gain_at(gain_attn_ref, me) - first_mean - normed_own * second_mean)
        o_bsecond[...] = (gs_ref[...].astype(F32) + back[0:SEQ]).astype(BF16)

    for name in TICKS["tail"]:
        if name == "first":
            end_first()
        elif name == "second":
            end_second()
        else:
            tick(name)
    assert not (small1.todo or small2.todo or any(one.todo for one, _ in scatters.values()))
    phase("drain")
    assert (net.sends, net.recvs) == (SENDS, RECVS), (net.sends, net.recvs)
    net.drain()
    phase(None)


def hand_over(*refs):
    half = len(refs) // 2
    for src, dst in zip(refs[:half], refs[half:]):
        dst[...] = src[...]


def on_device(
    out_first, out_second, grad_first, grad_second, gain_attn, gain_mlp,
    qkv_weight, proj_weight, inner_weight, inner_bias, outer_weight,
):
    sds = jax.ShapeDtypeStruct
    vmem = pl.BlockSpec(memory_space=pltpu.VMEM)
    hbm = pl.BlockSpec(memory_space=pltpu.HBM)

    def v(*shape, dtype=BF16):
        return pltpu.VMEM(shape, dtype)

    def piece_bufs(stages, cols):
        left = [a for stage in stages for a in stage[1:]]
        bufs = [v(*[SIZE[a] for a in left], 16, cols)]
        for how, *axes in stages:
            left = left[len(axes) :]
            shape = [SIZE[a] for a in left] + [16, cols]
            if how == "ring":
                shape = [2, SIZE[axes[0]] // 2] + shape
            elif how == "spread":
                count = 1
                for a in axes:
                    count *= SIZE[a]
                shape = [count] + shape
            bufs.append(v(*shape))
        return bufs

    pieces = []
    for _, _, kind, lo, hi in PIECES:
        pieces += piece_bufs(KINDS[kind], hi - lo)
    scratch = [
        *[v(SEQ, W) for _ in range(4)], v(1, 1024, dtype=F32), v(1, 1024, dtype=F32),
        v(3, 1024, W), v(1024, W), v(1024, 1024), v(1, 1024, dtype=F32), v(1024, 1024),
        pltpu.SemaphoreType.DMA((11,)),
        pltpu.SemaphoreType.DMA((SENDS,)), pltpu.SemaphoreType.DMA((RECVS,)),
        v(4, R, W), v(4, K, W), v(4, R, W), v(4, K, W), v(4, R, W, dtype=F32),
        v(K, 1024), v(K, 1024), v(R, 1024, dtype=F32), v(R, 1024, dtype=F32), v(K, 1024), v(1024, K), v(1024, K),
        *[v(2, 2, R, W, dtype=F32) for _ in range(4)],
        *[v(2, R, W, dtype=F32) for _ in range(2)],
        *[v(R, W) for _ in range(8)],
        v(4, 8, K, dtype=F32), v(4, 8, K, dtype=F32),
        *[v(K, W) for _ in range(4)],
        v(4, K, W, dtype=F32), v(4, K, K, dtype=F32), v(3, K, W),
        *pieces,
        *[v(n, 8, W, dtype=F32) for n in (4, 8, 2)], *[v(n, 8, 128, dtype=F32) for n in (8, 8)],
    ]
    shapes = [
        sds((SEQ, W), BF16), sds((SEQ, W), BF16), sds((SEQ, W), BF16), sds((SEQ, W), BF16),
        sds((3, 16, W), F32), sds((16, W), F32), sds((16, 1024), F32), sds((1, 1024), F32),
        sds((16, 1024), F32), sds((1, W), F32), sds((1, W), F32),
    ]
    outs = pl.pallas_call(
        kernel,
        out_shape=[pltpu.VMEM(o.shape, o.dtype) for o in shapes],
        in_specs=[hbm] * 11,
        out_specs=[vmem] * 11,
        scratch_shapes=scratch,
        compiler_params=pltpu.CompilerParams(
            collective_id=0, has_side_effects=True, vmem_limit_bytes=56 * 1024 * 1024
        ),
        name="block_pair",
    )(
        out_first[0], out_second[0], grad_first[0], grad_second[0],
        gain_attn.reshape(1, -1), gain_mlp.reshape(1, -1),
        jnp.swapaxes(qkv_weight, 0, 1), proj_weight, inner_weight, inner_bias.reshape(1, -1), outer_weight,
    )
    outs = pl.pallas_call(
        hand_over,
        out_shape=shapes,
        in_specs=[vmem] * 11,
        out_specs=[vmem] * 11,
        compiler_params=pltpu.CompilerParams(vmem_limit_bytes=8 * 1024 * 1024),
        name="hand_over",
    )(*outs)
    return (
        outs[0][None], outs[1][None], outs[2][None], outs[3][None],
        jnp.swapaxes(outs[4], 0, 1), outs[5], outs[6], outs[7].reshape(-1), outs[8],
        outs[9].reshape(-1), outs[10].reshape(-1),
    )


def solution(mesh):
    split = Mesh(mesh.devices.reshape(NZ, 2, NX, 2, 2), AXES)
    rows = P(DP, None, TENSOR)
    return jax.shard_map(
        on_device,
        mesh=split,
        in_specs=(
            rows, rows, rows, rows, P(), P(),
            P(None, None, TENSOR), P(None, TENSOR), P(None, TENSOR), P(TENSOR), P(None, TENSOR),
        ),
        out_specs=(
            rows, rows, rows, rows,
            P(DP, None, TENSOR), P(DP, TENSOR), P(DP, TENSOR), P(TENSOR), P(DP, TENSOR),
            P(TENSOR), P(TENSOR),
        ),
        check_vma=False,
    )
```
